32 devices in a mesh: dp: 4 (over y, x), fsdp: 8 (over z, core).
Axes of the slice: x: 2, y: 2, z: 4, core: 2. Of those that a mesh axis runs over, the one named last changes fastest.
Arguments:
- tokens: bfloat16 [8192, 2048], P(('dp', 'fsdp')), may hold values from -6 to 6
- seq_lengths: int32 [32], P(('dp', 'fsdp')), may hold values from 256 to 256, as said below
- w_qkv: bfloat16 [2048, 6144], P(('dp', 'fsdp')), may hold values from -0.125 to 0.125
- bias_q: bfloat16 [2048], P(('dp', 'fsdp')), may hold values from -3 to 3
- bias_v: bfloat16 [2048], P(('dp', 'fsdp')), may hold values from -3 to 3
- w_out: bfloat16 [2048, 2048], P(('dp', 'fsdp')), may hold values from -0.375 to 0.375
- bias_out: bfloat16 [2048], P(('dp', 'fsdp')), may hold values from -2 to 2
- ln1_gain: bfloat16 [2048], P(('dp', 'fsdp')), may hold values from 0.5 to 1.5
- ln1_bias: bfloat16 [2048], P(('dp', 'fsdp')), may hold values from -1.1953125 to 1.1953125
- w_up: bfloat16 [2048, 8192], P(('dp', 'fsdp')), may hold values from -0.125 to 0.125
- bias_up: bfloat16 [8192], P(('dp', 'fsdp')), may hold values from -3 to 3
- w_down: bfloat16 [8192, 2048], P(('dp', 'fsdp')), may hold values from -0.0625 to 0.0625
- bias_down: bfloat16 [2048], P(('dp', 'fsdp')), may hold values from -2 to 2
- ln2_gain: bfloat16 [2048], P(('dp', 'fsdp')), may hold values from 0.5 to 1.5
- ln2_bias: bfloat16 [2048], P(('dp', 'fsdp')), may hold values from -1.1953125 to 1.1953125
- cotangent: bfloat16 [8192, 2048], P(('dp', 'fsdp')), may hold values from -6 to 6
Outputs:
- output: bfloat16 [8192, 2048], P(('dp', 'fsdp'))
- grad_tokens: bfloat16 [8192, 2048], P(('dp', 'fsdp'))
- grad_w_qkv: float32 [2048, 6144], P(('dp', 'fsdp'))
- grad_bias_q: float32 [2048], P(('dp', 'fsdp'))
- grad_bias_v: float32 [2048], P(('dp', 'fsdp'))
- grad_w_out: float32 [2048, 2048], P(('dp', 'fsdp'))
- grad_bias_out: float32 [2048], P(('dp', 'fsdp'))
- grad_ln1_gain: float32 [2048], P(('dp', 'fsdp'))
- grad_ln1_bias: float32 [2048], P(('dp', 'fsdp'))
- grad_w_up: float32 [2048, 8192], P(('dp', 'fsdp'))
- grad_bias_up: float32 [8192], P(('dp', 'fsdp'))
- grad_w_down: float32 [8192, 2048], P(('dp', 'fsdp'))
- grad_bias_down: float32 [2048], P(('dp', 'fsdp'))
- grad_ln2_gain: float32 [2048], P(('dp', 'fsdp'))
- grad_ln2_bias: float32 [2048], P(('dp', 'fsdp'))
- clipped_qkv: bfloat16 [2048, 6144], P(('dp', 'fsdp'))
The draws below stay inside these ranges and needn't reach their ends.
Inputs may be any that keep to these rules, and one draw needn't show every extreme that they name: `seq_lengths`: each device's sequence starts at slot 0; the rest of its 256 slots are padding. Every sequence fills all 256 slots of its device, so no slot is padding.
All inputs are finite; a program needn't handle non-finite values.
Results may differ from the reference program's by a relative error of at most 0.012.
Values may be sent and summed in bfloat16 or wider, within the bound.
A program may use at most 384 MiB of HBM per device.

```python
import jax
import jax.numpy as jnp
from jax import lax

D = 2048
HEADS = 32
HEAD_DIM = 64
FF = 8192
TOK_DEV = 256
MIN_LEN = 256
TOKENS = 8192
DEVICES = 32


def draw_seq_lengths(key, part):
    key_len, key_full = jax.random.split(jax.random.fold_in(key, 11), 2)
    ranks = jnp.arange(DEVICES, dtype=jnp.int32)
    lengths = jax.random.randint(key_len, (DEVICES,), MIN_LEN, TOK_DEV + 1).astype(jnp.int32)
    full_rank = jax.random.randint(key_full, (), 0, DEVICES).astype(jnp.int32)
    short_rank = ((full_rank + 1) % DEVICES).astype(jnp.int32)
    lengths = jnp.where(ranks == full_rank, TOK_DEV, lengths).astype(jnp.int32)
    lengths = jnp.where(ranks == short_rank, MIN_LEN, lengths).astype(jnp.int32)
    return lengths


def shard_levels(stream_key, shape, shards, smallest, high):
    def one(dim, blocks):
        heights = jax.random.uniform(jax.random.fold_in(jax.random.fold_in(stream_key, 6), dim), (blocks,), jnp.float32, smallest / len(shards), high / len(shards))
        return jnp.repeat(jnp.exp(heights), shape[dim] // blocks).reshape((-1,) + (1,) * (len(shape) - dim - 1))

    loudness = one(*shards[0])
    for cut in shards[1:]:
        loudness = loudness * one(*cut)
    return loudness


def normal_values(stream_key, dims, width, reach, pieces=(), kind=jnp.bfloat16):
    factor_of = shard_levels(stream_key, dims, pieces, -0.22, 0.18) if pieces else 1.0
    array = jax.random.normal(stream_key, dims, jnp.float32) * width * factor_of
    return jnp.minimum(jnp.maximum(array, -reach), reach).astype(kind)


def setup_inputs(seed: int = 0) -> dict:
    keys = jax.random.split(jax.random.key(seed), 17)
    return {
        "tokens": normal_values(keys[0], (TOKENS, D), 1.0, 6.0, ((0, 32),)),
        "seq_lengths": draw_seq_lengths(jax.random.fold_in(keys[16], 71), 0),
        "w_qkv": normal_values(keys[2], (D, 3 * D), D ** -0.5, 0.125, ((0, 32),)),
        "bias_q": normal_values(keys[3], (D,), 0.5, 3.0, ((0, 32),)),
        "bias_v": normal_values(keys[4], (D,), 0.5, 3.0, ((0, 32),)),
        "w_out": normal_values(keys[5], (D, D), (D // 8) ** -0.5, 0.375, ((0, 32),)),
        "bias_out": normal_values(keys[6], (D,), 0.3, 2.0, ((0, 32),)),
        "ln1_gain": jnp.clip(1.0 + 0.1 * jax.random.normal(keys[7], (D,), jnp.float32), 0.5, 1.5).astype(jnp.bfloat16),
        "ln1_bias": normal_values(keys[8], (D,), 0.2, 1.1953125, ((0, 32),)),
        "w_up": normal_values(keys[9], (D, FF), D ** -0.5, 0.125, ((0, 32),)),
        "bias_up": normal_values(keys[10], (FF,), 0.5, 3.0, ((0, 32),)),
        "w_down": normal_values(keys[11], (FF, D), FF ** -0.5, 0.0625, ((0, 32),)),
        "bias_down": normal_values(keys[12], (D,), 0.3, 2.0, ((0, 32),)),
        "ln2_gain": jnp.clip(1.0 + 0.1 * jax.random.normal(keys[13], (D,), jnp.float32), 0.5, 1.5).astype(jnp.bfloat16),
        "ln2_bias": normal_values(keys[14], (D,), 0.2, 1.1953125, ((0, 32),)),
        "cotangent": normal_values(keys[15], (TOKENS, D), 1.0, 6.0, ((0, 32),)),
    }


@jax.custom_vjp
def low(v):
    return lax.optimization_barrier(v.astype(jnp.bfloat16)).astype(jnp.float32)

@jax.custom_vjp
def low_back(v):
    return v

def low_keep(v):
    return (low(v), None)

def low_pass(kept, grad):
    return (grad,)

def back_keep(v):
    return (v, None)

def back_low(kept, grad):
    return (low(grad),)
low.defvjp(low_keep, low_pass)
low_back.defvjp(back_keep, back_low)
EPS = 1e-05
CLIP_TAU = 5.0
HIGH = lax.Precision.HIGHEST

def head_slopes(heads):
    ranks = jnp.arange(1, heads + 1, dtype=jnp.float32)
    return jnp.exp2(-8.0 * ranks / heads)

def segment_of(length):
    places = jnp.arange(TOK_DEV, dtype=jnp.int32)
    return jnp.where(places < length, 0, -1).astype(jnp.int32)

def block_masks(length):
    places = jnp.arange(TOK_DEV, dtype=jnp.int32)
    segment = segment_of(length)
    same = (segment[:, None] == segment[None, :]) & (segment[:, None] >= 0)
    valid = same & (places[None, :] <= places[:, None])
    allowed = valid | (places[:, None] == places[None, :])
    distance = (places[:, None] - places[None, :]).astype(jnp.float32)
    return (valid, allowed, distance)

def layer_norm(values, gain, bias):
    row_mean = lax.optimization_barrier(jnp.mean(values, axis=-1, keepdims=True))
    centred = values - row_mean
    variance = lax.optimization_barrier(jnp.mean(centred * centred, axis=-1, keepdims=True))
    return centred * lax.rsqrt(variance + EPS) * gain + bias

def attend_block(query_rows, key_rows, value_rows, length):
    valid, allowed, distance = block_masks(length)
    scale = HEAD_DIM ** (-0.5)
    logits = jnp.einsum('qhd,khd->hqk', query_rows, key_rows, precision=HIGH) * scale
    scores = low_back(logits - (head_slopes(HEADS) * scale)[:, None, None] * distance[None])
    scores = jnp.where(allowed[None], scores, -1e+30)
    probs = low(jax.nn.softmax(scores, axis=-1))
    mixed = jnp.einsum('hqk,khd->qhd', probs, value_rows, precision=HIGH)
    head_top = lax.optimization_barrier(jnp.max(jnp.where(valid[None], logits, -1e+30), axis=(1, 2)))
    return (mixed, head_top)

def attend_parts(parts):
    return jax.checkpoint(attend_block)(parts[0], parts[1], parts[2], parts[3])

def forward(tokens, w_qkv, bias_q, bias_v, w_out, bias_out, ln1_gain, ln1_bias, w_up, bias_up, w_down, bias_down, ln2_gain, ln2_bias, seq_lengths, keep):
    first_in = low(layer_norm(tokens, ln1_gain, ln1_bias))
    projected = jnp.dot(first_in, w_qkv, precision=HIGH)
    query_rows = low(low_back(projected[:, :D] + bias_q))
    key_rows = low(low_back(projected[:, D:2 * D]))
    value_rows = low(low_back(projected[:, 2 * D:] + bias_v))
    head_shape = (DEVICES, TOK_DEV, HEADS, HEAD_DIM)
    mixed, tops = lax.map(attend_parts, (query_rows.reshape(head_shape), key_rows.reshape(head_shape), value_rows.reshape(head_shape), seq_lengths))
    mixed = low(low_back(mixed.reshape(TOKENS, D)))
    hidden = tokens + low_back(jnp.dot(mixed, w_out, precision=HIGH) + bias_out)
    second_in = low(layer_norm(hidden, ln2_gain, ln2_bias))
    upward = low_back(jnp.dot(second_in, w_up, precision=HIGH) + bias_up)
    active = low(jax.nn.gelu(upward, approximate=False))
    branch = low_back(jnp.dot(active, w_down, precision=HIGH) + bias_down)
    return ((hidden + branch) * keep, lax.optimization_barrier(jnp.max(tops, axis=0)))

def reference(tokens, seq_lengths, w_qkv, bias_q, bias_v, w_out, bias_out, ln1_gain, ln1_bias, w_up, bias_up, w_down, bias_down, ln2_gain, ln2_bias, cotangent):
    segment = jax.vmap(segment_of)(seq_lengths)
    keep = (segment.reshape(TOKENS) >= 0).astype(jnp.float32)[:, None]
    params = (tokens, w_qkv, bias_q, bias_v, w_out, bias_out, ln1_gain, ln1_bias, w_up, bias_up, w_down, bias_down, ln2_gain, ln2_bias)
    params = tuple((item.astype(jnp.float32) for item in params))

    def wrapped(*values):
        return forward(*values, seq_lengths, keep)
    output, pull, head_top = jax.vjp(wrapped, *params, has_aux=True)
    grads = pull(cotangent.astype(jnp.float32))
    factor = jnp.sqrt(CLIP_TAU / jnp.maximum(head_top, CLIP_TAU))
    column = jnp.repeat(factor, HEAD_DIM)
    columns = jnp.concatenate([column, column, jnp.ones((D,), jnp.float32)])
    clipped = (w_qkv.astype(jnp.float32) * columns[None, :]).astype(jnp.bfloat16)
    return (output.astype(jnp.bfloat16), grads[0].astype(jnp.bfloat16), grads[1], grads[2], grads[3], grads[4], grads[5], grads[6], grads[7], grads[8], grads[9], grads[10], grads[11], grads[12], grads[13], clipped)
```

```python
import functools

import jax
import jax.numpy as jnp
from jax import lax
from jax.experimental import pallas as pl
from jax.experimental.pallas import tpu as pltpu
from jax.sharding import PartitionSpec as P

HEAD_DIM = 64
EPS = 1e-05
CLIP_TAU = 5.0
MASKED = 1e35
F32 = jnp.float32
BF16 = jnp.bfloat16
SCALE = HEAD_DIM ** (-0.5)


def swap(value, axis, size, bit):
    return lax.ppermute(value, axis, [(i, i ^ bit) for i in range(size)])


def bits_of(size):
    return [1 << b for b in range(size.bit_length() - 1)]


def gather_path(block, size, bits):
    blocks = {0: block}
    for bit in bits:
        held = sorted(blocks)
        moved = swap(jnp.concatenate([blocks[r] for r in held], 0), "dp", size, bit)
        for place, r in enumerate(held):
            rows = block.shape[0]
            blocks[r ^ bit] = moved[place * rows : (place + 1) * rows]
    return blocks


def gather_dp(block, size):
    half = block.shape[0] // 2
    top = gather_path(block[:half], size, bits_of(size))
    low = gather_path(block[half:], size, bits_of(size)[::-1])
    parts = []
    for r in range(size):
        parts += [top[r], low[r]]
    return jnp.concatenate(parts, 0)


def scatter_path(blocks, size, bits):
    blocks = dict(blocks)
    for bit in bits:
        away = sorted(r for r in blocks if r & bit)
        rows = blocks[0].shape[0]
        sent = jnp.concatenate([blocks[r].astype(BF16) for r in away], 0)
        moved = swap(sent, "dp", size, bit)
        blocks = {
            r ^ bit: blocks[r ^ bit].astype(F32)
            + moved[place * rows : (place + 1) * rows].astype(F32)
            for place, r in enumerate(away)
        }
    return blocks[0]


def scatter_dp(partial, size):
    rows = partial.shape[0] // size
    half = rows // 2
    top = {r: partial[r * rows : r * rows + half] for r in range(size)}
    low = {r: partial[r * rows + half : (r + 1) * rows] for r in range(size)}
    return jnp.concatenate(
        [scatter_path(top, size, bits_of(size)), scatter_path(low, size, bits_of(size)[::-1])], 0
    )


def combine_all(value, sizes, join):
    for axis, size in sizes:
        for bit in bits_of(size):
            value = join(value, swap(value, axis, size, bit))
    return value


def head_parts(ref, offset, pair):
    both = ref[:, pl.ds(offset + pair * 2 * HEAD_DIM, 2 * HEAD_DIM)]
    return both[:, :HEAD_DIM], both[:, HEAD_DIM:]


def dot_nt(a, b):
    return lax.dot_general(a, b, (((1,), (1,)), ((), ())), preferred_element_type=F32)


def dot_tn(a, b):
    return lax.dot_general(a, b, (((0,), (0,)), ((), ())), preferred_element_type=F32)


def attend_kernel(slope_ref, distance_ref, qkv_ref, mixed_ref, top_ref):
    width = mixed_ref.shape[1]
    heads = width // HEAD_DIM
    distance = distance_ref[...]
    lane = lax.broadcasted_iota(jnp.int32, (8, 128), 1)
    tops = jnp.zeros((8, 128), F32)
    for pair in range(heads // 2):
        outs = []
        for t, (q, k, v) in enumerate(
            zip(*(head_parts(qkv_ref, part * width, pair) for part in range(3)))
        ):
            logits = dot_nt(q * jnp.asarray(SCALE, BF16), k)
            head_top = jnp.max(jnp.where(distance < MASKED, logits, -1e30))
            tops = jnp.where(lane == pair * 2 + t, head_top, tops)
            scores = logits - slope_ref[pair * 2 + t] * distance
            expos = jnp.exp(scores - jnp.max(scores, axis=-1, keepdims=True))
            probs = expos * (1.0 / jnp.sum(expos, axis=-1, keepdims=True))
            outs.append(jnp.dot(probs.astype(BF16), v, preferred_element_type=F32))
        mixed_ref[:, pl.ds(pair * 2 * HEAD_DIM, 2 * HEAD_DIM)] = jnp.concatenate(outs, 1).astype(
            BF16
        )
    top_ref[...] = tops


def attend_back_kernel(slope_ref, distance_ref, qkv_ref, grad_ref, out_ref):
    width = grad_ref.shape[1]
    heads = width // HEAD_DIM
    distance = distance_ref[...]
    for pair in range(heads // 2):
        outs = ([], [], [])
        parts = [head_parts(qkv_ref, part * width, pair) for part in range(3)]
        parts.append(head_parts(grad_ref, 0, pair))
        for t, (q, k, v, grad) in enumerate(zip(*parts)):
            low_q = q * jnp.asarray(SCALE, BF16)
            scores = dot_nt(low_q, k) - slope_ref[pair * 2 + t] * distance
            expos = jnp.exp(scores - jnp.max(scores, axis=-1, keepdims=True))
            probs = expos * (1.0 / jnp.sum(expos, axis=-1, keepdims=True))
            outs[2].append(dot_tn(probs.astype(BF16), grad))
            grad_probs = dot_nt(grad, v)
            inner = jnp.sum(grad_probs * probs, axis=-1, keepdims=True)
            grad_scores = (probs * (grad_probs - inner)).astype(BF16)
            outs[0].append(
                jnp.dot(grad_scores, k, preferred_element_type=F32) * SCALE
            )
            outs[1].append(dot_tn(grad_scores, low_q))
        for part in range(3):
            out_ref[:, pl.ds(part * width + pair * 2 * HEAD_DIM, 2 * HEAD_DIM)] = (
                jnp.concatenate(outs[part], 1).astype(BF16)
            )


def attend(slopes, distance, qkv, length):
    rows, width = qkv.shape[0], qkv.shape[1] // 3
    blocks = rows // length
    mixed, tops = pl.pallas_call(
        attend_kernel,
        grid=(blocks,),
        in_specs=[
            pl.BlockSpec(memory_space=pltpu.SMEM),
            pl.BlockSpec((length, length), lambda b: (0, 0)),
            pl.BlockSpec((length, 3 * width), lambda b: (b, 0)),
        ],
        out_specs=[
            pl.BlockSpec((length, width), lambda b: (b, 0)),
            pl.BlockSpec((8, 128), lambda b: (b, 0)),
        ],
        out_shape=[
            jax.ShapeDtypeStruct((rows, width), BF16),
            jax.ShapeDtypeStruct((blocks * 8, 128), F32),
        ],
        cost_estimate=pl.CostEstimate(
            flops=4 * rows * length * width, bytes_accessed=8 * rows * width,
            transcendentals=rows * length * width // HEAD_DIM,
        ),
        name="attend",
    )(slopes, distance, qkv)
    return mixed, jnp.max(tops, axis=0)[: width // HEAD_DIM]


def attend_back(slopes, distance, qkv, grad, length):
    rows, width = grad.shape
    return pl.pallas_call(
        attend_back_kernel,
        grid=(rows // length,),
        in_specs=[
            pl.BlockSpec(memory_space=pltpu.SMEM),
            pl.BlockSpec((length, length), lambda b: (0, 0)),
            pl.BlockSpec((length, 3 * width), lambda b: (b, 0)),
            pl.BlockSpec((length, width), lambda b: (b, 0)),
        ],
        out_specs=pl.BlockSpec((length, 3 * width), lambda b: (b, 0)),
        out_shape=jax.ShapeDtypeStruct((rows, 3 * width), BF16),
        cost_estimate=pl.CostEstimate(
            flops=10 * rows * length * width, bytes_accessed=14 * rows * width,
            transcendentals=rows * length * width // HEAD_DIM,
        ),
        name="attend_back",
    )(slopes, distance, qkv, grad)


def norm_stats(values):
    row_mean = jnp.mean(values, axis=-1, keepdims=True)
    centred = values - row_mean
    inverse_std = lax.rsqrt(jnp.mean(centred * centred, axis=-1, keepdims=True) + EPS)
    return centred * inverse_std, inverse_std


def norm_back(grad_norm, normed, inverse_std, gain):
    scaled = grad_norm * gain
    return inverse_std * (
        scaled
        - jnp.mean(scaled, axis=-1, keepdims=True)
        - normed * jnp.mean(scaled * normed, axis=-1, keepdims=True)
    )


def dot(a, b):
    return jnp.dot(a, b, preferred_element_type=F32)


def body(
    dp, fsdp, tokens, seq_lengths, w_qkv, bias_q, bias_v, w_out, bias_out, ln1_gain, ln1_bias,
    w_up, bias_up, w_down, bias_down, ln2_gain, ln2_bias, cotangent,
):
    length, width = tokens.shape
    shard = w_qkv.shape[0]
    ff = w_up.shape[1]
    heads = width // HEAD_DIM
    part, ff_part = width // dp, ff // dp
    local_heads = heads // dp
    spot, place = lax.axis_index("dp"), lax.axis_index("fsdp")
    rank = spot * fsdp + place
    both = (("fsdp", fsdp), ("dp", dp))

    full_small = (bias_out, ln1_gain, ln1_bias, bias_down, ln2_gain, ln2_bias)
    row = jnp.concatenate(full_small + (bias_q, bias_v, bias_up))[None]
    table = jnp.zeros((dp * fsdp, row.shape[1]), BF16)
    table = lax.dynamic_update_slice(table, row, (rank, 0))
    table = combine_all(table, both, jnp.add).astype(F32)
    small = [table[:, k * shard : (k + 1) * shard].reshape(1, width) for k in range(6)]
    out_b, gain1, shift1, down_b, gain2, shift2 = small
    mine = lax.dynamic_slice(table, (spot * fsdp, 0), (fsdp, row.shape[1]))[:, 6 * shard :]
    q_b, v_b = mine[:, :shard].reshape(1, part), mine[:, shard : 2 * shard].reshape(1, part)
    up_b = mine[:, 2 * shard :].reshape(1, ff_part)

    cols = w_qkv.reshape(shard, 3, dp, part).transpose(0, 2, 1, 3).reshape(shard, 3 * width)
    cols = lax.all_to_all(cols, "dp", 1, 0, tiled=True).reshape(dp, shard, 3 * part)
    qkv_w = lax.all_gather(cols, "fsdp", axis=1, tiled=True).reshape(width, 3 * part)
    out_w = lax.all_gather(w_out, "fsdp", axis=0, tiled=True)
    ups = lax.all_to_all(w_up, "dp", 1, 0, tiled=True).reshape(dp, shard, ff_part)
    up_w = lax.all_gather(ups, "fsdp", axis=1, tiled=True).reshape(width, ff_part)
    down_w = lax.all_gather(w_down, "fsdp", axis=0, tiled=True)

    ranks = (spot * local_heads + 1 + jnp.arange(local_heads)).astype(F32)
    slopes = jnp.exp2(-8.0 * ranks / heads) * SCALE
    places = jnp.arange(length, dtype=jnp.int32)
    gap = places[:, None] - places[None, :]
    distance = jnp.where(gap >= 0, gap.astype(F32), MASKED)

    all_tokens = gather_dp(tokens, dp)
    normed_all, _ = norm_stats(all_tokens.astype(F32))
    first_in = (normed_all * gain1 + shift1).astype(BF16)
    biases = jnp.concatenate([q_b, jnp.zeros_like(q_b), v_b], 1)
    qkv = (dot(first_in, qkv_w) + biases).astype(BF16)
    mixed, tops = attend(slopes, distance, qkv, length)
    inputs = tokens.astype(F32)
    hidden = inputs + scatter_dp(dot(mixed, out_w).astype(BF16), dp) + out_b

    normed2, inverse2 = norm_stats(hidden)
    second_in = gather_dp((normed2 * gain2 + shift2).astype(BF16), dp)
    upward = dot(second_in, up_w) + up_b
    active, gelu_pull = jax.vjp(functools.partial(jax.nn.gelu, approximate=False), upward)
    active = active.astype(BF16)
    output = hidden + scatter_dp(dot(active, down_w).astype(BF16), dp) + down_b

    grad_y = gather_dp(cotangent, dp)
    grad_active = dot_nt(grad_y, down_w)
    grad_upward = gelu_pull(grad_active)[0].astype(BF16)
    grad_second = scatter_dp(dot_nt(grad_upward, up_w).astype(BF16), dp)
    grad_hidden = cotangent.astype(F32) + norm_back(grad_second, normed2, inverse2, gain2)

    def reduce_rows(grad):
        return lax.psum_scatter(grad.astype(BF16), "fsdp", scatter_dimension=0, tiled=True)

    def reduce_columns(grad):
        grad = grad.astype(BF16).reshape(dp, fsdp * shard, grad.shape[1])
        grad = lax.psum_scatter(grad, "fsdp", scatter_dimension=1, tiled=True)
        return lax.all_to_all(
            grad.reshape(dp * shard, grad.shape[2]), "dp", 0, 1, tiled=True
        ).astype(F32)

    grad_w_down = reduce_rows(dot_tn(active, grad_y)).astype(F32)
    grad_w_up = reduce_columns(dot_tn(second_in, grad_upward))

    grad_branch = grad_hidden.astype(BF16)
    branch_all = gather_dp(grad_branch, dp)
    grad_w_out = reduce_rows(dot_tn(mixed, branch_all)).astype(F32)
    grad_mixed = dot_nt(branch_all, out_w).astype(BF16)
    grad_proj = attend_back(slopes, distance, qkv, grad_mixed, length)
    grad_first = scatter_dp(dot_nt(grad_proj, qkv_w).astype(BF16), dp)
    grad_w_qkv = reduce_columns(dot_tn(first_in, grad_proj))
    grad_w_qkv = (
        grad_w_qkv.reshape(shard, dp, 3, part).transpose(0, 2, 1, 3).reshape(shard, 3 * width)
    )
    normed1, inverse1 = norm_stats(inputs)
    grad_tokens = grad_hidden + norm_back(grad_first, normed1, inverse1, gain1)

    def spread(piece):
        wide = jnp.zeros((piece.shape[0] * dp,), F32)
        return lax.dynamic_update_slice(wide, piece, (spot * piece.shape[0],))

    def owned(total, start, size):
        step = size // (dp * fsdp)
        return lax.dynamic_slice(total, (start + rank * step,), (step,))

    early = jnp.concatenate([
        jnp.sum(cotangent.astype(F32), axis=0),
        jnp.sum(grad_second * normed2, axis=0),
        jnp.sum(grad_second, axis=0),
        jnp.sum(grad_branch.astype(F32), axis=0),
        spread(jnp.sum(grad_upward.astype(F32), axis=0)),
    ])
    early = combine_all(early, both, jnp.add)
    late = jnp.concatenate([
        spread(jnp.sum(grad_proj[:, :part].astype(F32), axis=0)),
        spread(jnp.sum(grad_proj[:, 2 * part :].astype(F32), axis=0)),
        jnp.sum(grad_first * normed1, axis=0),
        jnp.sum(grad_first, axis=0),
    ])
    late = combine_all(late, both, jnp.add)

    head_top = jnp.full((heads,), -1e30, F32)
    head_top = lax.dynamic_update_slice(head_top, tops, (spot * local_heads,))
    head_top = combine_all(head_top, both, jnp.maximum)
    factor = jnp.sqrt(CLIP_TAU / jnp.maximum(head_top, CLIP_TAU))
    column = jnp.repeat(factor, HEAD_DIM)
    columns = jnp.concatenate([column, column, jnp.ones((width,), F32)])
    clipped = (w_qkv.astype(F32) * columns[None, :]).astype(BF16)
    return (
        output.astype(BF16),
        grad_tokens.astype(BF16),
        grad_w_qkv,
        owned(late, 0, width),
        owned(late, width, width),
        grad_w_out,
        owned(early, 3 * width, width),
        owned(late, 2 * width, width),
        owned(late, 3 * width, width),
        grad_w_up,
        owned(early, 4 * width, ff),
        grad_w_down,
        owned(early, 0, width),
        owned(early, width, width),
        owned(early, 2 * width, width),
        clipped,
    )


def solution(mesh):
    rows, flat = P(("dp", "fsdp"), None), P(("dp", "fsdp"))
    return jax.shard_map(
        functools.partial(body, mesh.shape["dp"], mesh.shape["fsdp"]),
        mesh=mesh,
        in_specs=(
            rows, flat, rows, flat, flat, rows, flat, flat, flat, rows, flat, rows, flat, flat,
            flat, rows,
        ),
        out_specs=(
            rows, rows, rows, flat, flat, rows, flat, flat, flat, rows, flat, rows, flat, flat,
            flat, rows,
        ),
        check_vma=False,
    )
```

```python
import functools

import jax
import jax.numpy as jnp
from jax import lax
from jax.experimental import pallas as pl
from jax.experimental.pallas import tpu as pltpu
from jax.sharding import PartitionSpec as P


HEAD_DIM = 64
EPS = 1e-05
CLIP_TAU = 5.0
MASKED = 1e35
F32 = jnp.float32
BF16 = jnp.bfloat16
SCALE = HEAD_DIM ** (-0.5)


def swap(value, axis, size, bit):
    return lax.ppermute(value, axis, [(i, i ^ bit) for i in range(size)])


def bits_of(size):
    return [1 << b for b in range(size.bit_length() - 1)]


def gather_path(block, size, bits):
    blocks = {0: block}
    for bit in bits:
        held = sorted(blocks)
        moved = swap(jnp.concatenate([blocks[r] for r in held], 0), "dp", size, bit)
        for place, r in enumerate(held):
            rows = block.shape[0]
            blocks[r ^ bit] = moved[place * rows : (place + 1) * rows]
    return blocks


def gather_dp(block, size):
    half = block.shape[0] // 2
    top = gather_path(block[:half], size, bits_of(size))
    low = gather_path(block[half:], size, bits_of(size)[::-1])
    parts = []
    for r in range(size):
        parts += [top[r], low[r]]
    return jnp.concatenate(parts, 0)


def scatter_path(blocks, size, bits):
    blocks = dict(blocks)
    for bit in bits:
        away = sorted(r for r in blocks if r & bit)
        rows = blocks[0].shape[0]
        sent = jnp.concatenate([blocks[r].astype(BF16) for r in away], 0)
        moved = swap(sent, "dp", size, bit)
        blocks = {
            r ^ bit: blocks[r ^ bit].astype(F32)
            + moved[place * rows : (place + 1) * rows].astype(F32)
            for place, r in enumerate(away)
        }
    return blocks[0]


def scatter_dp(partial, size):
    rows = partial.shape[0] // size
    half = rows // 2
    top = {r: partial[r * rows : r * rows + half] for r in range(size)}
    low = {r: partial[r * rows + half : (r + 1) * rows] for r in range(size)}
    return jnp.concatenate(
        [scatter_path(top, size, bits_of(size)), scatter_path(low, size, bits_of(size)[::-1])], 0
    )


def combine_all(value, sizes, join):
    for axis, size in sizes:
        for bit in bits_of(size):
            value = join(value, swap(value, axis, size, bit))
    return value


STEPS = 4
MESH_IDS = pl.DeviceIdType.MESH
PATHS = ((1, 2), (2, 1))


def neighbours():
    me = lax.axis_index("dp")
    near = {1: {"dp": me + 1 - 2 * (me % 2)}, 2: {"dp": (me + 2) % 4}}
    barrier = pltpu.get_barrier_semaphore()
    for bit in (1, 2):
        pl.semaphore_signal(barrier, inc=1, device_id=near[bit], device_id_type=MESH_IDS)
    pl.semaphore_wait(barrier, 2)
    return near


def remote(source, target, sems, index, where):
    return pltpu.make_async_remote_copy(
        src_ref=source, dst_ref=target, send_sem=sems.at[0, index], recv_sem=sems.at[1, index],
        device_id=where, device_id_type=MESH_IDS,
    )


def each_step(act):
    def run(step, carry):
        act(step)
        return carry

    lax.fori_loop(0, STEPS, run, 0)


class Gather:
    def __init__(self, out, sems, near):
        self.out, self.sems, self.near = out, sems, near
        self.rows = out.shape[0] // 4
        self.step_rows = self.rows // 2 // STEPS

    def span(self, block, path, step):
        start = block * self.rows + path * (self.rows // 2) + step * self.step_rows
        return pl.ds(pl.multiple_of(start, self.step_rows), self.step_rows)

    def copy(self, source, bit, path, step, kind):
        return remote(
            self.out.at[self.span(source, path, step)],
            self.out.at[self.span(source + bit, path, step)],
            self.sems, (path * 3 + kind) * STEPS + step, self.near[bit],
        )

    def send(self, path, step):
        first, second = PATHS[path]
        self.copy(0, first, path, step, 0).start()
        self.copy(0, second, path, step, 1).start()

    def forward(self, path, step):
        first, second = PATHS[path]
        self.copy(0, first, path, step, 0).wait_recv()
        self.copy(first, second, path, step, 2).start()

    def finish(self, path, step):
        first, second = PATHS[path]
        self.copy(0, first, path, step, 0).wait_send()
        self.copy(0, second, path, step, 1).wait()
        self.copy(first, second, path, step, 2).wait()


class Scatter:
    def __init__(self, partial, landing, passing, last, sems, near):
        self.partial, self.landing, self.passing, self.last = partial, landing, passing, last
        self.sems, self.near = sems, near
        self.rows = partial.shape[0] // 4
        self.step_rows = self.rows // 2 // STEPS

    def span(self, block, path, step):
        start = block * self.rows + path * (self.rows // 2) + step * self.step_rows
        return pl.ds(pl.multiple_of(start, self.step_rows), self.step_rows)

    def own(self, path, step):
        return self.span(0, path, step)

    def opening(self, path, step, kind):
        first, _ = PATHS[path]
        return remote(
            self.partial.at[self.span((first, 3)[kind], path, step)],
            self.landing.at[kind, self.own(path, step)],
            self.sems, (path * 3 + kind) * STEPS + step, self.near[first],
        )

    def closing(self, path, step):
        rows = self.own(path, step)
        return remote(
            self.passing.at[rows], self.last.at[rows], self.sems,
            (path * 3 + 2) * STEPS + step, self.near[PATHS[path][1]],
        )

    def begin(self, path, step):
        for kind in range(2):
            self.opening(path, step, kind).start()

    def relay(self, path, step):
        _, second = PATHS[path]
        self.opening(path, step, 1).wait_recv()
        rows = self.own(path, step)
        self.passing[rows] = (
            self.partial[self.span(second, path, step)].astype(F32)
            + self.landing[1, rows].astype(F32)
        ).astype(BF16)
        self.closing(path, step).start()

    def total(self, path, step):
        self.opening(path, step, 0).wait_recv()
        self.closing(path, step).wait_recv()
        rows = self.own(path, step)
        return (
            self.partial[self.span(0, path, step)].astype(F32)
            + self.landing[0, rows].astype(F32)
            + self.last[rows].astype(F32)
        )

    def finish(self, path, step):
        for kind in range(2):
            self.opening(path, step, kind).wait_send()
        self.closing(path, step).wait_send()


def row_norm(values):
    centred = values - jnp.mean(values, axis=-1, keepdims=True)
    inverse_std = lax.rsqrt(jnp.mean(centred * centred, axis=-1, keepdims=True) + EPS)
    return centred * inverse_std, inverse_std


def row_back(grad_norm, normed, inverse_std, gain):
    scaled = grad_norm * gain
    return inverse_std * (
        scaled
        - jnp.mean(scaled, axis=-1, keepdims=True)
        - normed * jnp.mean(scaled * normed, axis=-1, keepdims=True)
    )


def gather_two_kernel(one_ref, two_ref, out_one, out_two, sems):
    near = neighbours()
    jobs = []
    for k, (source, out) in enumerate(((one_ref, out_one), (two_ref, out_two))):
        out[: source.shape[0]] = source[...]
        jobs.append(Gather(out, sems.at[k], near))
    for job in jobs:
        each_step(lambda step, job=job: [job.send(path, step) for path in range(2)])
    for job in jobs:
        each_step(lambda step, job=job: [job.forward(path, step) for path in range(2)])
    for job in jobs:
        each_step(lambda step, job=job: [job.finish(path, step) for path in range(2)])


def exchange(scatter, gather, rows_of):
    each_step(lambda step: [scatter.begin(path, step) for path in range(2)])
    each_step(lambda step: [scatter.relay(path, step) for path in range(2)])

    def middle(step):
        for path in range(2):
            rows = scatter.own(path, step)
            gather.out[rows] = rows_of(rows, scatter.total(path, step))
            gather.send(path, step)

        @pl.when(step > 0)
        def _():
            for path in range(2):
                gather.forward(path, step - 1)

    each_step(middle)
    for path in range(2):
        gather.forward(path, STEPS - 1)
    each_step(lambda step: [scatter.finish(path, step) for path in range(2)])
    each_step(lambda step: [gather.finish(path, step) for path in range(2)])


def add_sums(sums_ref, values):
    for k, value in enumerate(values):
        sums_ref[k : k + 1] += jnp.sum(value, axis=0, keepdims=True)


def hidden_kernel(
    partial_ref, tokens_ref, params_ref, out_ref, hidden_ref, landing, passing, last, sems
):
    near = neighbours()

    def rows_of(rows, total):
        hidden = tokens_ref[rows].astype(F32) + total + params_ref[0:1]
        hidden_ref[rows] = hidden
        normed, _ = row_norm(hidden)
        return (normed * params_ref[1:2] + params_ref[2:3]).astype(BF16)

    exchange(
        Scatter(partial_ref, landing, passing, last, sems.at[0], near),
        Gather(out_ref, sems.at[1], near), rows_of,
    )


def branch_kernel(
    partial_ref, hidden_ref, cotangent_ref, params_ref, out_ref, grad_ref, sums_ref, landing,
    passing, last, sems,
):
    near = neighbours()
    sums_ref[...] = jnp.zeros_like(sums_ref)

    def rows_of(rows, total):
        normed, inverse_std = row_norm(hidden_ref[rows])
        upper = cotangent_ref[rows].astype(F32)
        grad = upper + row_back(total, normed, inverse_std, params_ref[1:2])
        grad_ref[rows] = grad
        branch = grad.astype(BF16)
        add_sums(sums_ref, (upper, total * normed, total, branch.astype(F32)))
        return branch

    exchange(
        Scatter(partial_ref, landing, passing, last, sems.at[0], near),
        Gather(out_ref, sems.at[1], near), rows_of,
    )


def last_kernel(
    first_ref, output_ref, tokens_ref, hidden_ref, grad_ref, params_ref, tokens_out, output_out,
    sums_ref, landing, passing, last, sems,
):
    near = neighbours()
    sums_ref[...] = jnp.zeros_like(sums_ref)
    first, second = (
        Scatter(ref, landing.at[k], passing.at[k], last.at[k], sems.at[k], near)
        for k, ref in enumerate((first_ref, output_ref))
    )

    def first_rows(path, step):
        rows = first.own(path, step)
        total = first.total(path, step)
        normed, inverse_std = row_norm(tokens_ref[rows].astype(F32))
        grad = grad_ref[rows] + row_back(total, normed, inverse_std, params_ref[0:1])
        tokens_out[rows] = grad.astype(BF16)
        add_sums(sums_ref, (total * normed, total))

    def second_rows(path, step):
        rows = second.own(path, step)
        total = second.total(path, step)
        output_out[rows] = (hidden_ref[rows] + total + params_ref[1:2]).astype(BF16)

    for job in (first, second):
        each_step(lambda step, job=job: [job.begin(path, step) for path in range(2)])
    for job in (first, second):
        each_step(lambda step, job=job: [job.relay(path, step) for path in range(2)])
    each_step(lambda step: [first_rows(path, step) for path in range(2)])
    each_step(lambda step: [second_rows(path, step) for path in range(2)])
    for job in (first, second):
        each_step(lambda step, job=job: [job.finish(path, step) for path in range(2)])


def call_exchange(kernel, number, jobs, scatters, outs, args):
    rows, width = args[0].shape if scatters else (4 * args[0].shape[0], args[0].shape[1])
    own = rows // 4
    room = []
    if scatters == 1:
        room = [(2, own, width), (own, width), (own, width)]
    if scatters == 2:
        room = [(2, 2, own, width), (2, own, width), (2, own, width)]
    return pl.pallas_call(
        kernel,
        in_specs=[pl.BlockSpec(memory_space=pltpu.VMEM)] * len(args),
        out_specs=[pl.BlockSpec(memory_space=pltpu.VMEM)] * len(outs),
        out_shape=[jax.ShapeDtypeStruct(shape, dtype) for shape, dtype in outs],
        scratch_shapes=[
            *(pltpu.VMEM(shape, BF16) for shape in room),
            pltpu.SemaphoreType.DMA((jobs, 2, 6 * STEPS)),
        ],
        compiler_params=pltpu.CompilerParams(
            collective_id=number, has_side_effects=True, vmem_limit_bytes=48 << 20
        ),
        cost_estimate=pl.CostEstimate(
            flops=rows * width, bytes_accessed=200 << 20, transcendentals=0
        ),
    )(*args)


def pair_span(offset, pair):
    return pl.ds(pl.multiple_of(offset + pair * 2 * HEAD_DIM, 2 * HEAD_DIM), 2 * HEAD_DIM)


def head_parts(ref, offset, pair):
    both = ref[:, pair_span(offset, pair)]
    return both[:, :HEAD_DIM], both[:, HEAD_DIM:]


def dot_nt(a, b):
    return lax.dot_general(a, b, (((1,), (1,)), ((), ())), preferred_element_type=F32)


def dot_tn(a, b):
    return lax.dot_general(a, b, (((0,), (0,)), ((), ())), preferred_element_type=F32)


def attend_kernel(slope_ref, distance_ref, qkv_ref, mixed_ref, top_ref):
    width = mixed_ref.shape[1]
    lane = lax.broadcasted_iota(jnp.int32, (8, 128), 1)

    def pair_step(pair, tops):
        distance = distance_ref[...]
        outs = []
        for t, (q, k, v) in enumerate(
            zip(*(head_parts(qkv_ref, part * width, pair) for part in range(3)))
        ):
            logits = dot_nt(q * jnp.asarray(SCALE, BF16), k)
            head_top = jnp.max(jnp.where(distance < MASKED, logits, -1e30))
            tops = jnp.where(lane == pair * 2 + t, head_top, tops)
            scores = logits - slope_ref[pair * 2 + t] * distance
            expos = jnp.exp(scores - jnp.max(scores, axis=-1, keepdims=True))
            probs = expos * (1.0 / jnp.sum(expos, axis=-1, keepdims=True))
            outs.append(jnp.dot(probs.astype(BF16), v, preferred_element_type=F32))
        mixed_ref[:, pair_span(0, pair)] = jnp.concatenate(outs, 1).astype(BF16)
        return tops

    pairs = width // HEAD_DIM // 2
    top_ref[...] = lax.fori_loop(0, pairs, pair_step, jnp.zeros((8, 128), F32))


def attend_back_kernel(slope_ref, distance_ref, qkv_ref, grad_ref, out_ref):
    width = grad_ref.shape[1]

    def pair_step(pair, carry):
        distance = distance_ref[...]
        outs = ([], [], [])
        parts = [head_parts(qkv_ref, part * width, pair) for part in range(3)]
        parts.append(head_parts(grad_ref, 0, pair))
        for t, (q, k, v, grad) in enumerate(zip(*parts)):
            low_q = q * jnp.asarray(SCALE, BF16)
            scores = dot_nt(low_q, k) - slope_ref[pair * 2 + t] * distance
            expos = jnp.exp(scores - jnp.max(scores, axis=-1, keepdims=True))
            probs = expos * (1.0 / jnp.sum(expos, axis=-1, keepdims=True))
            outs[2].append(dot_tn(probs.astype(BF16), grad))
            grad_probs = dot_nt(grad, v)
            inner = jnp.sum(grad_probs * probs, axis=-1, keepdims=True)
            grad_scores = (probs * (grad_probs - inner)).astype(BF16)
            outs[0].append(jnp.dot(grad_scores, k, preferred_element_type=F32) * SCALE)
            outs[1].append(dot_tn(grad_scores, low_q))
        for part in range(3):
            out_ref[:, pair_span(part * width, pair)] = jnp.concatenate(outs[part], 1).astype(BF16)
        return carry

    lax.fori_loop(0, width // HEAD_DIM // 2, pair_step, 0)


def attend(slopes, distance, qkv, length):
    rows, width = qkv.shape[0], qkv.shape[1] // 3
    blocks = rows // length
    mixed, tops = pl.pallas_call(
        attend_kernel,
        grid=(blocks,),
        in_specs=[
            pl.BlockSpec(memory_space=pltpu.SMEM),
            pl.BlockSpec((length, length), lambda b: (0, 0)),
            pl.BlockSpec((length, 3 * width), lambda b: (b, 0)),
        ],
        out_specs=[
            pl.BlockSpec((length, width), lambda b: (b, 0)),
            pl.BlockSpec((8, 128), lambda b: (b, 0)),
        ],
        out_shape=[
            jax.ShapeDtypeStruct((rows, width), BF16),
            jax.ShapeDtypeStruct((blocks * 8, 128), F32),
        ],
        cost_estimate=pl.CostEstimate(
            flops=4 * rows * length * width, bytes_accessed=8 * rows * width,
            transcendentals=rows * length * width // HEAD_DIM,
        ),
        name="attend",
    )(slopes, distance, qkv)
    return mixed, jnp.max(tops, axis=0)[: width // HEAD_DIM]


def attend_back(slopes, distance, qkv, grad, length):
    rows, width = grad.shape
    return pl.pallas_call(
        attend_back_kernel,
        grid=(rows // length,),
        in_specs=[
            pl.BlockSpec(memory_space=pltpu.SMEM),
            pl.BlockSpec((length, length), lambda b: (0, 0)),
            pl.BlockSpec((length, 3 * width), lambda b: (b, 0)),
            pl.BlockSpec((length, width), lambda b: (b, 0)),
        ],
        out_specs=pl.BlockSpec((length, 3 * width), lambda b: (b, 0)),
        out_shape=jax.ShapeDtypeStruct((rows, 3 * width), BF16),
        cost_estimate=pl.CostEstimate(
            flops=10 * rows * length * width, bytes_accessed=14 * rows * width,
            transcendentals=rows * length * width // HEAD_DIM,
        ),
        name="attend_back",
    )(slopes, distance, qkv, grad)


def norm_stats(values):
    row_mean = jnp.mean(values, axis=-1, keepdims=True)
    centred = values - row_mean
    inverse_std = lax.rsqrt(jnp.mean(centred * centred, axis=-1, keepdims=True) + EPS)
    return centred * inverse_std, inverse_std


def norm_back(grad_norm, normed, inverse_std, gain):
    scaled = grad_norm * gain
    return inverse_std * (
        scaled
        - jnp.mean(scaled, axis=-1, keepdims=True)
        - normed * jnp.mean(scaled * normed, axis=-1, keepdims=True)
    )


def dot(a, b):
    return jnp.dot(a, b, preferred_element_type=F32)


def layer(
    dp, fsdp, tokens, seq_lengths, w_qkv, bias_q, bias_v, w_out, bias_out, ln1_gain, ln1_bias,
    w_up, bias_up, w_down, bias_down, ln2_gain, ln2_bias, cotangent,
):
    length, width = tokens.shape
    shard = w_qkv.shape[0]
    ff = w_up.shape[1]
    heads = width // HEAD_DIM
    part, ff_part = width // dp, ff // dp
    local_heads = heads // dp
    spot, place = lax.axis_index("dp"), lax.axis_index("fsdp")
    rank = spot * fsdp + place
    both = (("fsdp", fsdp), ("dp", dp))

    full_small = (bias_out, ln1_gain, ln1_bias, bias_down, ln2_gain, ln2_bias)
    row = jnp.concatenate(full_small + (bias_q, bias_v, bias_up))[None]
    table = jnp.zeros((dp * fsdp, row.shape[1]), BF16)
    table = lax.dynamic_update_slice(table, row, (rank, 0))
    table = combine_all(table, both, jnp.add).astype(F32)
    small = [table[:, k * shard : (k + 1) * shard].reshape(1, width) for k in range(6)]
    out_b, gain1, shift1, down_b, gain2, shift2 = small
    mine = lax.dynamic_slice(table, (spot * fsdp, 0), (fsdp, row.shape[1]))[:, 6 * shard :]
    q_b, v_b = mine[:, :shard].reshape(1, part), mine[:, shard : 2 * shard].reshape(1, part)
    up_b = mine[:, 2 * shard :].reshape(1, ff_part)

    out_w = lax.all_gather(w_out, "fsdp", axis=0, tiled=True)
    cols = w_qkv.reshape(shard, 3, dp, part).transpose(0, 2, 1, 3).reshape(shard, 3 * width)
    cols = lax.all_to_all(cols, "dp", 1, 0, tiled=True).reshape(dp, shard, 3 * part)
    qkv_w = lax.all_gather(cols, "fsdp", axis=1, tiled=True).reshape(width, 3 * part)
    w_up, cols = lax.optimization_barrier((w_up, cols))
    ups = lax.all_to_all(w_up, "dp", 1, 0, tiled=True).reshape(dp, shard, ff_part)
    up_w = lax.all_gather(ups, "fsdp", axis=1, tiled=True).reshape(width, ff_part)
    down_w = lax.all_gather(w_down, "fsdp", axis=0, tiled=True)

    ranks = (spot * local_heads + 1 + jnp.arange(local_heads)).astype(F32)
    slopes = jnp.exp2(-8.0 * ranks / heads) * SCALE
    places = jnp.arange(length, dtype=jnp.int32)
    gap = places[:, None] - places[None, :]
    distance = jnp.where(gap >= 0, gap.astype(F32), MASKED)

    inputs = tokens.astype(F32)
    wide = (4 * length, width)
    narrow = (length, width)
    kernels = dp == 4 and length % (32 * STEPS) == 0
    ordered_tokens, ups, cols = lax.optimization_barrier((tokens, ups, cols))
    if kernels:
        all_tokens, grad_y = call_exchange(
            gather_two_kernel, 1, 2, 0, [(wide, BF16)] * 2,
            [ordered_tokens, cotangent],
        )
    else:
        all_tokens, grad_y = gather_dp(ordered_tokens, dp), gather_dp(cotangent, dp)
    normed_all, _ = norm_stats(all_tokens.astype(F32))
    first_in = (normed_all * gain1 + shift1).astype(BF16)
    biases = jnp.concatenate([q_b, jnp.zeros_like(q_b), v_b], 1)
    qkv = (dot(first_in, qkv_w) + biases).astype(BF16)
    mixed, tops = attend(slopes, distance, qkv, length)
    out_part = dot(mixed, out_w).astype(BF16)
    if kernels:
        second_in, hidden = call_exchange(
            hidden_kernel, 2, 2, 1, [(wide, BF16), (narrow, F32)],
            [out_part, tokens, jnp.concatenate([out_b, gain2, shift2], 0)],
        )
    else:
        hidden = inputs + scatter_dp(out_part, dp) + out_b
        normed2, inverse2 = norm_stats(hidden)
        second_in = gather_dp((normed2 * gain2 + shift2).astype(BF16), dp)

    upward = dot(second_in, up_w) + up_b
    cumulative = 0.5 * (1.0 + lax.erf(upward * (0.5**0.5)))
    active = (upward * cumulative).astype(BF16)
    slope = cumulative + upward * jnp.exp(-0.5 * upward * upward) * ((0.5 / jnp.pi) ** 0.5)
    active, slope = lax.optimization_barrier((active, slope.astype(BF16)))

    def reduce_rows(grad):
        return lax.psum_scatter(grad, "fsdp", scatter_dimension=0, tiled=True).astype(F32)

    def reduce_columns(grad):
        grad = grad.reshape(dp, fsdp * shard, grad.shape[1])
        grad = lax.psum_scatter(grad, "fsdp", scatter_dimension=1, tiled=True)
        return lax.all_to_all(
            grad.reshape(dp * shard, grad.shape[2]), "dp", 0, 1, tiled=True
        ).astype(F32)

    local_down = dot_tn(active, grad_y).astype(BF16)
    late_y, slope, _ = lax.optimization_barrier((grad_y, slope, local_down))
    grad_upward = (dot_nt(late_y, down_w) * slope).astype(BF16)
    grad_w_down = reduce_rows(local_down)
    local_up = dot_tn(second_in, grad_upward).astype(BF16)
    late_upward, _ = lax.optimization_barrier((grad_upward, local_up))
    second_part = dot_nt(late_upward, up_w).astype(BF16)
    grad_w_up = reduce_columns(local_up)
    if kernels:
        branch_all, grad_hidden, branch_sums = call_exchange(
            branch_kernel, 3, 2, 1, [(wide, BF16), (narrow, F32), ((8, width), F32)],
            [second_part, hidden, cotangent, jnp.concatenate([out_b, gain2], 0)],
        )
    else:
        grad_second = scatter_dp(second_part, dp)
        grad_hidden = cotangent.astype(F32) + norm_back(grad_second, normed2, inverse2, gain2)
        grad_branch = grad_hidden.astype(BF16)
        branch_all = gather_dp(grad_branch, dp)
        branch_sums = jnp.stack([
            jnp.sum(piece, axis=0)
            for piece in (
                cotangent.astype(F32), grad_second * normed2, grad_second,
                grad_branch.astype(F32),
            )
        ])

    grad_mixed = dot_nt(branch_all, out_w).astype(BF16)
    grad_proj = attend_back(slopes, distance, qkv, grad_mixed, length)
    local_qkv = dot_tn(first_in, grad_proj).astype(BF16)
    late_branch, late_active, late_proj, _ = lax.optimization_barrier(
        (branch_all, active, grad_proj, local_qkv)
    )
    grad_w_qkv = reduce_columns(local_qkv)
    grad_w_qkv = (
        grad_w_qkv.reshape(shard, dp, 3, part).transpose(0, 2, 1, 3).reshape(shard, 3 * width)
    )
    local_out = dot_tn(mixed, late_branch).astype(BF16)
    grad_w_out = reduce_rows(local_out)
    first_part = dot_nt(late_proj, qkv_w).astype(BF16)
    output_part = dot(late_active, down_w).astype(BF16)
    if kernels:
        grad_tokens, output, last_sums = call_exchange(
            last_kernel, 4, 2, 2, [(narrow, BF16), (narrow, BF16), ((8, width), F32)],
            [first_part, output_part, tokens, hidden, grad_hidden,
             jnp.concatenate([gain1, down_b], 0)],
        )
    else:
        grad_first = scatter_dp(first_part, dp)
        normed1, inverse1 = norm_stats(inputs)
        grad_tokens = grad_hidden + norm_back(grad_first, normed1, inverse1, gain1)
        output = hidden + scatter_dp(output_part, dp) + down_b
        last_sums = jnp.stack([jnp.sum(grad_first * normed1, axis=0), jnp.sum(grad_first, axis=0)])

    def spread(piece):
        wide = jnp.zeros((piece.shape[0] * dp,), F32)
        return lax.dynamic_update_slice(wide, piece, (spot * piece.shape[0],))

    def owned(total, start, size):
        step = size // (dp * fsdp)
        return lax.dynamic_slice(total, (start + rank * step,), (step,))

    early = jnp.concatenate([
        branch_sums[:4].reshape(4 * width),
        spread(jnp.sum(grad_upward.astype(F32), axis=0)),
        spread(jnp.sum(grad_proj[:, :part].astype(F32), axis=0)),
        spread(jnp.sum(grad_proj[:, 2 * part :].astype(F32), axis=0)),
    ])
    early = combine_all(early, both, jnp.add)
    late = combine_all(last_sums[:2].reshape(2 * width), both, jnp.add)

    head_top = jnp.full((heads,), -1e30, F32)
    head_top = lax.dynamic_update_slice(head_top, tops, (spot * local_heads,))
    head_top = combine_all(head_top, both, jnp.maximum)
    factor = jnp.sqrt(CLIP_TAU / jnp.maximum(head_top, CLIP_TAU))
    column = jnp.repeat(factor, HEAD_DIM)
    columns = jnp.concatenate([column, column, jnp.ones((width,), F32)])
    clipped = (w_qkv.astype(F32) * columns[None, :]).astype(BF16)
    return (
        output.astype(BF16),
        grad_tokens.astype(BF16),
        grad_w_qkv,
        owned(early, 4 * width + ff, width),
        owned(early, 5 * width + ff, width),
        grad_w_out,
        owned(early, 3 * width, width),
        owned(late, 0, width),
        owned(late, width, width),
        grad_w_up,
        owned(early, 4 * width, ff),
        grad_w_down,
        owned(early, 0, width),
        owned(early, width, width),
        owned(early, 2 * width, width),
        clipped,
    )


def solution(mesh):
    rows, flat = P(("dp", "fsdp"), None), P(("dp", "fsdp"))
    return jax.shard_map(
        functools.partial(layer, mesh.shape["dp"], mesh.shape["fsdp"]),
        mesh=mesh,
        in_specs=(
            rows, flat, rows, flat, flat, rows, flat, flat, flat, rows, flat, rows, flat, flat,
            flat, rows,
        ),
        out_specs=(
            rows, rows, rows, flat, flat, rows, flat, flat, flat, rows, flat, rows, flat, flat,
            flat, rows,
        ),
        check_vma=False,
    )
```

```python
import functools

import jax
import jax.numpy as jnp
from jax import lax
from jax.experimental import pallas as pl
from jax.experimental.pallas import tpu as pltpu
from jax.sharding import PartitionSpec as P


HEAD_DIM = 64
EPS = 1e-05
CLIP_TAU = 5.0
MASKED = 1e35
F32 = jnp.float32
BF16 = jnp.bfloat16
SCALE = HEAD_DIM ** (-0.5)


def swap(value, axis, size, bit):
    return lax.ppermute(value, axis, [(i, i ^ bit) for i in range(size)])


def bits_of(size):
    return [1 << b for b in range(size.bit_length() - 1)]


def gather_path(block, size, bits):
    blocks = {0: block}
    for bit in bits:
        held = sorted(blocks)
        moved = swap(jnp.concatenate([blocks[r] for r in held], 0), "dp", size, bit)
        for place, r in enumerate(held):
            rows = block.shape[0]
            blocks[r ^ bit] = moved[place * rows : (place + 1) * rows]
    return blocks


def gather_dp(block, size):
    half = block.shape[0] // 2
    top = gather_path(block[:half], size, bits_of(size))
    low = gather_path(block[half:], size, bits_of(size)[::-1])
    parts = []
    for r in range(size):
        parts += [top[r], low[r]]
    return jnp.concatenate(parts, 0)


def scatter_path(blocks, size, bits):
    blocks = dict(blocks)
    for bit in bits:
        away = sorted(r for r in blocks if r & bit)
        rows = blocks[0].shape[0]
        sent = jnp.concatenate([blocks[r].astype(BF16) for r in away], 0)
        moved = swap(sent, "dp", size, bit)
        blocks = {
            r ^ bit: blocks[r ^ bit].astype(F32)
            + moved[place * rows : (place + 1) * rows].astype(F32)
            for place, r in enumerate(away)
        }
    return blocks[0]


def scatter_dp(partial, size):
    rows = partial.shape[0] // size
    half = rows // 2
    top = {r: partial[r * rows : r * rows + half] for r in range(size)}
    low = {r: partial[r * rows + half : (r + 1) * rows] for r in range(size)}
    return jnp.concatenate(
        [scatter_path(top, size, bits_of(size)), scatter_path(low, size, bits_of(size)[::-1])], 0
    )


def combine_all(value, sizes, join):
    for axis, size in sizes:
        for bit in bits_of(size):
            value = join(value, swap(value, axis, size, bit))
    return value


STEPS = 4
MESH_IDS = pl.DeviceIdType.MESH
PATHS = ((1, 2), (2, 1))


def flipped(axis, bit):
    me = lax.axis_index(axis)
    return {axis: me + bit - 2 * bit * ((me // bit) % 2)}


def neighbours(fsdp=1):
    near = {bit: flipped("dp", bit) for bit in (1, 2)}
    partners = [near[1], near[2]] + [flipped("fsdp", bit) for bit in bits_of(fsdp)]
    greeted = partners if fsdp > 1 else [near[1], near[2]]
    barrier = pltpu.get_barrier_semaphore()
    for where in greeted:
        pl.semaphore_signal(barrier, inc=1, device_id=where, device_id_type=MESH_IDS)
    pl.semaphore_wait(barrier, len(greeted))
    return near, partners


def remote(source, target, sems, index, where):
    return pltpu.make_async_remote_copy(
        src_ref=source, dst_ref=target, send_sem=sems.at[0, index], recv_sem=sems.at[1, index],
        device_id=where, device_id_type=MESH_IDS,
    )


def each_step(act):
    def run(step, carry):
        act(step)
        return carry

    lax.fori_loop(0, STEPS, run, 0)


class Gather:
    def __init__(self, out, sems, near):
        self.out, self.sems, self.near = out, sems, near
        self.rows = out.shape[0] // 4
        self.step_rows = self.rows // 2 // STEPS

    def span(self, block, path, step):
        start = block * self.rows + path * (self.rows // 2) + step * self.step_rows
        return pl.ds(pl.multiple_of(start, self.step_rows), self.step_rows)

    def copy(self, source, bit, path, step, kind):
        return remote(
            self.out.at[self.span(source, path, step)],
            self.out.at[self.span(source + bit, path, step)],
            self.sems, (path * 3 + kind) * STEPS + step, self.near[bit],
        )

    def send(self, path, step):
        first, second = PATHS[path]
        self.copy(0, first, path, step, 0).start()
        self.copy(0, second, path, step, 1).start()

    def forward(self, path, step):
        first, second = PATHS[path]
        self.copy(0, first, path, step, 0).wait_recv()
        self.copy(first, second, path, step, 2).start()

    def finish(self, path, step):
        first, second = PATHS[path]
        self.copy(0, first, path, step, 0).wait_send()
        self.copy(0, second, path, step, 1).wait()
        self.copy(first, second, path, step, 2).wait()


class Scatter:
    def __init__(self, partial, landing, passing, last, sems, near):
        self.partial, self.landing, self.passing, self.last = partial, landing, passing, last
        self.sems, self.near = sems, near
        self.rows = partial.shape[0] // 4
        self.step_rows = self.rows // 2 // STEPS

    def span(self, block, path, step):
        start = block * self.rows + path * (self.rows // 2) + step * self.step_rows
        return pl.ds(pl.multiple_of(start, self.step_rows), self.step_rows)

    def own(self, path, step):
        return self.span(0, path, step)

    def opening(self, path, step, kind):
        first, _ = PATHS[path]
        return remote(
            self.partial.at[self.span((first, 3)[kind], path, step)],
            self.landing.at[kind, self.own(path, step)],
            self.sems, (path * 3 + kind) * STEPS + step, self.near[first],
        )

    def closing(self, path, step):
        rows = self.own(path, step)
        return remote(
            self.passing.at[rows], self.last.at[rows], self.sems,
            (path * 3 + 2) * STEPS + step, self.near[PATHS[path][1]],
        )

    def begin(self, path, step):
        for kind in range(2):
            self.opening(path, step, kind).start()

    def relay(self, path, step):
        _, second = PATHS[path]
        self.opening(path, step, 1).wait_recv()
        rows = self.own(path, step)
        self.passing[rows] = (
            self.partial[self.span(second, path, step)].astype(F32)
            + self.landing[1, rows].astype(F32)
        ).astype(BF16)
        self.closing(path, step).start()

    def total(self, path, step):
        self.opening(path, step, 0).wait_recv()
        self.closing(path, step).wait_recv()
        rows = self.own(path, step)
        return (
            self.partial[self.span(0, path, step)].astype(F32)
            + self.landing[0, rows].astype(F32)
            + self.last[rows].astype(F32)
        )

    def finish(self, path, step):
        for kind in range(2):
            self.opening(path, step, kind).wait_send()
        self.closing(path, step).wait_send()


def row_norm(values):
    centred = values - jnp.mean(values, axis=-1, keepdims=True)
    inverse_std = lax.rsqrt(jnp.mean(centred * centred, axis=-1, keepdims=True) + EPS)
    return centred * inverse_std, inverse_std


def row_back(grad_norm, normed, inverse_std, gain):
    scaled = grad_norm * gain
    return inverse_std * (
        scaled
        - jnp.mean(scaled, axis=-1, keepdims=True)
        - normed * jnp.mean(scaled * normed, axis=-1, keepdims=True)
    )


def double_all(held, landing, sems, partners, join, stages=None):
    for stage in stages or range(len(partners)):
        where = partners[stage]
        copy = remote(held.at[stage], landing.at[stage], sems, stage, where)
        copy.start()
        copy.wait()
        held[stage + 1] = join(held[stage], landing[stage])


def gather_two_kernel(
    fsdp, one_ref, two_ref, table_ref, out_one, out_two, table_out, held, landing, sems, small_sems
):
    near, partners = neighbours(fsdp)
    jobs = []
    for k, (source, out) in enumerate(((one_ref, out_one), (two_ref, out_two))):
        out[: source.shape[0]] = source[...]
        jobs.append(Gather(out, sems.at[k], near))
    held[0] = table_ref[...]
    double_all(held, landing, small_sems, partners, jnp.add, range(2))
    for job in jobs:
        each_step(lambda step, job=job: [job.send(path, step) for path in range(2)])
    double_all(held, landing, small_sems, partners, jnp.add, range(2, len(partners)))
    table_out[...] = held[len(partners)]
    for job in jobs:
        each_step(lambda step, job=job: [job.forward(path, step) for path in range(2)])
    for job in jobs:
        each_step(lambda step, job=job: [job.finish(path, step) for path in range(2)])


def exchange(scatter, gather, rows_of, beside=None):
    each_step(lambda step: [scatter.begin(path, step) for path in range(2)])
    if beside is not None:
        beside()
    each_step(lambda step: [scatter.relay(path, step) for path in range(2)])

    def middle(step):
        for path in range(2):
            rows = scatter.own(path, step)
            gather.out[rows] = rows_of(rows, scatter.total(path, step))
            gather.send(path, step)

        @pl.when(step > 0)
        def _():
            for path in range(2):
                gather.forward(path, step - 1)

    each_step(middle)
    for path in range(2):
        gather.forward(path, STEPS - 1)
    each_step(lambda step: [scatter.finish(path, step) for path in range(2)])
    each_step(lambda step: [gather.finish(path, step) for path in range(2)])


def add_sums(sums_ref, values, start=0):
    for k, value in enumerate(values):
        row = start + k
        sums_ref[row : row + 1] += jnp.sum(value, axis=0, keepdims=True)


def hidden_kernel(
    partial_ref, tokens_ref, params_ref, out_ref, hidden_ref, landing, passing, last, sems
):
    near, _ = neighbours()

    def rows_of(rows, total):
        hidden = tokens_ref[rows].astype(F32) + total + params_ref[0:1]
        hidden_ref[rows] = hidden
        normed, _ = row_norm(hidden)
        return (normed * params_ref[1:2] + params_ref[2:3]).astype(BF16)

    exchange(
        Scatter(partial_ref, landing, passing, last, sems.at[0], near),
        Gather(out_ref, sems.at[1], near), rows_of,
    )


def branch_kernel(
    partial_ref, hidden_ref, cotangent_ref, params_ref, active_ref, weight_ref, out_ref, grad_ref,
    sums_ref, output_ref, landing, passing, last, active, weight, copy_sems, sems,
):
    copies = [
        pltpu.make_async_copy(active_ref, active, copy_sems.at[0]),
        pltpu.make_async_copy(weight_ref, weight, copy_sems.at[1]),
    ]
    for copy in copies:
        copy.start()
    near, _ = neighbours()
    sums_ref[...] = jnp.zeros_like(sums_ref)

    def rows_of(rows, total):
        normed, inverse_std = row_norm(hidden_ref[rows])
        upper = cotangent_ref[rows].astype(F32)
        grad = upper + row_back(total, normed, inverse_std, params_ref[1:2])
        grad_ref[rows] = grad
        branch = grad.astype(BF16)
        add_sums(sums_ref, (upper, total * normed, total, branch.astype(F32)))
        return branch

    def output_tile(tile, carry):
        columns = pl.ds(pl.multiple_of(tile * 256, 256), 256)
        output_ref[:, columns] = dot(active[...], weight[:, columns]).astype(BF16)
        return carry

    def beside():
        for copy in copies:
            copy.wait()
        lax.fori_loop(0, output_ref.shape[1] // 256, output_tile, 0)

    exchange(
        Scatter(partial_ref, landing, passing, last, sems.at[0], near),
        Gather(out_ref, sems.at[1], near), rows_of, beside,
    )


def sum_or_top(a, b):
    row = lax.broadcasted_iota(jnp.int32, a.shape, 0)
    return jnp.where(row < a.shape[0] - 1, a + b, jnp.maximum(a, b))


def last_kernel(
    fsdp, first_ref, output_ref, tokens_ref, hidden_ref, grad_ref, params_ref, small_ref,
    tokens_out, output_out, small_out, sums_out, landing, passing, last, held, small_landing,
    sums, sums_landing, sems, small_sems,
):
    near, partners = neighbours(fsdp)
    sums[0] = jnp.zeros_like(sums_out)
    first, second = (
        Scatter(ref, landing.at[k], passing.at[k], last.at[k], sems.at[k], near)
        for k, ref in enumerate((first_ref, output_ref))
    )

    def first_rows(path, step):
        rows = first.own(path, step)
        total = first.total(path, step)
        normed, inverse_std = row_norm(tokens_ref[rows].astype(F32))
        grad = grad_ref[rows] + row_back(total, normed, inverse_std, params_ref[0:1])
        tokens_out[rows] = grad.astype(BF16)
        add_sums(sums.at[0], (total * normed, total))

    def second_rows(path, step):
        rows = second.own(path, step)
        total = second.total(path, step)
        output_out[rows] = (hidden_ref[rows] + total + params_ref[1:2]).astype(BF16)

    held[0] = small_ref[...]
    for job in (first, second):
        each_step(lambda step, job=job: [job.begin(path, step) for path in range(2)])
    double_all(held, small_landing, small_sems.at[0], partners, sum_or_top)
    small_out[...] = held[len(partners)]
    for job in (first, second):
        each_step(lambda step, job=job: [job.relay(path, step) for path in range(2)])
    each_step(lambda step: [first_rows(path, step) for path in range(2)])
    double_all(sums, sums_landing, small_sems.at[1], partners, jnp.add)
    sums_out[...] = sums[len(partners)]
    each_step(lambda step: [second_rows(path, step) for path in range(2)])
    for job in (first, second):
        each_step(lambda step, job=job: [job.finish(path, step) for path in range(2)])


def call_exchange(kernel, number, jobs, scatters, outs, args, extra=(), stages=0, unplaced=0):
    rows, width = args[0].shape if scatters else (4 * args[0].shape[0], args[0].shape[1])
    own = rows // 4
    room = []
    if scatters == 1:
        room = [(2, own, width), (own, width), (own, width)]
    if scatters == 2:
        room = [(2, 2, own, width), (2, own, width), (2, own, width)]
    return pl.pallas_call(
        kernel,
        in_specs=[pl.BlockSpec(memory_space=pltpu.VMEM)] * (len(args) - unplaced)
        + [pl.BlockSpec(memory_space=pl.ANY)] * unplaced,
        out_specs=[pl.BlockSpec(memory_space=pltpu.VMEM)] * len(outs),
        out_shape=[jax.ShapeDtypeStruct(shape, dtype) for shape, dtype in outs],
        scratch_shapes=[
            *(pltpu.VMEM(shape, BF16) for shape in room),
            *extra,
            pltpu.SemaphoreType.DMA((jobs, 2, 6 * STEPS)),
            *([pltpu.SemaphoreType.DMA(stages)] if stages else []),
        ],
        compiler_params=pltpu.CompilerParams(
            collective_id=number, has_side_effects=True, vmem_limit_bytes=48 << 20
        ),
        cost_estimate=pl.CostEstimate(
            flops=rows * width, bytes_accessed=200 << 20, transcendentals=0
        ),
    )(*args)


def pair_span(offset, pair):
    return pl.ds(offset + pair * 2 * HEAD_DIM, 2 * HEAD_DIM)


def head_parts(ref, offset, pair):
    both = ref[:, pair_span(offset, pair)]
    return both[:, :HEAD_DIM], both[:, HEAD_DIM:]


def dot_nt(a, b):
    return lax.dot_general(a, b, (((1,), (1,)), ((), ())), preferred_element_type=F32)


def dot_tn(a, b):
    return lax.dot_general(a, b, (((0,), (0,)), ((), ())), preferred_element_type=F32)


def attend_kernel(slope_ref, distance_ref, qkv_ref, mixed_ref, top_ref):
    width = mixed_ref.shape[1]
    lane = lax.broadcasted_iota(jnp.int32, (8, 128), 1)

    distance = distance_ref[...]
    tops = jnp.zeros((8, 128), F32)
    for pair in range(width // HEAD_DIM // 2):
        outs = []
        for t, (q, k, v) in enumerate(
            zip(*(head_parts(qkv_ref, part * width, pair) for part in range(3)))
        ):
            logits = dot_nt(q * jnp.asarray(SCALE, BF16), k)
            head_top = jnp.max(jnp.where(distance < MASKED, logits, -1e30))
            tops = jnp.where(lane == pair * 2 + t, head_top, tops)
            scores = logits - slope_ref[pair * 2 + t] * distance
            expos = jnp.exp(scores - jnp.max(scores, axis=-1, keepdims=True))
            probs = expos * (1.0 / jnp.sum(expos, axis=-1, keepdims=True))
            outs.append(jnp.dot(probs.astype(BF16), v, preferred_element_type=F32))
        mixed_ref[:, pair_span(0, pair)] = jnp.concatenate(outs, 1).astype(BF16)
    top_ref[...] = tops


def attend_back_kernel(slope_ref, distance_ref, qkv_ref, grad_ref, out_ref):
    width = grad_ref.shape[1]

    distance = distance_ref[...]
    for pair in range(width // HEAD_DIM // 2):
        outs = ([], [], [])
        parts = [head_parts(qkv_ref, part * width, pair) for part in range(3)]
        parts.append(head_parts(grad_ref, 0, pair))
        for t, (q, k, v, grad) in enumerate(zip(*parts)):
            low_q = q * jnp.asarray(SCALE, BF16)
            scores = dot_nt(low_q, k) - slope_ref[pair * 2 + t] * distance
            expos = jnp.exp(scores - jnp.max(scores, axis=-1, keepdims=True))
            probs = expos * (1.0 / jnp.sum(expos, axis=-1, keepdims=True))
            outs[2].append(dot_tn(probs.astype(BF16), grad))
            grad_probs = dot_nt(grad, v)
            inner = jnp.sum(grad_probs * probs, axis=-1, keepdims=True)
            grad_scores = (probs * (grad_probs - inner)).astype(BF16)
            outs[0].append(jnp.dot(grad_scores, k, preferred_element_type=F32) * SCALE)
            outs[1].append(dot_tn(grad_scores, low_q))
        for part in range(3):
            out_ref[:, pair_span(part * width, pair)] = jnp.concatenate(outs[part], 1).astype(BF16)


def attend(slopes, distance, qkv, length):
    rows, width = qkv.shape[0], qkv.shape[1] // 3
    blocks = rows // length
    mixed, tops = pl.pallas_call(
        attend_kernel,
        grid=(blocks,),
        in_specs=[
            pl.BlockSpec(memory_space=pltpu.SMEM),
            pl.BlockSpec((length, length), lambda b: (0, 0)),
            pl.BlockSpec((length, 3 * width), lambda b: (b, 0)),
        ],
        out_specs=[
            pl.BlockSpec((length, width), lambda b: (b, 0)),
            pl.BlockSpec((8, 128), lambda b: (b, 0)),
        ],
        out_shape=[
            jax.ShapeDtypeStruct((rows, width), BF16),
            jax.ShapeDtypeStruct((blocks * 8, 128), F32),
        ],
        cost_estimate=pl.CostEstimate(
            flops=4 * rows * length * width, bytes_accessed=8 * rows * width,
            transcendentals=rows * length * width // HEAD_DIM,
        ),
        name="attend",
    )(slopes, distance, qkv)
    return mixed, jnp.max(tops, axis=0)[: width // HEAD_DIM]


def attend_back(slopes, distance, qkv, grad, length):
    rows, width = grad.shape
    return pl.pallas_call(
        attend_back_kernel,
        grid=(rows // length,),
        in_specs=[
            pl.BlockSpec(memory_space=pltpu.SMEM),
            pl.BlockSpec((length, length), lambda b: (0, 0)),
            pl.BlockSpec((length, 3 * width), lambda b: (b, 0)),
            pl.BlockSpec((length, width), lambda b: (b, 0)),
        ],
        out_specs=pl.BlockSpec((length, 3 * width), lambda b: (b, 0)),
        out_shape=jax.ShapeDtypeStruct((rows, 3 * width), BF16),
        cost_estimate=pl.CostEstimate(
            flops=10 * rows * length * width, bytes_accessed=14 * rows * width,
            transcendentals=rows * length * width // HEAD_DIM,
        ),
        name="attend_back",
    )(slopes, distance, qkv, grad)


def norm_stats(values):
    row_mean = jnp.mean(values, axis=-1, keepdims=True)
    centred = values - row_mean
    inverse_std = lax.rsqrt(jnp.mean(centred * centred, axis=-1, keepdims=True) + EPS)
    return centred * inverse_std, inverse_std


def norm_back(grad_norm, normed, inverse_std, gain):
    scaled = grad_norm * gain
    return inverse_std * (
        scaled
        - jnp.mean(scaled, axis=-1, keepdims=True)
        - normed * jnp.mean(scaled * normed, axis=-1, keepdims=True)
    )


def dot(a, b):
    return jnp.dot(a, b, preferred_element_type=F32)


def layer(
    dp, fsdp, tokens, seq_lengths, w_qkv, bias_q, bias_v, w_out, bias_out, ln1_gain, ln1_bias,
    w_up, bias_up, w_down, bias_down, ln2_gain, ln2_bias, cotangent,
):
    length, width = tokens.shape
    shard = w_qkv.shape[0]
    ff = w_up.shape[1]
    heads = width // HEAD_DIM
    part, ff_part = width // dp, ff // dp
    local_heads = heads // dp
    spot, place = lax.axis_index("dp"), lax.axis_index("fsdp")
    rank = spot * fsdp + place
    both = (("fsdp", fsdp), ("dp", dp))

    out_w = lax.all_gather(w_out, "fsdp", axis=0, tiled=True)
    cols = w_qkv.reshape(shard, 3, dp, part).transpose(0, 2, 1, 3).reshape(shard, 3 * width)
    cols = lax.all_to_all(cols, "dp", 1, 0, tiled=True).reshape(dp, shard, 3 * part)
    qkv_w = lax.all_gather(cols, "fsdp", axis=1, tiled=True).reshape(width, 3 * part)
    w_up, cols = lax.optimization_barrier((w_up, cols))
    ups = lax.all_to_all(w_up, "dp", 1, 0, tiled=True).reshape(dp, shard, ff_part)
    up_w = lax.all_gather(ups, "fsdp", axis=1, tiled=True).reshape(width, ff_part)
    down_w = lax.all_gather(w_down, "fsdp", axis=0, tiled=True)
    late_tokens, _ = lax.optimization_barrier((tokens, ups))

    full_small = (bias_out, ln1_gain, ln1_bias, bias_down, ln2_gain, ln2_bias)
    row = jnp.concatenate(full_small + (bias_q, bias_v, bias_up))[None]
    table = jnp.zeros((dp * fsdp, row.shape[1]), BF16)
    table = lax.dynamic_update_slice(table, row, (rank, 0))
    wide = (4 * length, width)
    narrow = (length, width)
    kernels = dp == 4 and length % (32 * STEPS) == 0 and ff == dp * width
    stages = len(bits_of(fsdp)) + 2
    if kernels:
        all_tokens, grad_y, table = call_exchange(
            functools.partial(gather_two_kernel, fsdp), 1, 2, 0,
            [(wide, BF16), (wide, BF16), (table.shape, BF16)], [late_tokens, cotangent, table],
            (pltpu.VMEM((stages + 1,) + table.shape, BF16), pltpu.VMEM((stages,) + table.shape, BF16)),
            (2, stages),
        )
    else:
        all_tokens, grad_y = gather_dp(late_tokens, dp), gather_dp(cotangent, dp)
        table = combine_all(table, both, jnp.add)
    table = table.astype(F32)
    small = [table[:, k * shard : (k + 1) * shard].reshape(1, width) for k in range(6)]
    out_b, gain1, shift1, down_b, gain2, shift2 = small
    mine = lax.dynamic_slice(table, (spot * fsdp, 0), (fsdp, row.shape[1]))[:, 6 * shard :]
    q_b, v_b = mine[:, :shard].reshape(1, part), mine[:, shard : 2 * shard].reshape(1, part)
    up_b = mine[:, 2 * shard :].reshape(1, ff_part)

    ranks = (spot * local_heads + 1 + jnp.arange(local_heads)).astype(F32)
    slopes = jnp.exp2(-8.0 * ranks / heads) * SCALE
    places = jnp.arange(length, dtype=jnp.int32)
    gap = places[:, None] - places[None, :]
    distance = jnp.where(gap >= 0, gap.astype(F32), MASKED)

    inputs = tokens.astype(F32)
    normed_all, _ = norm_stats(all_tokens.astype(F32))
    first_in = (normed_all * gain1 + shift1).astype(BF16)
    biases = jnp.concatenate([q_b, jnp.zeros_like(q_b), v_b], 1)
    qkv = (dot(first_in, qkv_w) + biases).astype(BF16)
    mixed, tops = attend(slopes, distance, qkv, length)
    out_part = dot(mixed, out_w).astype(BF16)
    if kernels:
        second_in, hidden = call_exchange(
            hidden_kernel, 2, 2, 1, [(wide, BF16), (narrow, F32)],
            [out_part, tokens, jnp.concatenate([out_b, gain2, shift2], 0)],
        )
    else:
        hidden = inputs + scatter_dp(out_part, dp) + out_b
        normed2, inverse2 = norm_stats(hidden)
        second_in = gather_dp((normed2 * gain2 + shift2).astype(BF16), dp)

    upward = dot(second_in, up_w) + up_b
    cumulative = 0.5 * (1.0 + lax.erf(upward * (0.5**0.5)))
    active = (upward * cumulative).astype(BF16)
    slope = cumulative + upward * jnp.exp(-0.5 * upward * upward) * ((0.5 / jnp.pi) ** 0.5)
    active, slope = lax.optimization_barrier((active, slope.astype(BF16)))

    def reduce_rows(grad):
        return lax.psum_scatter(grad, "fsdp", scatter_dimension=0, tiled=True).astype(F32)

    def reduce_columns(grad):
        grad = grad.reshape(dp, fsdp * shard, grad.shape[1])
        return lax.psum_scatter(grad, "fsdp", scatter_dimension=1, tiled=True)

    def exchange_columns(grad):
        return lax.all_to_all(
            grad.reshape(dp * shard, grad.shape[2]), "dp", 0, 1, tiled=True
        ).astype(F32)

    local_down = dot_tn(active, grad_y).astype(BF16)
    late_y, slope, _ = lax.optimization_barrier((grad_y, slope, local_down))
    grad_upward = (dot_nt(late_y, down_w) * slope).astype(BF16)
    grad_w_down = reduce_rows(local_down)
    local_up = dot_tn(second_in, grad_upward).astype(BF16)
    late_upward, _ = lax.optimization_barrier((grad_upward, local_up))
    second_part = dot_nt(late_upward, up_w).astype(BF16)
    scattered_up = reduce_columns(local_up)
    if kernels:
        branch_all, grad_hidden, branch_sums, output_part = call_exchange(
            branch_kernel, 3, 2, 1,
            [(wide, BF16), (narrow, F32), ((8, width), F32), (wide, BF16)],
            [second_part, hidden, cotangent, jnp.concatenate([out_b, gain2], 0), active, down_w],
            (pltpu.VMEM(active.shape, BF16), pltpu.VMEM(down_w.shape, BF16),
             pltpu.SemaphoreType.DMA((2,))),
            unplaced=2,
        )
    else:
        grad_second = scatter_dp(second_part, dp)
        grad_hidden = cotangent.astype(F32) + norm_back(grad_second, normed2, inverse2, gain2)
        grad_branch = grad_hidden.astype(BF16)
        branch_all = gather_dp(grad_branch, dp)
        branch_sums = jnp.stack([
            jnp.sum(piece, axis=0)
            for piece in (
                cotangent.astype(F32), grad_second * normed2, grad_second,
                grad_branch.astype(F32),
            )
        ])

    grad_mixed = dot_nt(branch_all, out_w).astype(BF16)
    grad_proj = attend_back(slopes, distance, qkv, grad_mixed, length)
    local_qkv = dot_tn(first_in, grad_proj).astype(BF16)
    late_branch, late_proj, _ = lax.optimization_barrier((branch_all, grad_proj, local_qkv))
    grad_w_qkv = exchange_columns(reduce_columns(local_qkv))
    grad_w_qkv = (
        grad_w_qkv.reshape(shard, dp, 3, part).transpose(0, 2, 1, 3).reshape(shard, 3 * width)
    )
    local_out = dot_tn(mixed, late_branch).astype(BF16)
    grad_w_out = reduce_rows(local_out)
    first_part = dot_nt(late_proj, qkv_w).astype(BF16)
    if not kernels:
        output_part = dot(active, down_w).astype(BF16)

    def spread(piece, size, fill=0.0):
        return lax.dynamic_update_slice(
            jnp.full((size,), fill, F32), piece, (spot * piece.shape[0],)
        )

    up_sum = jnp.sum(grad_upward.astype(F32), axis=0)
    q_sum = jnp.sum(grad_proj[:, :part].astype(F32), axis=0)
    v_sum = jnp.sum(grad_proj[:, 2 * part :].astype(F32), axis=0)
    small = jnp.concatenate([
        branch_sums[:4].reshape(4 * width), spread(up_sum, ff), spread(q_sum, width),
        spread(v_sum, width), jnp.zeros((5 * width,), F32), spread(tops, width, -1e30),
    ]).reshape(-1, width)
    if kernels:
        first_part, scattered_up = lax.optimization_barrier((first_part, scattered_up))
        sums = (8, width)
        grad_tokens, output, small, sums = call_exchange(
            functools.partial(last_kernel, fsdp), 4, 2, 2,
            [(narrow, BF16), (narrow, BF16), (small.shape, F32), (sums, F32)],
            [first_part, output_part, tokens, hidden, grad_hidden,
             jnp.concatenate([gain1, down_b], 0), small],
            (pltpu.VMEM((stages + 1,) + small.shape, F32),
             pltpu.VMEM((stages,) + small.shape, F32),
             pltpu.VMEM((stages + 1,) + sums, F32), pltpu.VMEM((stages,) + sums, F32)),
            (2, 2, stages),
        )
        sums = sums[:2]
    else:
        grad_first = scatter_dp(first_part, dp)
        normed1, inverse1 = norm_stats(inputs)
        grad_tokens = grad_hidden + norm_back(grad_first, normed1, inverse1, gain1)
        output = hidden + scatter_dp(output_part, dp) + down_b
        sums = jnp.stack([jnp.sum(grad_first * normed1, axis=0), jnp.sum(grad_first, axis=0)])
        small = combine_all(small, both, sum_or_top)
        sums = combine_all(sums, both, jnp.add)
    grad_w_up = exchange_columns(scattered_up)
    ups_at = 4 + ff // width
    owned = lax.dynamic_slice(small, (0, rank * shard), (small.shape[0], shard))
    owned_late = lax.dynamic_slice(sums, (0, rank * shard), (2, shard))
    ff_shard = ff // (dp * fsdp)
    owned_up = lax.dynamic_slice(
        small[4:ups_at].reshape(ff), (rank * ff_shard,), (ff_shard,)
    )

    head_top = small[-1, :heads]
    factor = jnp.sqrt(CLIP_TAU / jnp.maximum(head_top, CLIP_TAU))
    column = jnp.repeat(factor, HEAD_DIM)
    columns = jnp.concatenate([column, column, jnp.ones((width,), F32)])
    clipped = (w_qkv.astype(F32) * columns[None, :]).astype(BF16)
    return (
        output.astype(BF16),
        grad_tokens.astype(BF16),
        grad_w_qkv,
        owned[ups_at],
        owned[ups_at + 1],
        grad_w_out,
        owned[3],
        owned_late[0],
        owned_late[1],
        grad_w_up,
        owned_up,
        grad_w_down,
        owned[0],
        owned[1],
        owned[2],
        clipped,
    )


def solution(mesh):
    rows, flat = P(("dp", "fsdp"), None), P(("dp", "fsdp"))
    return jax.shard_map(
        functools.partial(layer, mesh.shape["dp"], mesh.shape["fsdp"]),
        mesh=mesh,
        in_specs=(
            rows, flat, rows, flat, flat, rows, flat, flat, flat, rows, flat, rows, flat, flat,
            flat, rows,
        ),
        out_specs=(
            rows, rows, rows, flat, flat, rows, flat, flat, flat, rows, flat, rows, flat, flat,
            flat, rows,
        ),
        check_vma=False,
    )
```

```python
import functools

import jax
import jax.numpy as jnp
from jax import lax
from jax.experimental import pallas as pl
from jax.experimental.pallas import tpu as pltpu
from jax.sharding import PartitionSpec as P


HEAD_DIM = 64
EPS = 1e-05
CLIP_TAU = 5.0
MASKED = 1e35
F32 = jnp.float32
BF16 = jnp.bfloat16
SCALE = HEAD_DIM ** (-0.5)


def swap(value, axis, size, bit):
    return lax.ppermute(value, axis, [(i, i ^ bit) for i in range(size)])


def bits_of(size):
    return [1 << b for b in range(size.bit_length() - 1)]


def gather_path(block, size, bits):
    blocks = {0: block}
    for bit in bits:
        held = sorted(blocks)
        moved = swap(jnp.concatenate([blocks[r] for r in held], 0), "dp", size, bit)
        for place, r in enumerate(held):
            rows = block.shape[0]
            blocks[r ^ bit] = moved[place * rows : (place + 1) * rows]
    return blocks


def gather_dp(block, size):
    half = block.shape[0] // 2
    top = gather_path(block[:half], size, bits_of(size))
    low = gather_path(block[half:], size, bits_of(size)[::-1])
    parts = []
    for r in range(size):
        parts += [top[r], low[r]]
    return jnp.concatenate(parts, 0)


def scatter_path(blocks, size, bits):
    blocks = dict(blocks)
    for bit in bits:
        away = sorted(r for r in blocks if r & bit)
        rows = blocks[0].shape[0]
        sent = jnp.concatenate([blocks[r].astype(BF16) for r in away], 0)
        moved = swap(sent, "dp", size, bit)
        blocks = {
            r ^ bit: blocks[r ^ bit].astype(F32)
            + moved[place * rows : (place + 1) * rows].astype(F32)
            for place, r in enumerate(away)
        }
    return blocks[0]


def scatter_dp(partial, size):
    rows = partial.shape[0] // size
    half = rows // 2
    top = {r: partial[r * rows : r * rows + half] for r in range(size)}
    low = {r: partial[r * rows + half : (r + 1) * rows] for r in range(size)}
    return jnp.concatenate(
        [scatter_path(top, size, bits_of(size)), scatter_path(low, size, bits_of(size)[::-1])], 0
    )


def combine_all(value, sizes, join):
    for axis, size in sizes:
        for bit in bits_of(size):
            value = join(value, swap(value, axis, size, bit))
    return value


STEPS = 4
MESH_IDS = pl.DeviceIdType.MESH
PATHS = ((1, 2), (2, 1))


def flipped(axis, bit):
    me = lax.axis_index(axis)
    return {axis: me + bit - 2 * bit * ((me // bit) % 2)}


def neighbours(fsdp=1):
    near = {bit: flipped("dp", bit) for bit in (1, 2)}
    partners = [near[1], near[2]] + [flipped("fsdp", bit) for bit in bits_of(fsdp)]
    greeted = partners if fsdp > 1 else [near[1], near[2]]
    barrier = pltpu.get_barrier_semaphore()
    for where in greeted:
        pl.semaphore_signal(barrier, inc=1, device_id=where, device_id_type=MESH_IDS)
    pl.semaphore_wait(barrier, len(greeted))
    return near, partners


def remote(source, target, sems, index, where):
    return pltpu.make_async_remote_copy(
        src_ref=source, dst_ref=target, send_sem=sems.at[0, index], recv_sem=sems.at[1, index],
        device_id=where, device_id_type=MESH_IDS,
    )


def each_step(act):
    def run(step, carry):
        act(step)
        return carry

    lax.fori_loop(0, STEPS, run, 0)


class Gather:
    def __init__(self, out, sems, near):
        self.out, self.sems, self.near = out, sems, near
        self.rows = out.shape[0] // 4
        self.step_rows = self.rows // 2 // STEPS

    def span(self, block, path, step):
        start = block * self.rows + path * (self.rows // 2) + step * self.step_rows
        return pl.ds(pl.multiple_of(start, self.step_rows), self.step_rows)

    def copy(self, source, bit, path, step, kind):
        return remote(
            self.out.at[self.span(source, path, step)],
            self.out.at[self.span(source + bit, path, step)],
            self.sems, (path * 3 + kind) * STEPS + step, self.near[bit],
        )

    def send(self, path, step):
        first, second = PATHS[path]
        self.copy(0, first, path, step, 0).start()
        self.copy(0, second, path, step, 1).start()

    def forward(self, path, step):
        first, second = PATHS[path]
        self.copy(0, first, path, step, 0).wait_recv()
        self.copy(first, second, path, step, 2).start()

    def finish(self, path, step):
        first, second = PATHS[path]
        self.copy(0, first, path, step, 0).wait_send()
        self.copy(0, second, path, step, 1).wait()
        self.copy(first, second, path, step, 2).wait()


class Scatter:
    def __init__(self, partial, landing, passing, last, sems, near):
        self.partial, self.landing, self.passing, self.last = partial, landing, passing, last
        self.sems, self.near = sems, near
        self.rows = partial.shape[0] // 4
        self.step_rows = self.rows // 2 // STEPS

    def span(self, block, path, step):
        start = block * self.rows + path * (self.rows // 2) + step * self.step_rows
        return pl.ds(pl.multiple_of(start, self.step_rows), self.step_rows)

    def own(self, path, step):
        return self.span(0, path, step)

    def opening(self, path, step, kind):
        first, _ = PATHS[path]
        return remote(
            self.partial.at[self.span((first, 3)[kind], path, step)],
            self.landing.at[kind, self.own(path, step)],
            self.sems, (path * 3 + kind) * STEPS + step, self.near[first],
        )

    def closing(self, path, step):
        rows = self.own(path, step)
        return remote(
            self.passing.at[rows], self.last.at[rows], self.sems,
            (path * 3 + 2) * STEPS + step, self.near[PATHS[path][1]],
        )

    def begin(self, path, step):
        for kind in range(2):
            self.opening(path, step, kind).start()

    def relay(self, path, step):
        _, second = PATHS[path]
        self.opening(path, step, 1).wait_recv()
        rows = self.own(path, step)
        self.passing[rows] = (
            self.partial[self.span(second, path, step)].astype(F32)
            + self.landing[1, rows].astype(F32)
        ).astype(BF16)
        self.closing(path, step).start()

    def total(self, path, step):
        self.opening(path, step, 0).wait_recv()
        self.closing(path, step).wait_recv()
        rows = self.own(path, step)
        return (
            self.partial[self.span(0, path, step)].astype(F32)
            + self.landing[0, rows].astype(F32)
            + self.last[rows].astype(F32)
        )

    def finish(self, path, step):
        for kind in range(2):
            self.opening(path, step, kind).wait_send()
        self.closing(path, step).wait_send()


def row_norm(values):
    centred = values - jnp.mean(values, axis=-1, keepdims=True)
    inverse_std = lax.rsqrt(jnp.mean(centred * centred, axis=-1, keepdims=True) + EPS)
    return centred * inverse_std, inverse_std


def row_back(grad_norm, normed, inverse_std, gain):
    scaled = grad_norm * gain
    return inverse_std * (
        scaled
        - jnp.mean(scaled, axis=-1, keepdims=True)
        - normed * jnp.mean(scaled * normed, axis=-1, keepdims=True)
    )


def double_all(held, landing, sems, partners, join, stages=None):
    for stage in stages or range(len(partners)):
        where = partners[stage]
        copy = remote(held.at[stage], landing.at[stage], sems, stage, where)
        copy.start()
        copy.wait()
        held[stage + 1] = join(held[stage], landing[stage])


def gather_two_kernel(
    fsdp, one_ref, two_ref, table_ref, out_one, out_two, table_out, held, landing, sems, small_sems
):
    near, partners = neighbours(fsdp)
    jobs = []
    for k, (source, out) in enumerate(((one_ref, out_one), (two_ref, out_two))):
        out[: source.shape[0]] = source[...]
        jobs.append(Gather(out, sems.at[k], near))
    held[0] = table_ref[...]
    double_all(held, landing, small_sems, partners, jnp.add, range(2))
    for job in jobs:
        each_step(lambda step, job=job: [job.send(path, step) for path in range(2)])
    double_all(held, landing, small_sems, partners, jnp.add, range(2, len(partners)))
    table_out[...] = held[len(partners)]
    for job in jobs:
        each_step(lambda step, job=job: [job.forward(path, step) for path in range(2)])
    for job in jobs:
        each_step(lambda step, job=job: [job.finish(path, step) for path in range(2)])


def exchange(scatter, gather, rows_of, beside=None):
    each_step(lambda step: [scatter.begin(path, step) for path in range(2)])
    if beside is not None:
        beside()
    each_step(lambda step: [scatter.relay(path, step) for path in range(2)])

    def middle(step):
        for path in range(2):
            rows = scatter.own(path, step)
            gather.out[rows] = rows_of(rows, scatter.total(path, step))
            gather.send(path, step)

        @pl.when(step > 0)
        def _():
            for path in range(2):
                gather.forward(path, step - 1)

    each_step(middle)
    for path in range(2):
        gather.forward(path, STEPS - 1)
    each_step(lambda step: [scatter.finish(path, step) for path in range(2)])
    each_step(lambda step: [gather.finish(path, step) for path in range(2)])


def add_sums(sums_ref, values, start=0):
    for k, value in enumerate(values):
        row = start + k
        sums_ref[row : row + 1] += jnp.sum(value, axis=0, keepdims=True)


def hidden_kernel(
    partial_ref, tokens_ref, params_ref, out_ref, hidden_ref, landing, passing, last, sems
):
    near, _ = neighbours()

    def rows_of(rows, total):
        hidden = tokens_ref[rows].astype(F32) + total + params_ref[0:1]
        hidden_ref[rows] = hidden
        normed, _ = row_norm(hidden)
        return (normed * params_ref[1:2] + params_ref[2:3]).astype(BF16)

    exchange(
        Scatter(partial_ref, landing, passing, last, sems.at[0], near),
        Gather(out_ref, sems.at[1], near), rows_of,
    )


def branch_kernel(
    partial_ref, hidden_ref, cotangent_ref, params_ref, active_ref, weight_ref, out_ref, grad_ref,
    sums_ref, output_ref, landing, passing, last, active, weight, copy_sems, sems,
):
    copies = [
        pltpu.make_async_copy(active_ref, active, copy_sems.at[0]),
        pltpu.make_async_copy(weight_ref, weight, copy_sems.at[1]),
    ]
    for copy in copies:
        copy.start()
    near, _ = neighbours()
    sums_ref[...] = jnp.zeros_like(sums_ref)

    def rows_of(rows, total):
        normed, inverse_std = row_norm(hidden_ref[rows])
        upper = cotangent_ref[rows].astype(F32)
        grad = upper + row_back(total, normed, inverse_std, params_ref[1:2])
        grad_ref[rows] = grad
        branch = grad.astype(BF16)
        add_sums(sums_ref, (upper, total * normed, total, branch.astype(F32)))
        return branch

    def output_tile(tile, carry):
        columns = pl.ds(pl.multiple_of(tile * 256, 256), 256)
        output_ref[:, columns] = dot(active[...], weight[:, columns]).astype(BF16)
        return carry

    def beside():
        for copy in copies:
            copy.wait()
        lax.fori_loop(0, output_ref.shape[1] // 256, output_tile, 0)

    exchange(
        Scatter(partial_ref, landing, passing, last, sems.at[0], near),
        Gather(out_ref, sems.at[1], near), rows_of, beside,
    )


def sum_or_top(a, b):
    row = lax.broadcasted_iota(jnp.int32, a.shape, 0)
    return jnp.where(row < a.shape[0] - 1, a + b, jnp.maximum(a, b))


def last_kernel(
    first_ref, output_ref, tokens_ref, hidden_ref, grad_ref, params_ref, tokens_out, output_out,
    sums_out, landing, passing, last, sems,
):
    near, _ = neighbours()
    sums_out[...] = jnp.zeros_like(sums_out)
    first, second = (
        Scatter(ref, landing.at[k], passing.at[k], last.at[k], sems.at[k], near)
        for k, ref in enumerate((first_ref, output_ref))
    )

    def first_rows(path, step):
        rows = first.own(path, step)
        total = first.total(path, step)
        normed, inverse_std = row_norm(tokens_ref[rows].astype(F32))
        grad = grad_ref[rows] + row_back(total, normed, inverse_std, params_ref[0:1])
        tokens_out[rows] = grad.astype(BF16)
        add_sums(sums_out, (total * normed, total))

    def second_rows(path, step):
        rows = second.own(path, step)
        total = second.total(path, step)
        output_out[rows] = (hidden_ref[rows] + total + params_ref[1:2]).astype(BF16)

    for job in (first, second):
        each_step(lambda step, job=job: [job.begin(path, step) for path in range(2)])
    for job in (first, second):
        each_step(lambda step, job=job: [job.relay(path, step) for path in range(2)])
    each_step(lambda step: [first_rows(path, step) for path in range(2)])
    each_step(lambda step: [second_rows(path, step) for path in range(2)])
    for job in (first, second):
        each_step(lambda step, job=job: [job.finish(path, step) for path in range(2)])


def call_exchange(kernel, number, jobs, scatters, outs, args, extra=(), stages=0, unplaced=0):
    rows, width = args[0].shape if scatters else (4 * args[0].shape[0], args[0].shape[1])
    own = rows // 4
    room = []
    if scatters == 1:
        room = [(2, own, width), (own, width), (own, width)]
    if scatters == 2:
        room = [(2, 2, own, width), (2, own, width), (2, own, width)]
    return pl.pallas_call(
        kernel,
        in_specs=[pl.BlockSpec(memory_space=pltpu.VMEM)] * (len(args) - unplaced)
        + [pl.BlockSpec(memory_space=pl.ANY)] * unplaced,
        out_specs=[pl.BlockSpec(memory_space=pltpu.VMEM)] * len(outs),
        out_shape=[jax.ShapeDtypeStruct(shape, dtype) for shape, dtype in outs],
        scratch_shapes=[
            *(pltpu.VMEM(shape, BF16) for shape in room),
            *extra,
            pltpu.SemaphoreType.DMA((jobs, 2, 6 * STEPS)),
            *([pltpu.SemaphoreType.DMA(stages)] if stages else []),
        ],
        compiler_params=pltpu.CompilerParams(
            collective_id=number, has_side_effects=True, vmem_limit_bytes=48 << 20
        ),
        cost_estimate=pl.CostEstimate(
            flops=rows * width, bytes_accessed=200 << 20, transcendentals=0
        ),
    )(*args)


def pair_span(offset, pair):
    return pl.ds(offset + pair * 2 * HEAD_DIM, 2 * HEAD_DIM)


def head_parts(ref, offset, pair):
    both = ref[:, pair_span(offset, pair)]
    return both[:, :HEAD_DIM], both[:, HEAD_DIM:]


def dot_nt(a, b):
    return lax.dot_general(a, b, (((1,), (1,)), ((), ())), preferred_element_type=F32)


def dot_tn(a, b):
    return lax.dot_general(a, b, (((0,), (0,)), ((), ())), preferred_element_type=F32)


def attend_kernel(slope_ref, distance_ref, qkv_ref, mixed_ref, top_ref):
    width = mixed_ref.shape[1]
    lane = lax.broadcasted_iota(jnp.int32, (8, 128), 1)

    distance = distance_ref[...]
    tops = jnp.zeros((8, 128), F32)
    for pair in range(width // HEAD_DIM // 2):
        outs = []
        for t, (q, k, v) in enumerate(
            zip(*(head_parts(qkv_ref, part * width, pair) for part in range(3)))
        ):
            logits = dot_nt(q * jnp.asarray(SCALE, BF16), k)
            head_top = jnp.max(jnp.where(distance < MASKED, logits, -1e30))
            tops = jnp.where(lane == pair * 2 + t, head_top, tops)
            scores = logits - slope_ref[pair * 2 + t] * distance
            expos = jnp.exp(scores - jnp.max(scores, axis=-1, keepdims=True))
            probs = expos * (1.0 / jnp.sum(expos, axis=-1, keepdims=True))
            outs.append(jnp.dot(probs.astype(BF16), v, preferred_element_type=F32))
        mixed_ref[:, pair_span(0, pair)] = jnp.concatenate(outs, 1).astype(BF16)
    top_ref[...] = tops


def attend_back_kernel(slope_ref, distance_ref, qkv_ref, grad_ref, out_ref):
    width = grad_ref.shape[1]

    distance = distance_ref[...]
    for pair in range(width // HEAD_DIM // 2):
        outs = ([], [], [])
        parts = [head_parts(qkv_ref, part * width, pair) for part in range(3)]
        parts.append(head_parts(grad_ref, 0, pair))
        for t, (q, k, v, grad) in enumerate(zip(*parts)):
            low_q = q * jnp.asarray(SCALE, BF16)
            scores = dot_nt(low_q, k) - slope_ref[pair * 2 + t] * distance
            expos = jnp.exp(scores - jnp.max(scores, axis=-1, keepdims=True))
            probs = expos * (1.0 / jnp.sum(expos, axis=-1, keepdims=True))
            outs[2].append(dot_tn(probs.astype(BF16), grad))
            grad_probs = dot_nt(grad, v)
            inner = jnp.sum(grad_probs * probs, axis=-1, keepdims=True)
            grad_scores = (probs * (grad_probs - inner)).astype(BF16)
            outs[0].append(jnp.dot(grad_scores, k, preferred_element_type=F32) * SCALE)
            outs[1].append(dot_tn(grad_scores, low_q))
        for part in range(3):
            out_ref[:, pair_span(part * width, pair)] = jnp.concatenate(outs[part], 1).astype(BF16)


def attend(slopes, distance, qkv, length):
    rows, width = qkv.shape[0], qkv.shape[1] // 3
    blocks = rows // length
    mixed, tops = pl.pallas_call(
        attend_kernel,
        grid=(blocks,),
        in_specs=[
            pl.BlockSpec(memory_space=pltpu.SMEM),
            pl.BlockSpec((length, length), lambda b: (0, 0)),
            pl.BlockSpec((length, 3 * width), lambda b: (b, 0)),
        ],
        out_specs=[
            pl.BlockSpec((length, width), lambda b: (b, 0)),
            pl.BlockSpec((8, 128), lambda b: (b, 0)),
        ],
        out_shape=[
            jax.ShapeDtypeStruct((rows, width), BF16),
            jax.ShapeDtypeStruct((blocks * 8, 128), F32),
        ],
        cost_estimate=pl.CostEstimate(
            flops=4 * rows * length * width, bytes_accessed=8 * rows * width,
            transcendentals=rows * length * width // HEAD_DIM,
        ),
        name="attend",
    )(slopes, distance, qkv)
    return mixed, jnp.max(tops, axis=0)[: width // HEAD_DIM]


def attend_back(slopes, distance, qkv, grad, length):
    rows, width = grad.shape
    return pl.pallas_call(
        attend_back_kernel,
        grid=(rows // length,),
        in_specs=[
            pl.BlockSpec(memory_space=pltpu.SMEM),
            pl.BlockSpec((length, length), lambda b: (0, 0)),
            pl.BlockSpec((length, 3 * width), lambda b: (b, 0)),
            pl.BlockSpec((length, width), lambda b: (b, 0)),
        ],
        out_specs=pl.BlockSpec((length, 3 * width), lambda b: (b, 0)),
        out_shape=jax.ShapeDtypeStruct((rows, 3 * width), BF16),
        cost_estimate=pl.CostEstimate(
            flops=10 * rows * length * width, bytes_accessed=14 * rows * width,
            transcendentals=rows * length * width // HEAD_DIM,
        ),
        name="attend_back",
    )(slopes, distance, qkv, grad)


def norm_stats(values):
    row_mean = jnp.mean(values, axis=-1, keepdims=True)
    centred = values - row_mean
    inverse_std = lax.rsqrt(jnp.mean(centred * centred, axis=-1, keepdims=True) + EPS)
    return centred * inverse_std, inverse_std


def norm_back(grad_norm, normed, inverse_std, gain):
    scaled = grad_norm * gain
    return inverse_std * (
        scaled
        - jnp.mean(scaled, axis=-1, keepdims=True)
        - normed * jnp.mean(scaled * normed, axis=-1, keepdims=True)
    )


def dot(a, b):
    return jnp.dot(a, b, preferred_element_type=F32)


def layer(
    dp, fsdp, tokens, seq_lengths, w_qkv, bias_q, bias_v, w_out, bias_out, ln1_gain, ln1_bias,
    w_up, bias_up, w_down, bias_down, ln2_gain, ln2_bias, cotangent,
):
    length, width = tokens.shape
    shard = w_qkv.shape[0]
    ff = w_up.shape[1]
    heads = width // HEAD_DIM
    part, ff_part = width // dp, ff // dp
    local_heads = heads // dp
    spot, place = lax.axis_index("dp"), lax.axis_index("fsdp")
    rank = spot * fsdp + place
    both = (("fsdp", fsdp), ("dp", dp))

    out_w = lax.all_gather(w_out, "fsdp", axis=0, tiled=True)
    cols = w_qkv.reshape(shard, 3, dp, part).transpose(0, 2, 1, 3).reshape(shard, 3 * width)
    cols = lax.all_to_all(cols, "dp", 1, 0, tiled=True).reshape(dp, shard, 3 * part)
    qkv_w = lax.all_gather(cols, "fsdp", axis=1, tiled=True).reshape(width, 3 * part)
    w_up, cols = lax.optimization_barrier((w_up, cols))
    ups = lax.all_to_all(w_up, "dp", 1, 0, tiled=True).reshape(dp, shard, ff_part)
    up_w = lax.all_gather(ups, "fsdp", axis=1, tiled=True).reshape(width, ff_part)
    down_w = lax.all_gather(w_down, "fsdp", axis=0, tiled=True)
    late_tokens, _ = lax.optimization_barrier((tokens, ups))

    full_small = (bias_out, ln1_gain, ln1_bias, bias_down, ln2_gain, ln2_bias)
    row = jnp.concatenate(full_small + (bias_q, bias_v, bias_up))[None]
    table = jnp.zeros((dp * fsdp, row.shape[1]), BF16)
    table = lax.dynamic_update_slice(table, row, (rank, 0))
    wide = (4 * length, width)
    narrow = (length, width)
    kernels = dp == 4 and length % (32 * STEPS) == 0 and ff == dp * width
    stages = len(bits_of(fsdp)) + 2
    if kernels:
        all_tokens, grad_y, table = call_exchange(
            functools.partial(gather_two_kernel, fsdp), 1, 2, 0,
            [(wide, BF16), (wide, BF16), (table.shape, BF16)], [late_tokens, cotangent, table],
            (pltpu.VMEM((stages + 1,) + table.shape, BF16), pltpu.VMEM((stages,) + table.shape, BF16)),
            (2, stages),
        )
    else:
        all_tokens, grad_y = gather_dp(late_tokens, dp), gather_dp(cotangent, dp)
        table = combine_all(table, both, jnp.add)
    table = table.astype(F32)
    small = [table[:, k * shard : (k + 1) * shard].reshape(1, width) for k in range(6)]
    out_b, gain1, shift1, down_b, gain2, shift2 = small
    mine = lax.dynamic_slice(table, (spot * fsdp, 0), (fsdp, row.shape[1]))[:, 6 * shard :]
    q_b, v_b = mine[:, :shard].reshape(1, part), mine[:, shard : 2 * shard].reshape(1, part)
    up_b = mine[:, 2 * shard :].reshape(1, ff_part)

    ranks = (spot * local_heads + 1 + jnp.arange(local_heads)).astype(F32)
    slopes = jnp.exp2(-8.0 * ranks / heads) * SCALE
    places = jnp.arange(length, dtype=jnp.int32)
    gap = places[:, None] - places[None, :]
    distance = jnp.where(gap >= 0, gap.astype(F32), MASKED)

    inputs = tokens.astype(F32)
    normed_all, _ = norm_stats(all_tokens.astype(F32))
    first_in = (normed_all * gain1 + shift1).astype(BF16)
    biases = jnp.concatenate([q_b, jnp.zeros_like(q_b), v_b], 1)
    qkv = (dot(first_in, qkv_w) + biases).astype(BF16)
    mixed, tops = attend(slopes, distance, qkv, length)
    out_part = dot(mixed, out_w).astype(BF16)
    if kernels:
        second_in, hidden = call_exchange(
            hidden_kernel, 2, 2, 1, [(wide, BF16), (narrow, F32)],
            [out_part, tokens, jnp.concatenate([out_b, gain2, shift2], 0)],
        )
    else:
        hidden = inputs + scatter_dp(out_part, dp) + out_b
        normed2, inverse2 = norm_stats(hidden)
        second_in = gather_dp((normed2 * gain2 + shift2).astype(BF16), dp)

    upward = dot(second_in, up_w) + up_b
    cumulative = 0.5 * (1.0 + lax.erf(upward * (0.5**0.5)))
    active = (upward * cumulative).astype(BF16)
    slope = cumulative + upward * jnp.exp(-0.5 * upward * upward) * ((0.5 / jnp.pi) ** 0.5)
    active, slope = lax.optimization_barrier((active, slope.astype(BF16)))

    def reduce_rows(grad):
        return lax.psum_scatter(grad, "fsdp", scatter_dimension=0, tiled=True).astype(F32)

    def reduce_columns(grad):
        grad = grad.reshape(dp, fsdp * shard, grad.shape[1])
        return lax.psum_scatter(grad, "fsdp", scatter_dimension=1, tiled=True)

    def exchange_columns(grad):
        return lax.all_to_all(
            grad.reshape(dp * shard, grad.shape[2]), "dp", 0, 1, tiled=True
        ).astype(F32)

    local_down = dot_tn(active, grad_y).astype(BF16)
    late_y, slope, _ = lax.optimization_barrier((grad_y, slope, local_down))
    grad_upward = (dot_nt(late_y, down_w) * slope).astype(BF16)
    grad_w_down = reduce_rows(local_down)
    local_up = dot_tn(second_in, grad_upward).astype(BF16)
    late_upward, _ = lax.optimization_barrier((grad_upward, local_up))
    second_part = dot_nt(late_upward, up_w).astype(BF16)
    scattered_up = reduce_columns(local_up)
    if kernels:
        branch_all, grad_hidden, branch_sums, output_part = call_exchange(
            branch_kernel, 3, 2, 1,
            [(wide, BF16), (narrow, F32), ((8, width), F32), (wide, BF16)],
            [second_part, hidden, cotangent, jnp.concatenate([out_b, gain2], 0), active, down_w],
            (pltpu.VMEM(active.shape, BF16), pltpu.VMEM(down_w.shape, BF16),
             pltpu.SemaphoreType.DMA((2,))),
            unplaced=2,
        )
    else:
        grad_second = scatter_dp(second_part, dp)
        grad_hidden = cotangent.astype(F32) + norm_back(grad_second, normed2, inverse2, gain2)
        grad_branch = grad_hidden.astype(BF16)
        branch_all = gather_dp(grad_branch, dp)
        branch_sums = jnp.stack([
            jnp.sum(piece, axis=0)
            for piece in (
                cotangent.astype(F32), grad_second * normed2, grad_second,
                grad_branch.astype(F32),
            )
        ])

    grad_mixed = dot_nt(branch_all, out_w).astype(BF16)
    grad_proj = attend_back(slopes, distance, qkv, grad_mixed, length)
    local_qkv = dot_tn(first_in, grad_proj).astype(BF16)
    late_branch, late_proj, _ = lax.optimization_barrier((branch_all, grad_proj, local_qkv))
    grad_w_qkv = exchange_columns(reduce_columns(local_qkv))
    grad_w_qkv = (
        grad_w_qkv.reshape(shard, dp, 3, part).transpose(0, 2, 1, 3).reshape(shard, 3 * width)
    )
    local_out = dot_tn(mixed, late_branch).astype(BF16)
    grad_w_out = reduce_rows(local_out)
    first_part = dot_nt(late_proj, qkv_w).astype(BF16)
    if not kernels:
        output_part = dot(active, down_w).astype(BF16)

    def spread(piece, size, fill=0.0):
        return lax.dynamic_update_slice(
            jnp.full((size,), fill, F32), piece, (spot * piece.shape[0],)
        )

    up_sum = jnp.sum(grad_upward.astype(F32), axis=0)
    q_sum = jnp.sum(grad_proj[:, :part].astype(F32), axis=0)
    v_sum = jnp.sum(grad_proj[:, 2 * part :].astype(F32), axis=0)
    if kernels:
        first_part, scattered_up = lax.optimization_barrier((first_part, scattered_up))
        grad_tokens, output, sums = call_exchange(
            last_kernel, 4, 2, 2, [(narrow, BF16), (narrow, BF16), ((8, width), F32)],
            [first_part, output_part, tokens, hidden, grad_hidden,
             jnp.concatenate([gain1, down_b], 0)],
        )
    else:
        grad_first = scatter_dp(first_part, dp)
        normed1, inverse1 = norm_stats(inputs)
        grad_tokens = grad_hidden + norm_back(grad_first, normed1, inverse1, gain1)
        output = hidden + scatter_dp(output_part, dp) + down_b
        sums = jnp.stack([jnp.sum(grad_first * normed1, axis=0), jnp.sum(grad_first, axis=0)])
    small = jnp.concatenate([
        branch_sums[:4].reshape(4 * width), spread(up_sum, ff), spread(q_sum, width),
        spread(v_sum, width), sums[:2].reshape(2 * width), spread(tops, width, -1e30),
    ]).reshape(-1, width)
    grad_w_up = exchange_columns(scattered_up)
    small, grad_w_up = lax.optimization_barrier((small, grad_w_up))
    small = combine_all(small, both, sum_or_top)
    ups_at = 4 + ff // width
    owned = lax.dynamic_slice(small, (0, rank * shard), (small.shape[0], shard))
    ff_shard = ff // (dp * fsdp)
    owned_up = lax.dynamic_slice(
        small[4:ups_at].reshape(ff), (rank * ff_shard,), (ff_shard,)
    )

    head_top = small[-1, :heads]
    factor = jnp.sqrt(CLIP_TAU / jnp.maximum(head_top, CLIP_TAU))
    column = jnp.repeat(factor, HEAD_DIM)
    columns = jnp.concatenate([column, column, jnp.ones((width,), F32)])
    clipped = (w_qkv.astype(F32) * columns[None, :]).astype(BF16)
    return (
        output.astype(BF16),
        grad_tokens.astype(BF16),
        grad_w_qkv,
        owned[ups_at],
        owned[ups_at + 1],
        grad_w_out,
        owned[3],
        owned[ups_at + 2],
        owned[ups_at + 3],
        grad_w_up,
        owned_up,
        grad_w_down,
        owned[0],
        owned[1],
        owned[2],
        clipped,
    )


def solution(mesh):
    rows, flat = P(("dp", "fsdp"), None), P(("dp", "fsdp"))
    return jax.shard_map(
        functools.partial(layer, mesh.shape["dp"], mesh.shape["fsdp"]),
        mesh=mesh,
        in_specs=(
            rows, flat, rows, flat, flat, rows, flat, flat, flat, rows, flat, rows, flat, flat,
            flat, rows,
        ),
        out_specs=(
            rows, rows, rows, flat, flat, rows, flat, flat, flat, rows, flat, rows, flat, flat,
            flat, rows,
        ),
        check_vma=False,
    )
```

```python
import functools

import jax
import jax.numpy as jnp
from jax import lax
from jax.experimental import pallas as pl
from jax.experimental.pallas import tpu as pltpu
from jax.sharding import PartitionSpec as P


HEAD_DIM = 64
EPS = 1e-05
CLIP_TAU = 5.0
MASKED = 1e35
F32 = jnp.float32
BF16 = jnp.bfloat16
SCALE = HEAD_DIM ** (-0.5)


def swap(value, axis, size, bit):
    return lax.ppermute(value, axis, [(i, i ^ bit) for i in range(size)])


def bits_of(size):
    return [1 << b for b in range(size.bit_length() - 1)]


def gather_path(block, size, bits):
    blocks = {0: block}
    for bit in bits:
        held = sorted(blocks)
        moved = swap(jnp.concatenate([blocks[r] for r in held], 0), "dp", size, bit)
        for place, r in enumerate(held):
            rows = block.shape[0]
            blocks[r ^ bit] = moved[place * rows : (place + 1) * rows]
    return blocks


def gather_dp(block, size):
    half = block.shape[0] // 2
    top = gather_path(block[:half], size, bits_of(size))
    low = gather_path(block[half:], size, bits_of(size)[::-1])
    parts = []
    for r in range(size):
        parts += [top[r], low[r]]
    return jnp.concatenate(parts, 0)


def scatter_path(blocks, size, bits):
    blocks = dict(blocks)
    for bit in bits:
        away = sorted(r for r in blocks if r & bit)
        rows = blocks[0].shape[0]
        sent = jnp.concatenate([blocks[r].astype(BF16) for r in away], 0)
        moved = swap(sent, "dp", size, bit)
        blocks = {
            r ^ bit: blocks[r ^ bit].astype(F32)
            + moved[place * rows : (place + 1) * rows].astype(F32)
            for place, r in enumerate(away)
        }
    return blocks[0]


def scatter_dp(partial, size):
    rows = partial.shape[0] // size
    half = rows // 2
    top = {r: partial[r * rows : r * rows + half] for r in range(size)}
    low = {r: partial[r * rows + half : (r + 1) * rows] for r in range(size)}
    return jnp.concatenate(
        [scatter_path(top, size, bits_of(size)), scatter_path(low, size, bits_of(size)[::-1])], 0
    )


def combine_all(value, sizes, join):
    for axis, size in sizes:
        for bit in bits_of(size):
            value = join(value, swap(value, axis, size, bit))
    return value


STEPS = 4
MESH_IDS = pl.DeviceIdType.MESH
PATHS = ((1, 2), (2, 1))


def flipped(axis, mask):
    me = lax.axis_index(axis)
    there = me
    for bit in bits_of(2 ** mask.bit_length()):
        if mask & bit:
            there = there + bit - 2 * bit * ((me // bit) % 2)
    return {axis: there}


def neighbours(fsdp=1, every=False):
    near = {bit: flipped("dp", bit) for bit in (1, 2)}
    partners = [near[1], near[2]] + [flipped("fsdp", bit) for bit in bits_of(fsdp)]
    greeted = partners if fsdp > 1 else [near[1], near[2]]
    if every:
        greeted = [flipped("dp", mask) for mask in (1, 2, 3)]
        greeted += [flipped("fsdp", mask) for mask in range(1, fsdp)]
    barrier = pltpu.get_barrier_semaphore()
    for where in greeted:
        pl.semaphore_signal(barrier, inc=1, device_id=where, device_id_type=MESH_IDS)
    pl.semaphore_wait(barrier, len(greeted))
    return near, partners


def remote(source, target, sems, index, where):
    return pltpu.make_async_remote_copy(
        src_ref=source, dst_ref=target, send_sem=sems.at[0, index], recv_sem=sems.at[1, index],
        device_id=where, device_id_type=MESH_IDS,
    )


def each_step(act):
    def run(step, carry):
        act(step)
        return carry

    lax.fori_loop(0, STEPS, run, 0)


class Gather:
    def __init__(self, out, sems, near):
        self.out, self.sems, self.near = out, sems, near
        self.rows = out.shape[0] // 4
        self.step_rows = self.rows // 2 // STEPS

    def span(self, block, path, step):
        start = block * self.rows + path * (self.rows // 2) + step * self.step_rows
        return pl.ds(pl.multiple_of(start, self.step_rows), self.step_rows)

    def copy(self, source, bit, path, step, kind):
        return remote(
            self.out.at[self.span(source, path, step)],
            self.out.at[self.span(source + bit, path, step)],
            self.sems, (path * 3 + kind) * STEPS + step, self.near[bit],
        )

    def send(self, path, step):
        first, second = PATHS[path]
        self.copy(0, first, path, step, 0).start()
        self.copy(0, second, path, step, 1).start()

    def forward(self, path, step):
        first, second = PATHS[path]
        self.copy(0, first, path, step, 0).wait_recv()
        self.copy(first, second, path, step, 2).start()

    def finish(self, path, step):
        first, second = PATHS[path]
        self.copy(0, first, path, step, 0).wait_send()
        self.copy(0, second, path, step, 1).wait()
        self.copy(first, second, path, step, 2).wait()


class Scatter:
    def __init__(self, partial, landing, passing, last, sems, near):
        self.partial, self.landing, self.passing, self.last = partial, landing, passing, last
        self.sems, self.near = sems, near
        self.rows = partial.shape[0] // 4
        self.step_rows = self.rows // 2 // STEPS

    def span(self, block, path, step):
        start = block * self.rows + path * (self.rows // 2) + step * self.step_rows
        return pl.ds(pl.multiple_of(start, self.step_rows), self.step_rows)

    def own(self, path, step):
        return self.span(0, path, step)

    def opening(self, path, step, kind):
        first, _ = PATHS[path]
        return remote(
            self.partial.at[self.span((first, 3)[kind], path, step)],
            self.landing.at[kind, self.own(path, step)],
            self.sems, (path * 3 + kind) * STEPS + step, self.near[first],
        )

    def closing(self, path, step):
        rows = self.own(path, step)
        return remote(
            self.passing.at[rows], self.last.at[rows], self.sems,
            (path * 3 + 2) * STEPS + step, self.near[PATHS[path][1]],
        )

    def begin(self, path, step):
        for kind in range(2):
            self.opening(path, step, kind).start()

    def relay(self, path, step):
        _, second = PATHS[path]
        self.opening(path, step, 1).wait_recv()
        rows = self.own(path, step)
        self.passing[rows] = (
            self.partial[self.span(second, path, step)].astype(F32)
            + self.landing[1, rows].astype(F32)
        ).astype(BF16)
        self.closing(path, step).start()

    def total(self, path, step):
        self.opening(path, step, 0).wait_recv()
        self.closing(path, step).wait_recv()
        rows = self.own(path, step)
        return (
            self.partial[self.span(0, path, step)].astype(F32)
            + self.landing[0, rows].astype(F32)
            + self.last[rows].astype(F32)
        )

    def finish(self, path, step):
        for kind in range(2):
            self.opening(path, step, kind).wait_send()
        self.closing(path, step).wait_send()


def row_norm(values):
    centred = values - jnp.mean(values, axis=-1, keepdims=True)
    inverse_std = lax.rsqrt(jnp.mean(centred * centred, axis=-1, keepdims=True) + EPS)
    return centred * inverse_std, inverse_std


def row_back(grad_norm, normed, inverse_std, gain):
    scaled = grad_norm * gain
    return inverse_std * (
        scaled
        - jnp.mean(scaled, axis=-1, keepdims=True)
        - normed * jnp.mean(scaled * normed, axis=-1, keepdims=True)
    )


def double_all(held, landing, sems, partners, join, stages=None):
    for stage in stages or range(len(partners)):
        where = partners[stage]
        copy = remote(held.at[stage], landing.at[stage], sems, stage, where)
        copy.start()
        copy.wait()
        held[stage + 1] = join(held[stage], landing[stage])


def gather_two_kernel(
    fsdp, one_ref, two_ref, table_ref, out_one, out_two, table_out, held, landing, sems, small_sems
):
    near, partners = neighbours(fsdp)
    jobs = []
    for k, (source, out) in enumerate(((one_ref, out_one), (two_ref, out_two))):
        out[: source.shape[0]] = source[...]
        jobs.append(Gather(out, sems.at[k], near))
    held[0] = table_ref[...]
    double_all(held, landing, small_sems, partners, jnp.add, range(2))
    for job in jobs:
        each_step(lambda step, job=job: [job.send(path, step) for path in range(2)])
    double_all(held, landing, small_sems, partners, jnp.add, range(2, len(partners)))
    table_out[...] = held[len(partners)]
    for job in jobs:
        each_step(lambda step, job=job: [job.forward(path, step) for path in range(2)])
    for job in jobs:
        each_step(lambda step, job=job: [job.finish(path, step) for path in range(2)])


def exchange(scatter, gather, rows_of, beside=None):
    each_step(lambda step: [scatter.begin(path, step) for path in range(2)])
    if beside is not None:
        beside()
    each_step(lambda step: [scatter.relay(path, step) for path in range(2)])

    def middle(step):
        for path in range(2):
            rows = scatter.own(path, step)
            gather.out[rows] = rows_of(rows, scatter.total(path, step))
            gather.send(path, step)

        @pl.when(step > 0)
        def _():
            for path in range(2):
                gather.forward(path, step - 1)

    each_step(middle)
    for path in range(2):
        gather.forward(path, STEPS - 1)
    each_step(lambda step: [scatter.finish(path, step) for path in range(2)])
    each_step(lambda step: [gather.finish(path, step) for path in range(2)])


def add_sums(sums_ref, values, start=0):
    for k, value in enumerate(values):
        row = start + k
        sums_ref[row : row + 1] += jnp.sum(value, axis=0, keepdims=True)


def hidden_kernel(
    partial_ref, tokens_ref, params_ref, out_ref, hidden_ref, landing, passing, last, sems
):
    near, _ = neighbours()

    def rows_of(rows, total):
        hidden = tokens_ref[rows].astype(F32) + total + params_ref[0:1]
        hidden_ref[rows] = hidden
        normed, _ = row_norm(hidden)
        return (normed * params_ref[1:2] + params_ref[2:3]).astype(BF16)

    exchange(
        Scatter(partial_ref, landing, passing, last, sems.at[0], near),
        Gather(out_ref, sems.at[1], near), rows_of,
    )


def branch_kernel(
    partial_ref, hidden_ref, cotangent_ref, params_ref, active_ref, weight_ref, out_ref, grad_ref,
    sums_ref, output_ref, landing, passing, last, active, weight, copy_sems, sems,
):
    copies = [
        pltpu.make_async_copy(active_ref, active, copy_sems.at[0]),
        pltpu.make_async_copy(weight_ref, weight, copy_sems.at[1]),
    ]
    for copy in copies:
        copy.start()
    near, _ = neighbours()
    sums_ref[...] = jnp.zeros_like(sums_ref)

    def rows_of(rows, total):
        normed, inverse_std = row_norm(hidden_ref[rows])
        upper = cotangent_ref[rows].astype(F32)
        grad = upper + row_back(total, normed, inverse_std, params_ref[1:2])
        grad_ref[rows] = grad
        branch = grad.astype(BF16)
        add_sums(sums_ref, (upper, total * normed, total, branch.astype(F32)))
        return branch

    def output_tile(tile, carry):
        columns = pl.ds(pl.multiple_of(tile * 256, 256), 256)
        output_ref[:, columns] = dot(active[...], weight[:, columns]).astype(BF16)
        return carry

    def beside():
        for copy in copies:
            copy.wait()
        lax.fori_loop(0, output_ref.shape[1] // 256, output_tile, 0)

    exchange(
        Scatter(partial_ref, landing, passing, last, sems.at[0], near),
        Gather(out_ref, sems.at[1], near), rows_of, beside,
    )


def sum_or_top(a, b):
    row = lax.broadcasted_iota(jnp.int32, a.shape, 0)
    return jnp.where(row < a.shape[0] - 1, a + b, jnp.maximum(a, b))


class LineSum:
    def __init__(self, grad, merged, down, up, sems, size):
        self.grad, self.merged, self.flows, self.sems = grad, merged, (down, up), sems
        self.chips, self.chunks = size // 2, grad.shape[0]
        place = lax.axis_index("fsdp")
        self.chip, self.core = place // 2, place % 2
        self.next = ({"fsdp": place - 2}, {"fsdp": place + 2})

    def core_copy(self, piece):
        return remote(
            self.grad.at[:, piece * 2 + 1 - self.core], self.merged.at[piece], self.sems, piece,
            flipped("fsdp", 1),
        )

    def begin(self):
        for piece in range(self.chips):
            self.core_copy(piece).start()

    def each_chunk(self, act):
        if self.chunks == 1:
            return act(0)

        def run(chunk, carry):
            act(chunk)
            return carry

        return lax.fori_loop(0, self.chunks, run, 0)

    def merge(self):
        for piece in range(self.chips):
            self.core_copy(piece).wait_recv()

            def add(chunk, piece=piece):
                self.merged[piece, chunk] = (
                    self.merged[piece, chunk].astype(F32)
                    + self.grad[chunk, piece * 2 + self.core].astype(F32)
                ).astype(BF16)

            self.each_chunk(add)

    def hop(self, flow, step, chunk, source):
        index = self.chips + (flow * (self.chips - 1) + step - 1) * self.chunks + chunk
        return remote(
            source, self.flows[flow].at[step - 1, chunk], self.sems, index, self.next[flow]
        )

    def landed(self, flow, step, chunk):
        return self.hop(flow, step, chunk, self.flows[flow].at[step - 1, chunk])

    def ends(self, flow):
        return self.chip == (self.chips - 1, 0)[flow]

    def receives(self, flow, step):
        far = (self.chips - 1 - self.chip, self.chip)[flow]
        return (far >= 1) & (far <= step)

    def sends(self, flow, step):
        far = (self.chips - 1 - self.chip, self.chip)[flow]
        return far <= step - 1

    def piece(self, flow, step):
        return self.chip + (step - self.chips + 1, self.chips - 1 - step)[flow]

    def open(self, step):
        for flow in range(2):
            piece = (step - 1, self.chips - step)[flow]

            @pl.when(self.ends(flow))
            def _(flow=flow, piece=piece):
                self.each_chunk(
                    lambda chunk: self.hop(
                        flow, step, chunk, self.merged.at[piece, chunk]
                    ).start()
                )

    def relay(self, step):
        def one(chunk):
            for flow in range(2):

                @pl.when(self.receives(flow, step))
                def _(flow=flow):
                    self.landed(flow, step, chunk).wait_recv()
                    held = self.flows[flow]
                    held[step - 1, chunk] = (
                        held[step - 1, chunk].astype(F32)
                        + self.merged[self.piece(flow, step), chunk].astype(F32)
                    ).astype(BF16)
                    self.hop(flow, step + 1, chunk, held.at[step - 1, chunk]).start()

        self.each_chunk(one)

    def total(self, out, chunk):
        step = self.chips - 1
        out[chunk] = self.merged[self.chip, chunk].astype(F32)
        for flow in range(2):

            @pl.when(self.receives(flow, step))
            def _(flow=flow):
                self.landed(flow, step, chunk).wait_recv()
                out[chunk] += self.flows[flow][step - 1, chunk].astype(F32)

    def finish(self):
        for piece in range(self.chips):
            self.core_copy(piece).wait_send()
        for flow in range(2):
            for step in range(1, self.chips):

                @pl.when(self.sends(flow, step))
                def _(flow=flow, step=step):
                    self.each_chunk(lambda chunk: self.landed(flow, step, chunk).wait_send())


class Across:
    def __init__(self, source, landing, sems):
        self.source, self.landing, self.sems = source, landing, sems
        self.me = lax.axis_index("dp")

    def copy(self, chunk, slot):
        return pltpu.make_async_remote_copy(
            src_ref=self.source.at[chunk], dst_ref=self.landing.at[slot],
            send_sem=self.sems.at[0, chunk], recv_sem=self.sems.at[1, slot],
            device_id={"dp": chunk}, device_id_type=MESH_IDS,
        )

    def send(self, chunk):
        @pl.when(self.me != chunk)
        def _():
            self.copy(chunk, self.me).start()

        @pl.when(self.me == chunk)
        def _():
            self.landing[chunk] = self.source[chunk]

    def receive(self, slot):
        @pl.when(self.me != slot)
        def _():
            self.copy(slot, slot).wait_recv()

    def finish(self, chunk):
        @pl.when(self.me != chunk)
        def _():
            self.copy(chunk, self.me).wait_send()


def last_kernel(
    fsdp, first_ref, output_ref, tokens_ref, hidden_ref, grad_ref, params_ref, small_ref, qkv_ref,
    out_ref, up_ref, tokens_out, output_out, small_out, qkv_out, out_out, up_out, landing,
    passing, last, held, small_landing, sums, qkv_merged, qkv_down, qkv_up, out_merged, out_down,
    out_up, qkv_total, qkv_low, qkv_in, up_in, qkv_sems, out_sems, across_sems, sems, small_sems,
):
    near, partners = neighbours(fsdp, True)
    dp, part = qkv_ref.shape[0], qkv_ref.shape[3] // 3
    lines = (
        LineSum(qkv_ref, qkv_merged, qkv_down, qkv_up, qkv_sems, fsdp),
        LineSum(out_ref, out_merged, out_down, out_up, out_sems, fsdp),
    )
    up_across = Across(up_ref, up_in, across_sems.at[0])
    qkv_across = Across(qkv_low, qkv_in, across_sems.at[1])
    first, second = (
        Scatter(ref, landing.at[k], passing.at[k], last.at[k], sems.at[k], near)
        for k, ref in enumerate((first_ref, output_ref))
    )

    def first_rows(path, step):
        rows = first.own(path, step)
        total = first.total(path, step)
        normed, inverse_std = row_norm(tokens_ref[rows].astype(F32))
        grad = grad_ref[rows] + row_back(total, normed, inverse_std, params_ref[0:1])
        tokens_out[rows] = grad.astype(BF16)
        add_sums(sums, (total * normed, total), 2)

    def second_rows(path, step):
        rows = second.own(path, step)
        total = second.total(path, step)
        output_out[rows] = (hidden_ref[rows] + total + params_ref[1:2]).astype(BF16)

    for line in lines:
        line.begin()
    for job in (first, second):
        each_step(lambda step, job=job: [job.begin(path, step) for path in range(2)])
    for chunk in range(dp):
        up_across.send(chunk)
    sums[...] = jnp.zeros_like(sums)
    for line in lines:
        line.merge()
    for step in range(1, fsdp // 2):
        for line in lines:
            line.open(step)
    each_step(lambda step: [first.relay(path, step) for path in range(2)])
    for line in lines:
        line.relay(1)
    each_step(lambda step: [second.relay(path, step) for path in range(2)])
    for step in range(2, fsdp // 2 - 1):
        for line in lines:
            line.relay(step)
    each_step(lambda step: [first_rows(path, step) for path in range(2)])
    each_step(lambda step: [second_rows(path, step) for path in range(2)])
    held[0, :8] = small_ref[:8]
    held[0, 8:] = small_ref[8:] + sums[...]
    double_all(held, small_landing, small_sems, partners, sum_or_top, range(2))
    for chunk in range(dp):
        lines[0].total(qkv_total, chunk)
        qkv_low[chunk] = qkv_total[chunk].astype(BF16)
        qkv_across.send(chunk)
    lines[1].total(out_out, 0)
    double_all(held, small_landing, small_sems, partners, sum_or_top, range(2, len(partners)))
    small_out[...] = held[len(partners)]
    columns = up_ref.shape[2]
    for slot in range(dp):
        up_across.receive(slot)
        up_out[:, slot * columns : (slot + 1) * columns] = up_in[slot].astype(F32)
    for slot in range(dp):
        qkv_across.receive(slot)
        for third in range(3):
            start = (third * dp + slot) * part
            qkv_out[:, start : start + part] = qkv_in[
                slot, :, third * part : (third + 1) * part
            ].astype(F32)
    for job in (first, second):
        each_step(lambda step, job=job: [job.finish(path, step) for path in range(2)])
    for line in lines:
        line.finish()
    for chunk in range(dp):
        up_across.finish(chunk)
        qkv_across.finish(chunk)


def call_exchange(kernel, number, jobs, scatters, outs, args, extra=(), stages=0, unplaced=0):
    rows, width = args[0].shape if scatters else (4 * args[0].shape[0], args[0].shape[1])
    own = rows // 4
    room = []
    if scatters == 1:
        room = [(2, own, width), (own, width), (own, width)]
    if scatters == 2:
        room = [(2, 2, own, width), (2, own, width), (2, own, width)]
    return pl.pallas_call(
        kernel,
        in_specs=[pl.BlockSpec(memory_space=pltpu.VMEM)] * (len(args) - unplaced)
        + [pl.BlockSpec(memory_space=pl.ANY)] * unplaced,
        out_specs=[pl.BlockSpec(memory_space=pltpu.VMEM)] * len(outs),
        out_shape=[jax.ShapeDtypeStruct(shape, dtype) for shape, dtype in outs],
        scratch_shapes=[
            *(pltpu.VMEM(shape, BF16) for shape in room),
            *extra,
            pltpu.SemaphoreType.DMA((jobs, 2, 6 * STEPS)),
            *([pltpu.SemaphoreType.DMA(stages)] if stages else []),
        ],
        compiler_params=pltpu.CompilerParams(
            collective_id=number, has_side_effects=True, vmem_limit_bytes=60 << 20
        ),
        cost_estimate=pl.CostEstimate(
            flops=rows * width, bytes_accessed=200 << 20, transcendentals=0
        ),
    )(*args)


def pair_span(offset, pair):
    return pl.ds(offset + pair * 2 * HEAD_DIM, 2 * HEAD_DIM)


def head_parts(ref, offset, pair):
    both = ref[:, pair_span(offset, pair)]
    return both[:, :HEAD_DIM], both[:, HEAD_DIM:]


def dot_nt(a, b):
    return lax.dot_general(a, b, (((1,), (1,)), ((), ())), preferred_element_type=F32)


def dot_tn(a, b):
    return lax.dot_general(a, b, (((0,), (0,)), ((), ())), preferred_element_type=F32)


def attend_kernel(slope_ref, distance_ref, qkv_ref, mixed_ref, top_ref):
    width = mixed_ref.shape[1]
    lane = lax.broadcasted_iota(jnp.int32, (8, 128), 1)

    distance = distance_ref[...]
    tops = jnp.zeros((8, 128), F32)
    for pair in range(width // HEAD_DIM // 2):
        outs = []
        for t, (q, k, v) in enumerate(
            zip(*(head_parts(qkv_ref, part * width, pair) for part in range(3)))
        ):
            logits = dot_nt(q * jnp.asarray(SCALE, BF16), k)
            head_top = jnp.max(jnp.where(distance < MASKED, logits, -1e30))
            tops = jnp.where(lane == pair * 2 + t, head_top, tops)
            scores = logits - slope_ref[pair * 2 + t] * distance
            expos = jnp.exp(scores - jnp.max(scores, axis=-1, keepdims=True))
            probs = expos * (1.0 / jnp.sum(expos, axis=-1, keepdims=True))
            outs.append(jnp.dot(probs.astype(BF16), v, preferred_element_type=F32))
        mixed_ref[:, pair_span(0, pair)] = jnp.concatenate(outs, 1).astype(BF16)
    top_ref[...] = tops


def attend_back_kernel(slope_ref, distance_ref, qkv_ref, grad_ref, out_ref):
    width = grad_ref.shape[1]

    distance = distance_ref[...]
    for pair in range(width // HEAD_DIM // 2):
        outs = ([], [], [])
        parts = [head_parts(qkv_ref, part * width, pair) for part in range(3)]
        parts.append(head_parts(grad_ref, 0, pair))
        for t, (q, k, v, grad) in enumerate(zip(*parts)):
            low_q = q * jnp.asarray(SCALE, BF16)
            scores = dot_nt(low_q, k) - slope_ref[pair * 2 + t] * distance
            expos = jnp.exp(scores - jnp.max(scores, axis=-1, keepdims=True))
            probs = expos * (1.0 / jnp.sum(expos, axis=-1, keepdims=True))
            outs[2].append(dot_tn(probs.astype(BF16), grad))
            grad_probs = dot_nt(grad, v)
            inner = jnp.sum(grad_probs * probs, axis=-1, keepdims=True)
            grad_scores = (probs * (grad_probs - inner)).astype(BF16)
            outs[0].append(jnp.dot(grad_scores, k, preferred_element_type=F32) * SCALE)
            outs[1].append(dot_tn(grad_scores, low_q))
        for part in range(3):
            out_ref[:, pair_span(part * width, pair)] = jnp.concatenate(outs[part], 1).astype(BF16)


def attend(slopes, distance, qkv, length):
    rows, width = qkv.shape[0], qkv.shape[1] // 3
    blocks = rows // length
    mixed, tops = pl.pallas_call(
        attend_kernel,
        grid=(blocks,),
        in_specs=[
            pl.BlockSpec(memory_space=pltpu.SMEM),
            pl.BlockSpec((length, length), lambda b: (0, 0)),
            pl.BlockSpec((length, 3 * width), lambda b: (b, 0)),
        ],
        out_specs=[
            pl.BlockSpec((length, width), lambda b: (b, 0)),
            pl.BlockSpec((8, 128), lambda b: (b, 0)),
        ],
        out_shape=[
            jax.ShapeDtypeStruct((rows, width), BF16),
            jax.ShapeDtypeStruct((blocks * 8, 128), F32),
        ],
        cost_estimate=pl.CostEstimate(
            flops=4 * rows * length * width, bytes_accessed=8 * rows * width,
            transcendentals=rows * length * width // HEAD_DIM,
        ),
        name="attend",
    )(slopes, distance, qkv)
    return mixed, jnp.max(tops, axis=0)[: width // HEAD_DIM]


def attend_back(slopes, distance, qkv, grad, length):
    rows, width = grad.shape
    return pl.pallas_call(
        attend_back_kernel,
        grid=(rows // length,),
        in_specs=[
            pl.BlockSpec(memory_space=pltpu.SMEM),
            pl.BlockSpec((length, length), lambda b: (0, 0)),
            pl.BlockSpec((length, 3 * width), lambda b: (b, 0)),
            pl.BlockSpec((length, width), lambda b: (b, 0)),
        ],
        out_specs=pl.BlockSpec((length, 3 * width), lambda b: (b, 0)),
        out_shape=jax.ShapeDtypeStruct((rows, 3 * width), BF16),
        cost_estimate=pl.CostEstimate(
            flops=10 * rows * length * width, bytes_accessed=14 * rows * width,
            transcendentals=rows * length * width // HEAD_DIM,
        ),
        name="attend_back",
    )(slopes, distance, qkv, grad)


def norm_stats(values):
    row_mean = jnp.mean(values, axis=-1, keepdims=True)
    centred = values - row_mean
    inverse_std = lax.rsqrt(jnp.mean(centred * centred, axis=-1, keepdims=True) + EPS)
    return centred * inverse_std, inverse_std


def norm_back(grad_norm, normed, inverse_std, gain):
    scaled = grad_norm * gain
    return inverse_std * (
        scaled
        - jnp.mean(scaled, axis=-1, keepdims=True)
        - normed * jnp.mean(scaled * normed, axis=-1, keepdims=True)
    )


def dot(a, b):
    return jnp.dot(a, b, preferred_element_type=F32)


def layer(
    dp, fsdp, tokens, seq_lengths, w_qkv, bias_q, bias_v, w_out, bias_out, ln1_gain, ln1_bias,
    w_up, bias_up, w_down, bias_down, ln2_gain, ln2_bias, cotangent,
):
    length, width = tokens.shape
    shard = w_qkv.shape[0]
    ff = w_up.shape[1]
    heads = width // HEAD_DIM
    part, ff_part = width // dp, ff // dp
    local_heads = heads // dp
    spot, place = lax.axis_index("dp"), lax.axis_index("fsdp")
    rank = spot * fsdp + place
    both = (("fsdp", fsdp), ("dp", dp))

    out_w = lax.all_gather(w_out, "fsdp", axis=0, tiled=True)
    cols = w_qkv.reshape(shard, 3, dp, part).transpose(0, 2, 1, 3).reshape(shard, 3 * width)
    cols = lax.all_to_all(cols, "dp", 1, 0, tiled=True).reshape(dp, shard, 3 * part)
    qkv_w = lax.all_gather(cols, "fsdp", axis=1, tiled=True).reshape(width, 3 * part)
    w_up, cols = lax.optimization_barrier((w_up, cols))
    ups = lax.all_to_all(w_up, "dp", 1, 0, tiled=True).reshape(dp, shard, ff_part)
    up_w = lax.all_gather(ups, "fsdp", axis=1, tiled=True).reshape(width, ff_part)
    down_w = lax.all_gather(w_down, "fsdp", axis=0, tiled=True)
    late_tokens, _ = lax.optimization_barrier((tokens, ups))

    full_small = (bias_out, ln1_gain, ln1_bias, bias_down, ln2_gain, ln2_bias)
    row = jnp.concatenate(full_small + (bias_q, bias_v, bias_up))[None]
    table = jnp.zeros((dp * fsdp, row.shape[1]), BF16)
    table = lax.dynamic_update_slice(table, row, (rank, 0))
    wide = (4 * length, width)
    narrow = (length, width)
    kernels = dp == 4 and fsdp == 8 and length % (32 * STEPS) == 0 and ff == dp * width
    stages = len(bits_of(fsdp)) + 2
    if kernels:
        all_tokens, grad_y, table = call_exchange(
            functools.partial(gather_two_kernel, fsdp), 1, 2, 0,
            [(wide, BF16), (wide, BF16), (table.shape, BF16)], [late_tokens, cotangent, table],
            (pltpu.VMEM((stages + 1,) + table.shape, BF16), pltpu.VMEM((stages,) + table.shape, BF16)),
            (2, stages),
        )
    else:
        all_tokens, grad_y = gather_dp(late_tokens, dp), gather_dp(cotangent, dp)
        table = combine_all(table, both, jnp.add)
    table = table.astype(F32)
    small = [table[:, k * shard : (k + 1) * shard].reshape(1, width) for k in range(6)]
    out_b, gain1, shift1, down_b, gain2, shift2 = small
    mine = lax.dynamic_slice(table, (spot * fsdp, 0), (fsdp, row.shape[1]))[:, 6 * shard :]
    q_b, v_b = mine[:, :shard].reshape(1, part), mine[:, shard : 2 * shard].reshape(1, part)
    up_b = mine[:, 2 * shard :].reshape(1, ff_part)

    ranks = (spot * local_heads + 1 + jnp.arange(local_heads)).astype(F32)
    slopes = jnp.exp2(-8.0 * ranks / heads) * SCALE
    places = jnp.arange(length, dtype=jnp.int32)
    gap = places[:, None] - places[None, :]
    distance = jnp.where(gap >= 0, gap.astype(F32), MASKED)

    inputs = tokens.astype(F32)
    normed_all, _ = norm_stats(all_tokens.astype(F32))
    first_in = (normed_all * gain1 + shift1).astype(BF16)
    biases = jnp.concatenate([q_b, jnp.zeros_like(q_b), v_b], 1)
    qkv = (dot(first_in, qkv_w) + biases).astype(BF16)
    mixed, tops = attend(slopes, distance, qkv, length)
    out_part = dot(mixed, out_w).astype(BF16)
    if kernels:
        second_in, hidden = call_exchange(
            hidden_kernel, 2, 2, 1, [(wide, BF16), (narrow, F32)],
            [out_part, tokens, jnp.concatenate([out_b, gain2, shift2], 0)],
        )
    else:
        hidden = inputs + scatter_dp(out_part, dp) + out_b
        normed2, inverse2 = norm_stats(hidden)
        second_in = gather_dp((normed2 * gain2 + shift2).astype(BF16), dp)

    upward = dot(second_in, up_w) + up_b
    cumulative = 0.5 * (1.0 + lax.erf(upward * (0.5**0.5)))
    active = (upward * cumulative).astype(BF16)
    slope = cumulative + upward * jnp.exp(-0.5 * upward * upward) * ((0.5 / jnp.pi) ** 0.5)
    active, slope = lax.optimization_barrier((active, slope.astype(BF16)))

    def reduce_rows(grad):
        return lax.psum_scatter(grad, "fsdp", scatter_dimension=0, tiled=True).astype(F32)

    def reduce_columns(grad):
        grad = grad.reshape(dp, fsdp * shard, grad.shape[1])
        return lax.psum_scatter(grad, "fsdp", scatter_dimension=1, tiled=True)

    def exchange_columns(grad):
        return lax.all_to_all(
            grad.reshape(dp * shard, grad.shape[2]), "dp", 0, 1, tiled=True
        ).astype(F32)

    local_down = dot_tn(active, grad_y).astype(BF16)
    late_y, slope, _ = lax.optimization_barrier((grad_y, slope, local_down))
    grad_upward = (dot_nt(late_y, down_w) * slope).astype(BF16)
    grad_w_down = reduce_rows(local_down)
    local_up = dot_tn(second_in, grad_upward).astype(BF16)
    late_upward, _ = lax.optimization_barrier((grad_upward, local_up))
    second_part = dot_nt(late_upward, up_w).astype(BF16)
    scattered_up = reduce_columns(local_up)
    if kernels:
        branch_all, grad_hidden, branch_sums, output_part = call_exchange(
            branch_kernel, 3, 2, 1,
            [(wide, BF16), (narrow, F32), ((8, width), F32), (wide, BF16)],
            [second_part, hidden, cotangent, jnp.concatenate([out_b, gain2], 0), active, down_w],
            (pltpu.VMEM(active.shape, BF16), pltpu.VMEM(down_w.shape, BF16),
             pltpu.SemaphoreType.DMA((2,))),
            unplaced=2,
        )
    else:
        grad_second = scatter_dp(second_part, dp)
        grad_hidden = cotangent.astype(F32) + norm_back(grad_second, normed2, inverse2, gain2)
        grad_branch = grad_hidden.astype(BF16)
        branch_all = gather_dp(grad_branch, dp)
        branch_sums = jnp.stack([
            jnp.sum(piece, axis=0)
            for piece in (
                cotangent.astype(F32), grad_second * normed2, grad_second,
                grad_branch.astype(F32),
            )
        ])

    grad_mixed = dot_nt(branch_all, out_w).astype(BF16)
    grad_proj = attend_back(slopes, distance, qkv, grad_mixed, length)
    local_qkv = dot_tn(first_in, grad_proj).astype(BF16)
    late_branch, late_proj, _ = lax.optimization_barrier((branch_all, grad_proj, local_qkv))
    local_out = dot_tn(mixed, late_branch).astype(BF16)
    if not kernels:
        grad_w_qkv = exchange_columns(reduce_columns(local_qkv))
        grad_w_qkv = (
            grad_w_qkv.reshape(shard, dp, 3, part).transpose(0, 2, 1, 3).reshape(shard, 3 * width)
        )
        grad_w_out = reduce_rows(local_out)
    first_part = dot_nt(late_proj, qkv_w).astype(BF16)
    if not kernels:
        output_part = dot(active, down_w).astype(BF16)

    def spread(piece, size, fill=0.0):
        return lax.dynamic_update_slice(
            jnp.full((size,), fill, F32), piece, (spot * piece.shape[0],)
        )

    up_sum = jnp.sum(grad_upward.astype(F32), axis=0)
    q_sum = jnp.sum(grad_proj[:, :part].astype(F32), axis=0)
    v_sum = jnp.sum(grad_proj[:, 2 * part :].astype(F32), axis=0)
    if kernels:
        small = jnp.concatenate([
            branch_sums[:4].reshape(4 * width), spread(up_sum, ff), spread(q_sum, width),
            spread(v_sum, width), jnp.zeros((5 * width,), F32), spread(tops, width, -1e30),
        ]).reshape(-1, width)

        def room(grad):
            chips, piece = fsdp // 2, (grad.shape[0],) + grad.shape[2:]
            return tuple(
                pltpu.VMEM((count,) + piece, BF16) for count in (chips, chips - 1, chips - 1)
            )

        def line_sems(grad):
            chips = fsdp // 2
            return pltpu.SemaphoreType.DMA((2, chips + 2 * (chips - 1) * grad.shape[0]))

        qkv_grad = local_qkv.reshape(dp, fsdp, shard, 3 * part)
        out_grad = local_out.reshape(1, fsdp, shard, width)
        grad_tokens, output, small, grad_w_qkv, grad_w_out, grad_w_up = call_exchange(
            functools.partial(last_kernel, fsdp), 4, 2, 2,
            [(narrow, BF16), (narrow, BF16), (small.shape, F32), (w_qkv.shape, F32),
             ((1, shard, width), F32), (w_up.shape, F32)],
            [first_part, output_part, tokens, hidden, grad_hidden,
             jnp.concatenate([gain1, down_b], 0), small, qkv_grad, out_grad,
             scattered_up.reshape(dp, shard, ff_part)],
            (
                pltpu.VMEM((stages + 1,) + small.shape, F32),
                pltpu.VMEM((stages,) + small.shape, F32), pltpu.VMEM((8, width), F32),
                *room(qkv_grad), *room(out_grad),
                pltpu.VMEM((dp, shard, 3 * part), F32), pltpu.VMEM((dp, shard, 3 * part), BF16),
                pltpu.VMEM((dp, shard, 3 * part), BF16), pltpu.VMEM((dp, shard, ff_part), BF16),
                line_sems(qkv_grad), line_sems(out_grad), pltpu.SemaphoreType.DMA((2, 2, dp)),
            ),
            (2, stages),
        )
        grad_w_out = grad_w_out[0]
    else:
        grad_first = scatter_dp(first_part, dp)
        normed1, inverse1 = norm_stats(inputs)
        grad_tokens = grad_hidden + norm_back(grad_first, normed1, inverse1, gain1)
        output = hidden + scatter_dp(output_part, dp) + down_b
        sums = (jnp.sum(grad_first * normed1, axis=0), jnp.sum(grad_first, axis=0))
        small = jnp.concatenate([
            branch_sums[:4].reshape(4 * width), spread(up_sum, ff), spread(q_sum, width),
            spread(v_sum, width), *sums, jnp.zeros((3 * width,), F32), spread(tops, width, -1e30),
        ]).reshape(-1, width)
        grad_w_up = exchange_columns(scattered_up)
        small = combine_all(small, both, sum_or_top)
    ups_at = 4 + ff // width
    owned = lax.dynamic_slice(small, (0, rank * shard), (small.shape[0], shard))
    ff_shard = ff // (dp * fsdp)
    owned_up = lax.dynamic_slice(
        small[4:ups_at].reshape(ff), (rank * ff_shard,), (ff_shard,)
    )

    head_top = small[-1, :heads]
    factor = jnp.sqrt(CLIP_TAU / jnp.maximum(head_top, CLIP_TAU))
    column = jnp.repeat(factor, HEAD_DIM)
    columns = jnp.concatenate([column, column, jnp.ones((width,), F32)])
    clipped = (w_qkv.astype(F32) * columns[None, :]).astype(BF16)
    return (
        output.astype(BF16),
        grad_tokens.astype(BF16),
        grad_w_qkv,
        owned[ups_at],
        owned[ups_at + 1],
        grad_w_out,
        owned[3],
        owned[ups_at + 2],
        owned[ups_at + 3],
        grad_w_up,
        owned_up,
        grad_w_down,
        owned[0],
        owned[1],
        owned[2],
        clipped,
    )


def solution(mesh):
    rows, flat = P(("dp", "fsdp"), None), P(("dp", "fsdp"))
    return jax.shard_map(
        functools.partial(layer, mesh.shape["dp"], mesh.shape["fsdp"]),
        mesh=mesh,
        in_specs=(
            rows, flat, rows, flat, flat, rows, flat, flat, flat, rows, flat, rows, flat, flat,
            flat, rows,
        ),
        out_specs=(
            rows, rows, rows, flat, flat, rows, flat, flat, flat, rows, flat, rows, flat, flat,
            flat, rows,
        ),
        check_vma=False,
    )
```

```python
import functools

import jax
import jax.numpy as jnp
from jax import lax
from jax.experimental import pallas as pl
from jax.experimental.pallas import tpu as pltpu
from jax.sharding import PartitionSpec as P


HEAD_DIM = 64
EPS = 1e-05
CLIP_TAU = 5.0
MASKED = 1e35
F32 = jnp.float32
BF16 = jnp.bfloat16
SCALE = HEAD_DIM ** (-0.5)


def swap(value, axis, size, bit):
    return lax.ppermute(value, axis, [(i, i ^ bit) for i in range(size)])


def bits_of(size):
    return [1 << b for b in range(size.bit_length() - 1)]


def gather_path(block, size, bits):
    blocks = {0: block}
    for bit in bits:
        held = sorted(blocks)
        moved = swap(jnp.concatenate([blocks[r] for r in held], 0), "dp", size, bit)
        for place, r in enumerate(held):
            rows = block.shape[0]
            blocks[r ^ bit] = moved[place * rows : (place + 1) * rows]
    return blocks


def gather_dp(block, size):
    half = block.shape[0] // 2
    top = gather_path(block[:half], size, bits_of(size))
    low = gather_path(block[half:], size, bits_of(size)[::-1])
    parts = []
    for r in range(size):
        parts += [top[r], low[r]]
    return jnp.concatenate(parts, 0)


def scatter_path(blocks, size, bits):
    blocks = dict(blocks)
    for bit in bits:
        away = sorted(r for r in blocks if r & bit)
        rows = blocks[0].shape[0]
        sent = jnp.concatenate([blocks[r].astype(BF16) for r in away], 0)
        moved = swap(sent, "dp", size, bit)
        blocks = {
            r ^ bit: blocks[r ^ bit].astype(F32)
            + moved[place * rows : (place + 1) * rows].astype(F32)
            for place, r in enumerate(away)
        }
    return blocks[0]


def scatter_dp(partial, size):
    rows = partial.shape[0] // size
    half = rows // 2
    top = {r: partial[r * rows : r * rows + half] for r in range(size)}
    low = {r: partial[r * rows + half : (r + 1) * rows] for r in range(size)}
    return jnp.concatenate(
        [scatter_path(top, size, bits_of(size)), scatter_path(low, size, bits_of(size)[::-1])], 0
    )


def combine_all(value, sizes, join):
    for axis, size in sizes:
        for bit in bits_of(size):
            value = join(value, swap(value, axis, size, bit))
    return value


STEPS = 4
MESH_IDS = pl.DeviceIdType.MESH
PATHS = ((1, 2), (2, 1))


def flipped(axis, mask):
    me = lax.axis_index(axis)
    there = me
    for bit in bits_of(2 ** mask.bit_length()):
        if mask & bit:
            there = there + bit - 2 * bit * ((me // bit) % 2)
    return {axis: there}


def neighbours(fsdp=1, every=False):
    near = {bit: flipped("dp", bit) for bit in (1, 2)}
    partners = [near[1], near[2]] + [flipped("fsdp", bit) for bit in bits_of(fsdp)]
    greeted = partners if fsdp > 1 else [near[1], near[2]]
    if every:
        greeted = [flipped("dp", mask) for mask in (1, 2, 3)]
        greeted += [flipped("fsdp", mask) for mask in range(1, fsdp)]
    barrier = pltpu.get_barrier_semaphore()
    for where in greeted:
        pl.semaphore_signal(barrier, inc=1, device_id=where, device_id_type=MESH_IDS)
    pl.semaphore_wait(barrier, len(greeted))
    return near, partners


def remote(source, target, sems, index, where):
    return pltpu.make_async_remote_copy(
        src_ref=source, dst_ref=target, send_sem=sems.at[0, index], recv_sem=sems.at[1, index],
        device_id=where, device_id_type=MESH_IDS,
    )


def each_step(act):
    def run(step, carry):
        act(step)
        return carry

    lax.fori_loop(0, STEPS, run, 0)


class Gather:
    def __init__(self, out, sems, near):
        self.out, self.sems, self.near = out, sems, near
        self.rows = out.shape[0] // 4
        self.step_rows = self.rows // 2 // STEPS

    def span(self, block, path, step):
        start = block * self.rows + path * (self.rows // 2) + step * self.step_rows
        return pl.ds(pl.multiple_of(start, self.step_rows), self.step_rows)

    def copy(self, source, bit, path, step, kind):
        return remote(
            self.out.at[self.span(source, path, step)],
            self.out.at[self.span(source + bit, path, step)],
            self.sems, (path * 3 + kind) * STEPS + step, self.near[bit],
        )

    def send(self, path, step):
        first, second = PATHS[path]
        self.copy(0, first, path, step, 0).start()
        self.copy(0, second, path, step, 1).start()

    def forward(self, path, step):
        first, second = PATHS[path]
        self.copy(0, first, path, step, 0).wait_recv()
        self.copy(first, second, path, step, 2).start()

    def finish(self, path, step):
        first, second = PATHS[path]
        self.copy(0, first, path, step, 0).wait_send()
        self.copy(0, second, path, step, 1).wait()
        self.copy(first, second, path, step, 2).wait()


class Scatter:
    def __init__(self, partial, landing, passing, last, sems, near):
        self.partial, self.landing, self.passing, self.last = partial, landing, passing, last
        self.sems, self.near = sems, near
        self.rows = partial.shape[0] // 4
        self.step_rows = self.rows // 2 // STEPS

    def span(self, block, path, step):
        start = block * self.rows + path * (self.rows // 2) + step * self.step_rows
        return pl.ds(pl.multiple_of(start, self.step_rows), self.step_rows)

    def own(self, path, step):
        return self.span(0, path, step)

    def opening(self, path, step, kind):
        first, _ = PATHS[path]
        return remote(
            self.partial.at[self.span((first, 3)[kind], path, step)],
            self.landing.at[kind, self.own(path, step)],
            self.sems, (path * 3 + kind) * STEPS + step, self.near[first],
        )

    def closing(self, path, step):
        rows = self.own(path, step)
        return remote(
            self.passing.at[rows], self.last.at[rows], self.sems,
            (path * 3 + 2) * STEPS + step, self.near[PATHS[path][1]],
        )

    def begin(self, path, step):
        for kind in range(2):
            self.opening(path, step, kind).start()

    def relay(self, path, step):
        _, second = PATHS[path]
        self.opening(path, step, 1).wait_recv()
        rows = self.own(path, step)
        self.passing[rows] = (
            self.partial[self.span(second, path, step)].astype(F32)
            + self.landing[1, rows].astype(F32)
        ).astype(BF16)
        self.closing(path, step).start()

    def total(self, path, step):
        self.opening(path, step, 0).wait_recv()
        self.closing(path, step).wait_recv()
        rows = self.own(path, step)
        return (
            self.partial[self.span(0, path, step)].astype(F32)
            + self.landing[0, rows].astype(F32)
            + self.last[rows].astype(F32)
        )

    def finish(self, path, step):
        for kind in range(2):
            self.opening(path, step, kind).wait_send()
        self.closing(path, step).wait_send()


def row_norm(values):
    centred = values - jnp.mean(values, axis=-1, keepdims=True)
    inverse_std = lax.rsqrt(jnp.mean(centred * centred, axis=-1, keepdims=True) + EPS)
    return centred * inverse_std, inverse_std


def row_back(grad_norm, normed, inverse_std, gain):
    scaled = grad_norm * gain
    return inverse_std * (
        scaled
        - jnp.mean(scaled, axis=-1, keepdims=True)
        - normed * jnp.mean(scaled * normed, axis=-1, keepdims=True)
    )


class Doubling:
    def __init__(self, held, landing, sems, partners, join):
        self.held, self.landing, self.sems = held, landing, sems
        self.partners, self.join = partners, join

    def copy(self, stage):
        return remote(
            self.held.at[stage], self.landing.at[stage], self.sems, stage, self.partners[stage]
        )

    def start(self, stage):
        self.copy(stage).start()

    def end(self, stage):
        self.copy(stage).wait()
        self.held[stage + 1] = self.join(self.held[stage], self.landing[stage])

    def run(self, *stages):
        for stage in stages:
            self.start(stage)
            self.end(stage)


def gather_two_kernel(
    fsdp, one_ref, two_ref, table_ref, out_one, out_two, table_out, held, landing, sems, small_sems
):
    near, partners = neighbours(fsdp)
    jobs = []
    for k, (source, out) in enumerate(((one_ref, out_one), (two_ref, out_two))):
        out[: source.shape[0]] = source[...]
        jobs.append(Gather(out, sems.at[k], near))
    held[0] = table_ref[...]
    small = Doubling(held, landing, small_sems, partners, jnp.add)
    small.run(0, 1)
    for job in jobs:
        each_step(lambda step, job=job: [job.send(path, step) for path in range(2)])
    small.run(*range(2, len(partners)))
    table_out[...] = held[len(partners)]
    for job in jobs:
        each_step(lambda step, job=job: [job.forward(path, step) for path in range(2)])
    for job in jobs:
        each_step(lambda step, job=job: [job.finish(path, step) for path in range(2)])


def exchange(scatter, gather, rows_of, beside=None):
    each_step(lambda step: [scatter.begin(path, step) for path in range(2)])
    if beside is not None:
        beside()
    each_step(lambda step: [scatter.relay(path, step) for path in range(2)])

    def middle(step):
        for path in range(2):
            rows = scatter.own(path, step)
            gather.out[rows] = rows_of(rows, scatter.total(path, step))
            gather.send(path, step)

        @pl.when(step > 0)
        def _():
            for path in range(2):
                gather.forward(path, step - 1)

    each_step(middle)
    for path in range(2):
        gather.forward(path, STEPS - 1)
    each_step(lambda step: [scatter.finish(path, step) for path in range(2)])
    each_step(lambda step: [gather.finish(path, step) for path in range(2)])


def add_sums(sums_ref, values, start=0):
    for k, value in enumerate(values):
        row = start + k
        sums_ref[row : row + 1] += jnp.sum(value, axis=0, keepdims=True)


def hidden_kernel(
    partial_ref, tokens_ref, params_ref, out_ref, hidden_ref, landing, passing, last, sems
):
    near, _ = neighbours()

    def rows_of(rows, total):
        hidden = tokens_ref[rows].astype(F32) + total + params_ref[0:1]
        hidden_ref[rows] = hidden
        normed, _ = row_norm(hidden)
        return (normed * params_ref[1:2] + params_ref[2:3]).astype(BF16)

    exchange(
        Scatter(partial_ref, landing, passing, last, sems.at[0], near),
        Gather(out_ref, sems.at[1], near), rows_of,
    )


def branch_kernel(
    partial_ref, hidden_ref, cotangent_ref, params_ref, active_ref, weight_ref, out_ref, grad_ref,
    sums_ref, output_ref, landing, passing, last, active, weight, copy_sems, sems,
):
    copies = [
        pltpu.make_async_copy(active_ref, active, copy_sems.at[0]),
        pltpu.make_async_copy(weight_ref, weight, copy_sems.at[1]),
    ]
    for copy in copies:
        copy.start()
    near, _ = neighbours()
    sums_ref[...] = jnp.zeros_like(sums_ref)

    def rows_of(rows, total):
        normed, inverse_std = row_norm(hidden_ref[rows])
        upper = cotangent_ref[rows].astype(F32)
        grad = upper + row_back(total, normed, inverse_std, params_ref[1:2])
        grad_ref[rows] = grad
        branch = grad.astype(BF16)
        add_sums(sums_ref, (upper, total * normed, total, branch.astype(F32)))
        return branch

    def output_tile(tile, carry):
        columns = pl.ds(pl.multiple_of(tile * 256, 256), 256)
        output_ref[:, columns] = dot(active[...], weight[:, columns]).astype(BF16)
        return carry

    def beside():
        for copy in copies:
            copy.wait()
        lax.fori_loop(0, output_ref.shape[1] // 256, output_tile, 0)

    exchange(
        Scatter(partial_ref, landing, passing, last, sems.at[0], near),
        Gather(out_ref, sems.at[1], near), rows_of, beside,
    )


def sum_or_top(a, b):
    row = lax.broadcasted_iota(jnp.int32, a.shape, 0)
    return jnp.where(row < a.shape[0] - 1, a + b, jnp.maximum(a, b))


class LineSum:
    def __init__(self, grad, own, merged, down, up, own_sems, sems, size):
        self.grad, self.merged, self.flows, self.sems = grad, merged, (down, up), sems
        self.own, self.own_sems = own, own_sems
        self.chips, self.chunks = size // 2, grad.shape[0]
        place = lax.axis_index("fsdp")
        self.chip, self.core = place // 2, place % 2
        self.next = ({"fsdp": place - 2}, {"fsdp": place + 2})

    def core_copy(self, piece):
        return remote(
            self.grad.at[:, piece * 2 + 1 - self.core], self.merged.at[piece], self.sems, piece,
            flipped("fsdp", 1),
        )

    def own_copy(self, piece):
        return pltpu.make_async_copy(
            self.grad.at[:, piece * 2 + self.core], self.own.at[piece], self.own_sems.at[piece]
        )

    def begin(self):
        for piece in range(self.chips):
            self.core_copy(piece).start()
            self.own_copy(piece).start()

    def each_chunk(self, act):
        if self.chunks == 1:
            return act(0)

        def run(chunk, carry):
            act(chunk)
            return carry

        return lax.fori_loop(0, self.chunks, run, 0)

    def merge(self):
        for piece in range(self.chips):
            self.core_copy(piece).wait_recv()
            self.own_copy(piece).wait()

            def add(chunk, piece=piece):
                self.merged[piece, chunk] = (
                    self.merged[piece, chunk].astype(F32)
                    + self.own[piece, chunk].astype(F32)
                ).astype(BF16)

            self.each_chunk(add)

    def hop(self, flow, step, chunk, source):
        index = self.chips + (flow * (self.chips - 1) + step - 1) * self.chunks + chunk
        return remote(
            source, self.flows[flow].at[step - 1, chunk], self.sems, index, self.next[flow]
        )

    def landed(self, flow, step, chunk):
        return self.hop(flow, step, chunk, self.flows[flow].at[step - 1, chunk])

    def ends(self, flow):
        return self.chip == (self.chips - 1, 0)[flow]

    def receives(self, flow, step):
        far = (self.chips - 1 - self.chip, self.chip)[flow]
        return (far >= 1) & (far <= step)

    def sends(self, flow, step):
        far = (self.chips - 1 - self.chip, self.chip)[flow]
        return far <= step - 1

    def piece(self, flow, step):
        return self.chip + (step - self.chips + 1, self.chips - 1 - step)[flow]

    def open(self, step):
        for flow in range(2):
            piece = (step - 1, self.chips - step)[flow]

            @pl.when(self.ends(flow))
            def _(flow=flow, piece=piece):
                self.each_chunk(
                    lambda chunk: self.hop(
                        flow, step, chunk, self.merged.at[piece, chunk]
                    ).start()
                )

    def relay(self, step):
        def one(chunk):
            for flow in range(2):

                @pl.when(self.receives(flow, step))
                def _(flow=flow):
                    self.landed(flow, step, chunk).wait_recv()
                    held = self.flows[flow]
                    held[step - 1, chunk] = (
                        held[step - 1, chunk].astype(F32)
                        + self.merged[self.piece(flow, step), chunk].astype(F32)
                    ).astype(BF16)
                    self.hop(flow, step + 1, chunk, held.at[step - 1, chunk]).start()

        self.each_chunk(one)

    def total(self, out, chunk):
        step = self.chips - 1
        out[chunk] = self.merged[self.chip, chunk].astype(F32)
        for flow in range(2):

            @pl.when(self.receives(flow, step))
            def _(flow=flow):
                self.landed(flow, step, chunk).wait_recv()
                out[chunk] += self.flows[flow][step - 1, chunk].astype(F32)

    def finish(self):
        for piece in range(self.chips):
            self.core_copy(piece).wait_send()
        for flow in range(2):
            for step in range(1, self.chips):

                @pl.when(self.sends(flow, step))
                def _(flow=flow, step=step):
                    self.each_chunk(lambda chunk: self.landed(flow, step, chunk).wait_send())


class Across:
    def __init__(self, source, landing, sems):
        self.source, self.landing, self.sems = source, landing, sems
        self.me = lax.axis_index("dp")

    def copy(self, chunk, slot):
        return pltpu.make_async_remote_copy(
            src_ref=self.source.at[chunk], dst_ref=self.landing.at[slot],
            send_sem=self.sems.at[0, chunk], recv_sem=self.sems.at[1, slot],
            device_id={"dp": chunk}, device_id_type=MESH_IDS,
        )

    def send(self, chunk):
        @pl.when(self.me != chunk)
        def _():
            self.copy(chunk, self.me).start()

        @pl.when(self.me == chunk)
        def _():
            self.landing[chunk] = self.source[chunk]

    def receive(self, slot):
        @pl.when(self.me != slot)
        def _():
            self.copy(slot, slot).wait_recv()

    def finish(self, chunk):
        @pl.when(self.me != chunk)
        def _():
            self.copy(chunk, self.me).wait_send()


def last_kernel(
    fsdp, first_ref, params_ref, small_ref, up_ref, output_any, tokens_any, hidden_any, grad_any,
    qkv_ref, out_ref, tokens_out, output_out, small_out, qkv_out, out_out, up_out, landing,
    passing, last, held, small_landing, sums, output_ref, tokens_ref, hidden_ref, grad_ref,
    qkv_own, qkv_merged, qkv_down, qkv_up, out_own, out_merged, out_down, out_up, qkv_total,
    qkv_low, qkv_in, up_in, copy_sems, qkv_own_sems, out_own_sems, qkv_sems, out_sems,
    across_sems, sems, small_sems,
):
    copies = [
        pltpu.make_async_copy(source, target, copy_sems.at[k])
        for k, (source, target) in enumerate((
            (output_any, output_ref), (tokens_any, tokens_ref), (hidden_any, hidden_ref),
            (grad_any, grad_ref),
        ))
    ]
    near, partners = neighbours(fsdp, True)
    dp, part = qkv_ref.shape[0], qkv_ref.shape[3] // 3
    chips = fsdp // 2
    lines = (
        LineSum(qkv_ref, qkv_own, qkv_merged, qkv_down, qkv_up, qkv_own_sems, qkv_sems, fsdp),
        LineSum(out_ref, out_own, out_merged, out_down, out_up, out_own_sems, out_sems, fsdp),
    )
    up_across = Across(up_ref, up_in, across_sems.at[0])
    qkv_across = Across(qkv_low, qkv_in, across_sems.at[1])
    small = Doubling(held, small_landing, small_sems, partners, sum_or_top)
    first, second = (
        Scatter(ref, landing.at[k], passing.at[k], last.at[k], sems.at[k], near)
        for k, ref in enumerate((first_ref, output_ref))
    )

    def first_rows(path, step):
        rows = first.own(path, step)
        total = first.total(path, step)
        normed, inverse_std = row_norm(tokens_ref[rows].astype(F32))
        grad = grad_ref[rows] + row_back(total, normed, inverse_std, params_ref[0:1])
        tokens_out[rows] = grad.astype(BF16)
        add_sums(sums, (total * normed, total), 2)

    def second_rows(path, step):
        rows = second.own(path, step)
        total = second.total(path, step)
        output_out[rows] = (hidden_ref[rows] + total + params_ref[1:2]).astype(BF16)

    def paths(act):
        each_step(lambda step: [act(path, step) for path in range(2)])

    paths(first.begin)
    for line in lines:
        line.begin()
    for copy in copies:
        copy.start()
    sums[...] = jnp.zeros_like(sums)
    for line in lines:
        line.merge()
    for step in range(1, chips):
        for line in lines:
            line.open(step)
    for copy in copies:
        copy.wait()
    paths(first.relay)
    paths(second.begin)
    for line in lines:
        line.relay(1)
    paths(first_rows)
    held[0, :8] = small_ref[:8]
    held[0, 8:] = small_ref[8:] + sums[...]
    small.start(0)
    paths(second.relay)
    small.end(0)
    small.start(1)
    for chunk in range(dp):
        up_across.send(chunk)
    for step in range(2, chips - 1):
        for line in lines:
            line.relay(step)
    small.end(1)
    small.start(2)
    paths(second_rows)
    small.end(2)
    small.start(3)
    for chunk in range(dp):
        lines[0].total(qkv_total, chunk)
        qkv_low[chunk] = qkv_total[chunk].astype(BF16)
        qkv_across.send(chunk)
    small.end(3)
    small.start(4)
    lines[1].total(out_out, 0)
    columns = up_ref.shape[2]
    for slot in range(dp):
        up_across.receive(slot)
        up_out[:, slot * columns : (slot + 1) * columns] = up_in[slot].astype(F32)
    small.end(4)
    small_out[...] = held[len(partners)]
    for slot in range(dp):
        qkv_across.receive(slot)
        for third in range(3):
            start = (third * dp + slot) * part
            qkv_out[:, start : start + part] = qkv_in[
                slot, :, third * part : (third + 1) * part
            ].astype(F32)
    paths(first.finish)
    paths(second.finish)
    for line in lines:
        line.finish()
    for chunk in range(dp):
        up_across.finish(chunk)
        qkv_across.finish(chunk)


def call_exchange(kernel, number, jobs, scatters, outs, args, extra=(), stages=0, unplaced=0):
    rows, width = args[0].shape if scatters else (4 * args[0].shape[0], args[0].shape[1])
    own = rows // 4
    room = []
    if scatters == 1:
        room = [(2, own, width), (own, width), (own, width)]
    if scatters == 2:
        room = [(2, 2, own, width), (2, own, width), (2, own, width)]
    return pl.pallas_call(
        kernel,
        in_specs=[pl.BlockSpec(memory_space=pltpu.VMEM)] * (len(args) - unplaced)
        + [pl.BlockSpec(memory_space=pl.ANY)] * unplaced,
        out_specs=[pl.BlockSpec(memory_space=pltpu.VMEM)] * len(outs),
        out_shape=[jax.ShapeDtypeStruct(shape, dtype) for shape, dtype in outs],
        scratch_shapes=[
            *(pltpu.VMEM(shape, BF16) for shape in room),
            *extra,
            pltpu.SemaphoreType.DMA((jobs, 2, 6 * STEPS)),
            *([pltpu.SemaphoreType.DMA(stages)] if stages else []),
        ],
        compiler_params=pltpu.CompilerParams(
            collective_id=number, has_side_effects=True, vmem_limit_bytes=60 << 20
        ),
        cost_estimate=pl.CostEstimate(
            flops=rows * width, bytes_accessed=200 << 20, transcendentals=0
        ),
    )(*args)


def pair_span(offset, pair):
    return pl.ds(offset + pair * 2 * HEAD_DIM, 2 * HEAD_DIM)


def head_parts(ref, offset, pair):
    both = ref[:, pair_span(offset, pair)]
    return both[:, :HEAD_DIM], both[:, HEAD_DIM:]


def dot_nt(a, b):
    return lax.dot_general(a, b, (((1,), (1,)), ((), ())), preferred_element_type=F32)


def dot_tn(a, b):
    return lax.dot_general(a, b, (((0,), (0,)), ((), ())), preferred_element_type=F32)


def attend_kernel(slope_ref, distance_ref, qkv_ref, mixed_ref, top_ref):
    width = mixed_ref.shape[1]
    lane = lax.broadcasted_iota(jnp.int32, (8, 128), 1)

    distance = distance_ref[...]
    tops = jnp.zeros((8, 128), F32)
    for pair in range(width // HEAD_DIM // 2):
        outs = []
        for t, (q, k, v) in enumerate(
            zip(*(head_parts(qkv_ref, part * width, pair) for part in range(3)))
        ):
            logits = dot_nt(q * jnp.asarray(SCALE, BF16), k)
            head_top = jnp.max(jnp.where(distance < MASKED, logits, -1e30))
            tops = jnp.where(lane == pair * 2 + t, head_top, tops)
            scores = logits - slope_ref[pair * 2 + t] * distance
            expos = jnp.exp(scores - jnp.max(scores, axis=-1, keepdims=True))
            probs = expos * (1.0 / jnp.sum(expos, axis=-1, keepdims=True))
            outs.append(jnp.dot(probs.astype(BF16), v, preferred_element_type=F32))
        mixed_ref[:, pair_span(0, pair)] = jnp.concatenate(outs, 1).astype(BF16)
    top_ref[...] = tops


def attend_back_kernel(slope_ref, distance_ref, qkv_ref, grad_ref, out_ref):
    width = grad_ref.shape[1]

    distance = distance_ref[...]
    for pair in range(width // HEAD_DIM // 2):
        outs = ([], [], [])
        parts = [head_parts(qkv_ref, part * width, pair) for part in range(3)]
        parts.append(head_parts(grad_ref, 0, pair))
        for t, (q, k, v, grad) in enumerate(zip(*parts)):
            low_q = q * jnp.asarray(SCALE, BF16)
            scores = dot_nt(low_q, k) - slope_ref[pair * 2 + t] * distance
            expos = jnp.exp(scores - jnp.max(scores, axis=-1, keepdims=True))
            probs = expos * (1.0 / jnp.sum(expos, axis=-1, keepdims=True))
            outs[2].append(dot_tn(probs.astype(BF16), grad))
            grad_probs = dot_nt(grad, v)
            inner = jnp.sum(grad_probs * probs, axis=-1, keepdims=True)
            grad_scores = (probs * (grad_probs - inner)).astype(BF16)
            outs[0].append(jnp.dot(grad_scores, k, preferred_element_type=F32) * SCALE)
            outs[1].append(dot_tn(grad_scores, low_q))
        for part in range(3):
            out_ref[:, pair_span(part * width, pair)] = jnp.concatenate(outs[part], 1).astype(BF16)


def attend(slopes, distance, qkv, length):
    rows, width = qkv.shape[0], qkv.shape[1] // 3
    blocks = rows // length
    mixed, tops = pl.pallas_call(
        attend_kernel,
        grid=(blocks,),
        in_specs=[
            pl.BlockSpec(memory_space=pltpu.SMEM),
            pl.BlockSpec((length, length), lambda b: (0, 0)),
            pl.BlockSpec((length, 3 * width), lambda b: (b, 0)),
        ],
        out_specs=[
            pl.BlockSpec((length, width), lambda b: (b, 0)),
            pl.BlockSpec((8, 128), lambda b: (b, 0)),
        ],
        out_shape=[
            jax.ShapeDtypeStruct((rows, width), BF16),
            jax.ShapeDtypeStruct((blocks * 8, 128), F32),
        ],
        cost_estimate=pl.CostEstimate(
            flops=4 * rows * length * width, bytes_accessed=8 * rows * width,
            transcendentals=rows * length * width // HEAD_DIM,
        ),
        name="attend",
    )(slopes, distance, qkv)
    return mixed, jnp.max(tops, axis=0)[: width // HEAD_DIM]


def attend_back(slopes, distance, qkv, grad, length):
    rows, width = grad.shape
    return pl.pallas_call(
        attend_back_kernel,
        grid=(rows // length,),
        in_specs=[
            pl.BlockSpec(memory_space=pltpu.SMEM),
            pl.BlockSpec((length, length), lambda b: (0, 0)),
            pl.BlockSpec((length, 3 * width), lambda b: (b, 0)),
            pl.BlockSpec((length, width), lambda b: (b, 0)),
        ],
        out_specs=pl.BlockSpec((length, 3 * width), lambda b: (b, 0)),
        out_shape=jax.ShapeDtypeStruct((rows, 3 * width), BF16),
        cost_estimate=pl.CostEstimate(
            flops=10 * rows * length * width, bytes_accessed=14 * rows * width,
            transcendentals=rows * length * width // HEAD_DIM,
        ),
        name="attend_back",
    )(slopes, distance, qkv, grad)


def norm_stats(values):
    row_mean = jnp.mean(values, axis=-1, keepdims=True)
    centred = values - row_mean
    inverse_std = lax.rsqrt(jnp.mean(centred * centred, axis=-1, keepdims=True) + EPS)
    return centred * inverse_std, inverse_std


def norm_back(grad_norm, normed, inverse_std, gain):
    scaled = grad_norm * gain
    return inverse_std * (
        scaled
        - jnp.mean(scaled, axis=-1, keepdims=True)
        - normed * jnp.mean(scaled * normed, axis=-1, keepdims=True)
    )


def dot(a, b):
    return jnp.dot(a, b, preferred_element_type=F32)


def layer(
    dp, fsdp, tokens, seq_lengths, w_qkv, bias_q, bias_v, w_out, bias_out, ln1_gain, ln1_bias,
    w_up, bias_up, w_down, bias_down, ln2_gain, ln2_bias, cotangent,
):
    length, width = tokens.shape
    shard = w_qkv.shape[0]
    ff = w_up.shape[1]
    heads = width // HEAD_DIM
    part, ff_part = width // dp, ff // dp
    local_heads = heads // dp
    spot, place = lax.axis_index("dp"), lax.axis_index("fsdp")
    rank = spot * fsdp + place
    both = (("fsdp", fsdp), ("dp", dp))

    out_w = lax.all_gather(w_out, "fsdp", axis=0, tiled=True)
    cols = w_qkv.reshape(shard, 3, dp, part).transpose(0, 2, 1, 3).reshape(shard, 3 * width)
    cols = lax.all_to_all(cols, "dp", 1, 0, tiled=True).reshape(dp, shard, 3 * part)
    qkv_w = lax.all_gather(cols, "fsdp", axis=1, tiled=True).reshape(width, 3 * part)
    w_up, cols = lax.optimization_barrier((w_up, cols))
    ups = lax.all_to_all(w_up, "dp", 1, 0, tiled=True).reshape(dp, shard, ff_part)
    up_w = lax.all_gather(ups, "fsdp", axis=1, tiled=True).reshape(width, ff_part)
    down_w = lax.all_gather(w_down, "fsdp", axis=0, tiled=True)
    late_tokens, _ = lax.optimization_barrier((tokens, ups))

    full_small = (bias_out, ln1_gain, ln1_bias, bias_down, ln2_gain, ln2_bias)
    row = jnp.concatenate(full_small + (bias_q, bias_v, bias_up))[None]
    table = jnp.zeros((dp * fsdp, row.shape[1]), BF16)
    table = lax.dynamic_update_slice(table, row, (rank, 0))
    wide = (4 * length, width)
    narrow = (length, width)
    kernels = dp == 4 and fsdp == 8 and length % (32 * STEPS) == 0 and ff == dp * width
    stages = len(bits_of(fsdp)) + 2
    if kernels:
        all_tokens, grad_y, table = call_exchange(
            functools.partial(gather_two_kernel, fsdp), 1, 2, 0,
            [(wide, BF16), (wide, BF16), (table.shape, BF16)], [late_tokens, cotangent, table],
            (pltpu.VMEM((stages + 1,) + table.shape, BF16), pltpu.VMEM((stages,) + table.shape, BF16)),
            (2, stages),
        )
    else:
        all_tokens, grad_y = gather_dp(late_tokens, dp), gather_dp(cotangent, dp)
        table = combine_all(table, both, jnp.add)
    table = table.astype(F32)
    small = [table[:, k * shard : (k + 1) * shard].reshape(1, width) for k in range(6)]
    out_b, gain1, shift1, down_b, gain2, shift2 = small
    mine = lax.dynamic_slice(table, (spot * fsdp, 0), (fsdp, row.shape[1]))[:, 6 * shard :]
    q_b, v_b = mine[:, :shard].reshape(1, part), mine[:, shard : 2 * shard].reshape(1, part)
    up_b = mine[:, 2 * shard :].reshape(1, ff_part)

    ranks = (spot * local_heads + 1 + jnp.arange(local_heads)).astype(F32)
    slopes = jnp.exp2(-8.0 * ranks / heads) * SCALE
    places = jnp.arange(length, dtype=jnp.int32)
    gap = places[:, None] - places[None, :]
    distance = jnp.where(gap >= 0, gap.astype(F32), MASKED)

    inputs = tokens.astype(F32)
    normed_all, _ = norm_stats(all_tokens.astype(F32))
    first_in = (normed_all * gain1 + shift1).astype(BF16)
    biases = jnp.concatenate([q_b, jnp.zeros_like(q_b), v_b], 1)
    qkv = (dot(first_in, qkv_w) + biases).astype(BF16)
    mixed, tops = attend(slopes, distance, qkv, length)
    out_part = dot(mixed, out_w).astype(BF16)
    if kernels:
        second_in, hidden = call_exchange(
            hidden_kernel, 2, 2, 1, [(wide, BF16), (narrow, F32)],
            [out_part, tokens, jnp.concatenate([out_b, gain2, shift2], 0)],
        )
    else:
        hidden = inputs + scatter_dp(out_part, dp) + out_b
        normed2, inverse2 = norm_stats(hidden)
        second_in = gather_dp((normed2 * gain2 + shift2).astype(BF16), dp)

    upward = dot(second_in, up_w) + up_b
    cumulative = 0.5 * (1.0 + lax.erf(upward * (0.5**0.5)))
    active = (upward * cumulative).astype(BF16)
    slope = cumulative + upward * jnp.exp(-0.5 * upward * upward) * ((0.5 / jnp.pi) ** 0.5)
    active, slope = lax.optimization_barrier((active, slope.astype(BF16)))

    def reduce_rows(grad):
        return lax.psum_scatter(grad, "fsdp", scatter_dimension=0, tiled=True).astype(F32)

    def reduce_columns(grad):
        grad = grad.reshape(dp, fsdp * shard, grad.shape[1])
        return lax.psum_scatter(grad, "fsdp", scatter_dimension=1, tiled=True)

    def exchange_columns(grad):
        return lax.all_to_all(
            grad.reshape(dp * shard, grad.shape[2]), "dp", 0, 1, tiled=True
        ).astype(F32)

    local_down = dot_tn(active, grad_y).astype(BF16)
    late_y, slope, _ = lax.optimization_barrier((grad_y, slope, local_down))
    grad_upward = (dot_nt(late_y, down_w) * slope).astype(BF16)
    grad_w_down = reduce_rows(local_down)
    local_up = dot_tn(second_in, grad_upward).astype(BF16)
    late_upward, _ = lax.optimization_barrier((grad_upward, local_up))
    second_part = dot_nt(late_upward, up_w).astype(BF16)
    scattered_up = reduce_columns(local_up)
    if kernels:
        branch_all, grad_hidden, branch_sums, output_part = call_exchange(
            branch_kernel, 3, 2, 1,
            [(wide, BF16), (narrow, F32), ((8, width), F32), (wide, BF16)],
            [second_part, hidden, cotangent, jnp.concatenate([out_b, gain2], 0), active, down_w],
            (pltpu.VMEM(active.shape, BF16), pltpu.VMEM(down_w.shape, BF16),
             pltpu.SemaphoreType.DMA((2,))),
            unplaced=2,
        )
    else:
        grad_second = scatter_dp(second_part, dp)
        grad_hidden = cotangent.astype(F32) + norm_back(grad_second, normed2, inverse2, gain2)
        grad_branch = grad_hidden.astype(BF16)
        branch_all = gather_dp(grad_branch, dp)
        branch_sums = jnp.stack([
            jnp.sum(piece, axis=0)
            for piece in (
                cotangent.astype(F32), grad_second * normed2, grad_second,
                grad_branch.astype(F32),
            )
        ])

    grad_mixed = dot_nt(branch_all, out_w).astype(BF16)
    grad_proj = attend_back(slopes, distance, qkv, grad_mixed, length)
    local_qkv = dot_tn(first_in, grad_proj).astype(BF16)
    late_branch, late_proj, _ = lax.optimization_barrier((branch_all, grad_proj, local_qkv))
    local_out = dot_tn(mixed, late_branch).astype(BF16)
    if not kernels:
        grad_w_qkv = exchange_columns(reduce_columns(local_qkv))
        grad_w_qkv = (
            grad_w_qkv.reshape(shard, dp, 3, part).transpose(0, 2, 1, 3).reshape(shard, 3 * width)
        )
        grad_w_out = reduce_rows(local_out)
    first_part = dot_nt(late_proj, qkv_w).astype(BF16)
    if not kernels:
        output_part = dot(active, down_w).astype(BF16)

    def spread(piece, size, fill=0.0):
        return lax.dynamic_update_slice(
            jnp.full((size,), fill, F32), piece, (spot * piece.shape[0],)
        )

    up_sum = jnp.sum(grad_upward.astype(F32), axis=0)
    q_sum = jnp.sum(grad_proj[:, :part].astype(F32), axis=0)
    v_sum = jnp.sum(grad_proj[:, 2 * part :].astype(F32), axis=0)
    if kernels:
        small = jnp.concatenate([
            branch_sums[:4].reshape(4 * width), spread(up_sum, ff), spread(q_sum, width),
            spread(v_sum, width), jnp.zeros((5 * width,), F32), spread(tops, width, -1e30),
        ]).reshape(-1, width)

        def room(grad):
            chips, piece = fsdp // 2, (grad.shape[0],) + grad.shape[2:]
            return tuple(
                pltpu.VMEM((count,) + piece, BF16) for count in (chips, chips, chips - 1, chips - 1)
            )

        def line_sems(grad):
            chips = fsdp // 2
            return pltpu.SemaphoreType.DMA((2, chips + 2 * (chips - 1) * grad.shape[0]))

        qkv_grad = local_qkv.reshape(dp, fsdp, shard, 3 * part)
        out_grad = local_out.reshape(1, fsdp, shard, width)
        grad_tokens, output, small, grad_w_qkv, grad_w_out, grad_w_up = call_exchange(
            functools.partial(last_kernel, fsdp), 4, 2, 2,
            [(narrow, BF16), (narrow, BF16), (small.shape, F32), (w_qkv.shape, F32),
             ((1, shard, width), F32), (w_up.shape, F32)],
            [first_part, jnp.concatenate([gain1, down_b], 0), small,
             scattered_up.reshape(dp, shard, ff_part), output_part, tokens, hidden, grad_hidden,
             qkv_grad, out_grad],
            (
                pltpu.VMEM((stages + 1,) + small.shape, F32),
                pltpu.VMEM((stages,) + small.shape, F32), pltpu.VMEM((8, width), F32),
                pltpu.VMEM(wide, BF16), pltpu.VMEM(narrow, BF16), pltpu.VMEM(narrow, F32),
                pltpu.VMEM(narrow, F32),
                *room(qkv_grad), *room(out_grad),
                pltpu.VMEM((dp, shard, 3 * part), F32), pltpu.VMEM((dp, shard, 3 * part), BF16),
                pltpu.VMEM((dp, shard, 3 * part), BF16), pltpu.VMEM((dp, shard, ff_part), BF16),
                pltpu.SemaphoreType.DMA((4,)), pltpu.SemaphoreType.DMA((fsdp // 2,)),
                pltpu.SemaphoreType.DMA((fsdp // 2,)), line_sems(qkv_grad), line_sems(out_grad),
                pltpu.SemaphoreType.DMA((2, 2, dp)),
            ),
            (2, stages), 6,
        )
        grad_w_out = grad_w_out[0]
    else:
        grad_first = scatter_dp(first_part, dp)
        normed1, inverse1 = norm_stats(inputs)
        grad_tokens = grad_hidden + norm_back(grad_first, normed1, inverse1, gain1)
        output = hidden + scatter_dp(output_part, dp) + down_b
        sums = (jnp.sum(grad_first * normed1, axis=0), jnp.sum(grad_first, axis=0))
        small = jnp.concatenate([
            branch_sums[:4].reshape(4 * width), spread(up_sum, ff), spread(q_sum, width),
            spread(v_sum, width), *sums, jnp.zeros((3 * width,), F32), spread(tops, width, -1e30),
        ]).reshape(-1, width)
        grad_w_up = exchange_columns(scattered_up)
        small = combine_all(small, both, sum_or_top)
    ups_at = 4 + ff // width
    owned = lax.dynamic_slice(small, (0, rank * shard), (small.shape[0], shard))
    ff_shard = ff // (dp * fsdp)
    owned_up = lax.dynamic_slice(
        small[4:ups_at].reshape(ff), (rank * ff_shard,), (ff_shard,)
    )

    head_top = small[-1, :heads]
    factor = jnp.sqrt(CLIP_TAU / jnp.maximum(head_top, CLIP_TAU))
    column = jnp.repeat(factor, HEAD_DIM)
    columns = jnp.concatenate([column, column, jnp.ones((width,), F32)])
    clipped = (w_qkv.astype(F32) * columns[None, :]).astype(BF16)
    return (
        output.astype(BF16),
        grad_tokens.astype(BF16),
        grad_w_qkv,
        owned[ups_at],
        owned[ups_at + 1],
        grad_w_out,
        owned[3],
        owned[ups_at + 2],
        owned[ups_at + 3],
        grad_w_up,
        owned_up,
        grad_w_down,
        owned[0],
        owned[1],
        owned[2],
        clipped,
    )


def solution(mesh):
    rows, flat = P(("dp", "fsdp"), None), P(("dp", "fsdp"))
    return jax.shard_map(
        functools.partial(layer, mesh.shape["dp"], mesh.shape["fsdp"]),
        mesh=mesh,
        in_specs=(
            rows, flat, rows, flat, flat, rows, flat, flat, flat, rows, flat, rows, flat, flat,
            flat, rows,
        ),
        out_specs=(
            rows, rows, rows, flat, flat, rows, flat, flat, flat, rows, flat, rows, flat, flat,
            flat, rows,
        ),
        check_vma=False,
    )
```

```python
import functools

import jax
import jax.numpy as jnp
from jax import lax
from jax.experimental import pallas as pl
from jax.experimental.pallas import tpu as pltpu
from jax.sharding import PartitionSpec as P


HEAD_DIM = 64
EPS = 1e-05
CLIP_TAU = 5.0
MASKED = 1e35
F32 = jnp.float32
BF16 = jnp.bfloat16
SCALE = HEAD_DIM ** (-0.5)


def swap(value, axis, size, bit):
    return lax.ppermute(value, axis, [(i, i ^ bit) for i in range(size)])


def bits_of(size):
    return [1 << b for b in range(size.bit_length() - 1)]


def gather_path(block, size, bits):
    blocks = {0: block}
    for bit in bits:
        held = sorted(blocks)
        moved = swap(jnp.concatenate([blocks[r] for r in held], 0), "dp", size, bit)
        for place, r in enumerate(held):
            rows = block.shape[0]
            blocks[r ^ bit] = moved[place * rows : (place + 1) * rows]
    return blocks


def gather_dp(block, size):
    half = block.shape[0] // 2
    top = gather_path(block[:half], size, bits_of(size))
    low = gather_path(block[half:], size, bits_of(size)[::-1])
    parts = []
    for r in range(size):
        parts += [top[r], low[r]]
    return jnp.concatenate(parts, 0)


def scatter_path(blocks, size, bits):
    blocks = dict(blocks)
    for bit in bits:
        away = sorted(r for r in blocks if r & bit)
        rows = blocks[0].shape[0]
        sent = jnp.concatenate([blocks[r].astype(BF16) for r in away], 0)
        moved = swap(sent, "dp", size, bit)
        blocks = {
            r ^ bit: blocks[r ^ bit].astype(F32)
            + moved[place * rows : (place + 1) * rows].astype(F32)
            for place, r in enumerate(away)
        }
    return blocks[0]


def scatter_dp(partial, size):
    rows = partial.shape[0] // size
    half = rows // 2
    top = {r: partial[r * rows : r * rows + half] for r in range(size)}
    low = {r: partial[r * rows + half : (r + 1) * rows] for r in range(size)}
    return jnp.concatenate(
        [scatter_path(top, size, bits_of(size)), scatter_path(low, size, bits_of(size)[::-1])], 0
    )


def combine_all(value, sizes, join):
    for axis, size in sizes:
        for bit in bits_of(size):
            value = join(value, swap(value, axis, size, bit))
    return value


STEPS = 4
MESH_IDS = pl.DeviceIdType.MESH
PATHS = ((1, 2), (2, 1))


def flipped(axis, mask):
    me = lax.axis_index(axis)
    there = me
    for bit in bits_of(2 ** mask.bit_length()):
        if mask & bit:
            there = there + bit - 2 * bit * ((me // bit) % 2)
    return {axis: there}


def neighbours(fsdp=1, every=False):
    near = {bit: flipped("dp", bit) for bit in (1, 2)}
    partners = [near[1], near[2]] + [flipped("fsdp", bit) for bit in bits_of(fsdp)]
    greeted = partners if fsdp > 1 else [near[1], near[2]]
    if every:
        greeted = [flipped("dp", mask) for mask in (1, 2, 3)]
        greeted += [flipped("fsdp", mask) for mask in range(1, fsdp)]
    barrier = pltpu.get_barrier_semaphore()
    for where in greeted:
        pl.semaphore_signal(barrier, inc=1, device_id=where, device_id_type=MESH_IDS)
    pl.semaphore_wait(barrier, len(greeted))
    return near, partners


def remote(source, target, sems, index, where):
    return pltpu.make_async_remote_copy(
        src_ref=source, dst_ref=target, send_sem=sems.at[0, index], recv_sem=sems.at[1, index],
        device_id=where, device_id_type=MESH_IDS,
    )


def each_step(act):
    def run(step, carry):
        act(step)
        return carry

    lax.fori_loop(0, STEPS, run, 0)


class Gather:
    def __init__(self, out, sems, near):
        self.out, self.sems, self.near = out, sems, near
        self.rows = out.shape[0] // 4
        self.step_rows = self.rows // 2 // STEPS

    def span(self, block, path, step):
        start = block * self.rows + path * (self.rows // 2) + step * self.step_rows
        return pl.ds(pl.multiple_of(start, self.step_rows), self.step_rows)

    def copy(self, source, bit, path, step, kind):
        return remote(
            self.out.at[self.span(source, path, step)],
            self.out.at[self.span(source + bit, path, step)],
            self.sems, (path * 3 + kind) * STEPS + step, self.near[bit],
        )

    def send(self, path, step):
        first, second = PATHS[path]
        self.copy(0, first, path, step, 0).start()
        self.copy(0, second, path, step, 1).start()

    def forward(self, path, step):
        first, second = PATHS[path]
        self.copy(0, first, path, step, 0).wait_recv()
        self.copy(first, second, path, step, 2).start()

    def finish(self, path, step):
        first, second = PATHS[path]
        self.copy(0, first, path, step, 0).wait_send()
        self.copy(0, second, path, step, 1).wait()
        self.copy(first, second, path, step, 2).wait()


class Scatter:
    def __init__(self, partial, landing, passing, last, sems, near):
        self.partial, self.landing, self.passing, self.last = partial, landing, passing, last
        self.sems, self.near = sems, near
        self.rows = partial.shape[0] // 4
        self.step_rows = self.rows // 2 // STEPS

    def span(self, block, path, step):
        start = block * self.rows + path * (self.rows // 2) + step * self.step_rows
        return pl.ds(pl.multiple_of(start, self.step_rows), self.step_rows)

    def own(self, path, step):
        return self.span(0, path, step)

    def opening(self, path, step, kind):
        first, _ = PATHS[path]
        return remote(
            self.partial.at[self.span((first, 3)[kind], path, step)],
            self.landing.at[kind, self.own(path, step)],
            self.sems, (path * 3 + kind) * STEPS + step, self.near[first],
        )

    def closing(self, path, step):
        rows = self.own(path, step)
        return remote(
            self.passing.at[rows], self.last.at[rows], self.sems,
            (path * 3 + 2) * STEPS + step, self.near[PATHS[path][1]],
        )

    def begin(self, path, step):
        for kind in range(2):
            self.opening(path, step, kind).start()

    def relay(self, path, step):
        _, second = PATHS[path]
        self.opening(path, step, 1).wait_recv()
        rows = self.own(path, step)
        self.passing[rows] = (
            self.partial[self.span(second, path, step)].astype(F32)
            + self.landing[1, rows].astype(F32)
        ).astype(BF16)
        self.closing(path, step).start()

    def total(self, path, step):
        self.opening(path, step, 0).wait_recv()
        self.closing(path, step).wait_recv()
        rows = self.own(path, step)
        return (
            self.partial[self.span(0, path, step)].astype(F32)
            + self.landing[0, rows].astype(F32)
            + self.last[rows].astype(F32)
        )

    def finish(self, path, step):
        for kind in range(2):
            self.opening(path, step, kind).wait_send()
        self.closing(path, step).wait_send()


def regroup(values, outer, inner):
    piece = values.shape[1] // (outer * inner)
    starts = [(o * inner + i) * piece for i in range(inner) for o in range(outer)]
    return jnp.concatenate([values[:, start : start + piece] for start in starts], 1)


def row_norm(values):
    centred = values - jnp.mean(values, axis=-1, keepdims=True)
    inverse_std = lax.rsqrt(jnp.mean(centred * centred, axis=-1, keepdims=True) + EPS)
    return centred * inverse_std, inverse_std


def row_back(grad_norm, normed, inverse_std, gain):
    scaled = grad_norm * gain
    return inverse_std * (
        scaled
        - jnp.mean(scaled, axis=-1, keepdims=True)
        - normed * jnp.mean(scaled * normed, axis=-1, keepdims=True)
    )


class Doubling:
    def __init__(self, held, landing, sems, partners, join):
        self.held, self.landing, self.sems = held, landing, sems
        self.partners, self.join = partners, join

    def copy(self, stage):
        return remote(
            self.held.at[stage], self.landing.at[stage], self.sems, stage, self.partners[stage]
        )

    def start(self, stage):
        self.copy(stage).start()

    def end(self, stage):
        self.copy(stage).wait()
        self.held[stage + 1] = self.join(self.held[stage], self.landing[stage])

    def run(self, *stages):
        for stage in stages:
            self.start(stage)
            self.end(stage)


def gather_two_kernel(
    fsdp, one_ref, two_ref, table_ref, out_one, out_two, table_out, held, landing, sems, small_sems
):
    near, partners = neighbours(fsdp)
    jobs = []
    for k, (source, out) in enumerate(((one_ref, out_one), (two_ref, out_two))):
        out[: source.shape[0]] = source[...]
        jobs.append(Gather(out, sems.at[k], near))
    held[0] = table_ref[...]
    small = Doubling(held, landing, small_sems, partners[2:] + partners[:2], jnp.add)

    def paths(act):
        each_step(lambda step: [act(path, step) for path in range(2)])

    paths(jobs[0].send)
    small.run(*range(len(partners) - 2))
    small.start(len(partners) - 2)
    paths(jobs[0].forward)
    small.end(len(partners) - 2)
    small.start(len(partners) - 1)
    paths(jobs[1].send)
    small.end(len(partners) - 1)
    table_out[...] = held[len(partners)]
    paths(jobs[1].forward)
    for job in jobs:
        paths(job.finish)


def exchange(scatter, gather, rows_of, beside=None):
    each_step(lambda step: [scatter.begin(path, step) for path in range(2)])
    if beside is not None:
        beside()
    each_step(lambda step: [scatter.relay(path, step) for path in range(2)])

    def middle(step):
        for path in range(2):
            rows = scatter.own(path, step)
            gather.out[rows] = rows_of(rows, scatter.total(path, step))
            gather.send(path, step)

        @pl.when(step > 0)
        def _():
            for path in range(2):
                gather.forward(path, step - 1)

    each_step(middle)
    for path in range(2):
        gather.forward(path, STEPS - 1)
    each_step(lambda step: [scatter.finish(path, step) for path in range(2)])
    each_step(lambda step: [gather.finish(path, step) for path in range(2)])


def add_sums(sums_ref, values, start=0):
    for k, value in enumerate(values):
        row = start + k
        sums_ref[row : row + 1] += jnp.sum(value, axis=0, keepdims=True)


def hidden_kernel(
    fsdp, partial_ref, tokens_ref, params_ref, out_ref, hidden_ref, landing, passing, last, sems
):
    near, _ = neighbours()

    def rows_of(rows, total):
        hidden = tokens_ref[rows].astype(F32) + total + params_ref[0:1]
        hidden_ref[rows] = hidden
        normed, _ = row_norm(hidden)
        return regroup(normed * params_ref[1:2] + params_ref[2:3], 4, fsdp).astype(BF16)

    exchange(
        Scatter(partial_ref, landing, passing, last, sems.at[0], near),
        Gather(out_ref, sems.at[1], near), rows_of,
    )


def branch_kernel(
    fsdp, partial_ref, hidden_ref, cotangent_ref, params_ref, active_ref, weight_ref, out_ref, grad_ref,
    sums_ref, output_ref, landing, passing, last, active, weight, copy_sems, sems,
):
    copies = [
        pltpu.make_async_copy(active_ref, active, copy_sems.at[0]),
        pltpu.make_async_copy(weight_ref, weight, copy_sems.at[1]),
    ]
    for copy in copies:
        copy.start()
    near, _ = neighbours()
    sums_ref[...] = jnp.zeros_like(sums_ref)

    def rows_of(rows, total):
        total = regroup(total, fsdp, 4)
        normed, inverse_std = row_norm(hidden_ref[rows])
        upper = cotangent_ref[rows].astype(F32)
        grad = upper + row_back(total, normed, inverse_std, params_ref[1:2])
        grad_ref[rows] = grad
        branch = grad.astype(BF16)
        add_sums(sums_ref, (upper, total * normed, total, branch.astype(F32)))
        return branch

    def output_tile(tile, carry):
        columns = pl.ds(pl.multiple_of(tile * 256, 256), 256)
        output_ref[:, columns] = dot(active[...], weight[:, columns]).astype(BF16)
        return carry

    def beside():
        for copy in copies:
            copy.wait()
        lax.fori_loop(0, output_ref.shape[1] // 256, output_tile, 0)

    exchange(
        Scatter(partial_ref, landing, passing, last, sems.at[0], near),
        Gather(out_ref, sems.at[1], near), rows_of, beside,
    )


def sum_or_top(a, b):
    row = lax.broadcasted_iota(jnp.int32, a.shape, 0)
    return jnp.where(row < a.shape[0] - 1, a + b, jnp.maximum(a, b))


class LineSum:
    def __init__(self, grad, own, merged, down, up, own_sems, sems, size):
        self.grad, self.merged, self.flows, self.sems = grad, merged, (down, up), sems
        self.own, self.own_sems = own, own_sems
        self.chips, self.chunks = size // 2, grad.shape[0]
        place = lax.axis_index("fsdp")
        self.chip, self.core = place // 2, place % 2
        self.next = ({"fsdp": place - 2}, {"fsdp": place + 2})

    def core_copy(self, piece):
        return remote(
            self.grad.at[:, piece * 2 + 1 - self.core], self.merged.at[piece], self.sems, piece,
            flipped("fsdp", 1),
        )

    def own_copy(self, piece):
        return pltpu.make_async_copy(
            self.grad.at[:, piece * 2 + self.core], self.own.at[piece], self.own_sems.at[piece]
        )

    def begin(self):
        for piece in range(self.chips):
            self.core_copy(piece).start()
            self.own_copy(piece).start()

    def each_chunk(self, act):
        if self.chunks == 1:
            return act(0)

        def run(chunk, carry):
            act(chunk)
            return carry

        return lax.fori_loop(0, self.chunks, run, 0)

    def merge(self):
        for piece in range(self.chips):
            self.core_copy(piece).wait_recv()
            self.own_copy(piece).wait()

            def add(chunk, piece=piece):
                self.merged[piece, chunk] = (
                    self.merged[piece, chunk].astype(F32)
                    + self.own[piece, chunk].astype(F32)
                ).astype(BF16)

            self.each_chunk(add)

    def hop(self, flow, step, chunk, source):
        index = self.chips + (flow * (self.chips - 1) + step - 1) * self.chunks + chunk
        return remote(
            source, self.flows[flow].at[step - 1, chunk], self.sems, index, self.next[flow]
        )

    def landed(self, flow, step, chunk):
        return self.hop(flow, step, chunk, self.flows[flow].at[step - 1, chunk])

    def ends(self, flow):
        return self.chip == (self.chips - 1, 0)[flow]

    def receives(self, flow, step):
        far = (self.chips - 1 - self.chip, self.chip)[flow]
        return (far >= 1) & (far <= step)

    def sends(self, flow, step):
        far = (self.chips - 1 - self.chip, self.chip)[flow]
        return far <= step - 1

    def piece(self, flow, step):
        return self.chip + (step - self.chips + 1, self.chips - 1 - step)[flow]

    def open(self, step):
        for flow in range(2):
            piece = (step - 1, self.chips - step)[flow]

            @pl.when(self.ends(flow))
            def _(flow=flow, piece=piece):
                self.each_chunk(
                    lambda chunk: self.hop(
                        flow, step, chunk, self.merged.at[piece, chunk]
                    ).start()
                )

    def relay(self, step):
        def one(chunk):
            for flow in range(2):

                @pl.when(self.receives(flow, step))
                def _(flow=flow):
                    self.landed(flow, step, chunk).wait_recv()
                    held = self.flows[flow]
                    held[step - 1, chunk] = (
                        held[step - 1, chunk].astype(F32)
                        + self.merged[self.piece(flow, step), chunk].astype(F32)
                    ).astype(BF16)
                    self.hop(flow, step + 1, chunk, held.at[step - 1, chunk]).start()

        self.each_chunk(one)

    def total(self, out, chunk):
        step = self.chips - 1
        out[chunk] = self.merged[self.chip, chunk].astype(F32)
        for flow in range(2):

            @pl.when(self.receives(flow, step))
            def _(flow=flow):
                self.landed(flow, step, chunk).wait_recv()
                out[chunk] += self.flows[flow][step - 1, chunk].astype(F32)

    def finish(self):
        for piece in range(self.chips):
            self.core_copy(piece).wait_send()
        for flow in range(2):
            for step in range(1, self.chips):

                @pl.when(self.sends(flow, step))
                def _(flow=flow, step=step):
                    self.each_chunk(lambda chunk: self.landed(flow, step, chunk).wait_send())


class Across:
    def __init__(self, source, landing, sems):
        self.source, self.landing, self.sems = source, landing, sems
        self.me = lax.axis_index("dp")

    def copy(self, chunk, slot):
        return pltpu.make_async_remote_copy(
            src_ref=self.source.at[chunk], dst_ref=self.landing.at[slot],
            send_sem=self.sems.at[0, chunk], recv_sem=self.sems.at[1, slot],
            device_id={"dp": chunk}, device_id_type=MESH_IDS,
        )

    def send(self, chunk):
        @pl.when(self.me != chunk)
        def _():
            self.copy(chunk, self.me).start()

        @pl.when(self.me == chunk)
        def _():
            self.landing[chunk] = self.source[chunk]

    def receive(self, slot):
        @pl.when(self.me != slot)
        def _():
            self.copy(slot, slot).wait_recv()

    def finish(self, chunk):
        @pl.when(self.me != chunk)
        def _():
            self.copy(chunk, self.me).wait_send()


def last_kernel(
    fsdp, first_ref, params_ref, small_ref, up_ref, output_any, tokens_any, hidden_any, grad_any,
    qkv_ref, out_ref, tokens_out, output_out, small_out, qkv_out, out_out, up_out, landing,
    passing, last, held, small_landing, sums, output_ref, tokens_ref, hidden_ref, grad_ref,
    qkv_own, qkv_merged, qkv_down, qkv_up, out_own, out_merged, out_down, out_up, qkv_total,
    qkv_low, qkv_in, up_in, copy_sems, qkv_own_sems, out_own_sems, qkv_sems, out_sems,
    across_sems, sems, small_sems,
):
    copies = [
        pltpu.make_async_copy(source, target, copy_sems.at[k])
        for k, (source, target) in enumerate((
            (output_any, output_ref), (tokens_any, tokens_ref), (hidden_any, hidden_ref),
            (grad_any, grad_ref),
        ))
    ]
    near, partners = neighbours(fsdp, True)
    dp, part = qkv_ref.shape[0], qkv_ref.shape[3] // 3
    chips = fsdp // 2
    lines = (
        LineSum(qkv_ref, qkv_own, qkv_merged, qkv_down, qkv_up, qkv_own_sems, qkv_sems, fsdp),
        LineSum(out_ref, out_own, out_merged, out_down, out_up, out_own_sems, out_sems, fsdp),
    )
    up_across = Across(up_ref, up_in, across_sems.at[0])
    qkv_across = Across(qkv_low, qkv_in, across_sems.at[1])
    small = Doubling(held, small_landing, small_sems, partners, sum_or_top)
    first, second = (
        Scatter(ref, landing.at[k], passing.at[k], last.at[k], sems.at[k], near)
        for k, ref in enumerate((first_ref, output_ref))
    )

    def first_rows(path, step):
        rows = first.own(path, step)
        total = first.total(path, step)
        normed, inverse_std = row_norm(tokens_ref[rows].astype(F32))
        grad = grad_ref[rows] + row_back(total, normed, inverse_std, params_ref[0:1])
        tokens_out[rows] = grad.astype(BF16)
        add_sums(sums, (total * normed, total), 2)

    def second_rows(path, step):
        rows = second.own(path, step)
        total = second.total(path, step)
        output_out[rows] = (hidden_ref[rows] + total + params_ref[1:2]).astype(BF16)

    def paths(act):
        each_step(lambda step: [act(path, step) for path in range(2)])

    paths(first.begin)
    for line in lines:
        line.begin()
    for copy in copies:
        copy.start()
    sums[...] = jnp.zeros_like(sums)
    for line in lines:
        line.merge()
    for step in range(1, chips):
        for line in lines:
            line.open(step)
    for copy in copies:
        copy.wait()
    paths(first.relay)
    paths(second.begin)
    for line in lines:
        line.relay(1)
    paths(first_rows)
    held[0, :8] = small_ref[:8]
    held[0, 8:] = small_ref[8:] + sums[...]
    small.start(0)
    paths(second.relay)
    small.end(0)
    small.start(1)
    for chunk in range(dp):
        up_across.send(chunk)
    for step in range(2, chips - 1):
        for line in lines:
            line.relay(step)
    small.end(1)
    small.start(2)
    paths(second_rows)
    small.end(2)
    small.start(3)
    for chunk in range(dp):
        lines[0].total(qkv_total, chunk)
        qkv_low[chunk] = qkv_total[chunk].astype(BF16)
        qkv_across.send(chunk)
    small.end(3)
    small.start(4)
    lines[1].total(out_out, 0)
    columns = up_ref.shape[2]
    for slot in range(dp):
        up_across.receive(slot)
        up_out[:, slot * columns : (slot + 1) * columns] = up_in[slot]
    small.end(4)
    small_out[...] = held[len(partners)]
    for slot in range(dp):
        qkv_across.receive(slot)
        for third in range(3):
            start = (third * dp + slot) * part
            qkv_out[:, start : start + part] = qkv_in[
                slot, :, third * part : (third + 1) * part
            ]
    paths(first.finish)
    paths(second.finish)
    for line in lines:
        line.finish()
    for chunk in range(dp):
        up_across.finish(chunk)
        qkv_across.finish(chunk)


def call_exchange(kernel, number, jobs, scatters, outs, args, extra=(), stages=0, unplaced=0):
    rows, width = args[0].shape if scatters else (4 * args[0].shape[0], args[0].shape[1])
    own = rows // 4
    room = []
    if scatters == 1:
        room = [(2, own, width), (own, width), (own, width)]
    if scatters == 2:
        room = [(2, 2, own, width), (2, own, width), (2, own, width)]
    return pl.pallas_call(
        kernel,
        in_specs=[pl.BlockSpec(memory_space=pltpu.VMEM)] * (len(args) - unplaced)
        + [pl.BlockSpec(memory_space=pl.ANY)] * unplaced,
        out_specs=[pl.BlockSpec(memory_space=pltpu.VMEM)] * len(outs),
        out_shape=[jax.ShapeDtypeStruct(shape, dtype) for shape, dtype in outs],
        scratch_shapes=[
            *(pltpu.VMEM(shape, BF16) for shape in room),
            *extra,
            pltpu.SemaphoreType.DMA((jobs, 2, 6 * STEPS)),
            *([pltpu.SemaphoreType.DMA(stages)] if stages else []),
        ],
        compiler_params=pltpu.CompilerParams(
            collective_id=number, has_side_effects=True, vmem_limit_bytes=60 << 20
        ),
        cost_estimate=pl.CostEstimate(
            flops=rows * width, bytes_accessed=200 << 20, transcendentals=0
        ),
    )(*args)


def pair_span(offset, pair):
    return pl.ds(offset + pair * 2 * HEAD_DIM, 2 * HEAD_DIM)


def head_parts(ref, offset, pair):
    both = ref[:, pair_span(offset, pair)]
    return both[:, :HEAD_DIM], both[:, HEAD_DIM:]


def dot_nt(a, b):
    return lax.dot_general(a, b, (((1,), (1,)), ((), ())), preferred_element_type=F32)


def dot_tn(a, b):
    return lax.dot_general(a, b, (((0,), (0,)), ((), ())), preferred_element_type=F32)


def attend_kernel(slope_ref, distance_ref, qkv_ref, mixed_ref, top_ref):
    width = mixed_ref.shape[1]
    lane = lax.broadcasted_iota(jnp.int32, (8, 128), 1)

    distance = distance_ref[...]
    tops = jnp.zeros((8, 128), F32)
    for pair in range(width // HEAD_DIM // 2):
        outs = []
        for t, (q, k, v) in enumerate(
            zip(*(head_parts(qkv_ref, part * width, pair) for part in range(3)))
        ):
            logits = dot_nt(q * jnp.asarray(SCALE, BF16), k)
            head_top = jnp.max(jnp.where(distance < MASKED, logits, -1e30))
            tops = jnp.where(lane == pair * 2 + t, head_top, tops)
            scores = logits - slope_ref[pair * 2 + t] * distance
            expos = jnp.exp(scores - jnp.max(scores, axis=-1, keepdims=True))
            probs = expos * (1.0 / jnp.sum(expos, axis=-1, keepdims=True))
            outs.append(jnp.dot(probs.astype(BF16), v, preferred_element_type=F32))
        mixed_ref[:, pair_span(0, pair)] = jnp.concatenate(outs, 1).astype(BF16)
    top_ref[...] = tops


def attend_back_kernel(slope_ref, distance_ref, qkv_ref, grad_ref, out_ref):
    width = grad_ref.shape[1]

    distance = distance_ref[...]
    for pair in range(width // HEAD_DIM // 2):
        outs = ([], [], [])
        parts = [head_parts(qkv_ref, part * width, pair) for part in range(3)]
        parts.append(head_parts(grad_ref, 0, pair))
        for t, (q, k, v, grad) in enumerate(zip(*parts)):
            low_q = q * jnp.asarray(SCALE, BF16)
            scores = dot_nt(low_q, k) - slope_ref[pair * 2 + t] * distance
            expos = jnp.exp(scores - jnp.max(scores, axis=-1, keepdims=True))
            probs = expos * (1.0 / jnp.sum(expos, axis=-1, keepdims=True))
            outs[2].append(dot_tn(probs.astype(BF16), grad))
            grad_probs = dot_nt(grad, v)
            inner = jnp.sum(grad_probs * probs, axis=-1, keepdims=True)
            grad_scores = (probs * (grad_probs - inner)).astype(BF16)
            outs[0].append(jnp.dot(grad_scores, k, preferred_element_type=F32) * SCALE)
            outs[1].append(dot_tn(grad_scores, low_q))
        for part in range(3):
            out_ref[:, pair_span(part * width, pair)] = jnp.concatenate(outs[part], 1).astype(BF16)


def attend(slopes, distance, qkv, length):
    rows, width = qkv.shape[0], qkv.shape[1] // 3
    blocks = rows // length
    mixed, tops = pl.pallas_call(
        attend_kernel,
        grid=(blocks,),
        in_specs=[
            pl.BlockSpec(memory_space=pltpu.SMEM),
            pl.BlockSpec((length, length), lambda b: (0, 0)),
            pl.BlockSpec((length, 3 * width), lambda b: (b, 0)),
        ],
        out_specs=[
            pl.BlockSpec((length, width), lambda b: (b, 0)),
            pl.BlockSpec((8, 128), lambda b: (b, 0)),
        ],
        out_shape=[
            jax.ShapeDtypeStruct((rows, width), BF16),
            jax.ShapeDtypeStruct((blocks * 8, 128), F32),
        ],
        cost_estimate=pl.CostEstimate(
            flops=4 * rows * length * width, bytes_accessed=8 * rows * width,
            transcendentals=rows * length * width // HEAD_DIM,
        ),
        name="attend",
    )(slopes, distance, qkv)
    return mixed, jnp.max(tops, axis=0)[: width // HEAD_DIM]


def attend_back(slopes, distance, qkv, grad, length):
    rows, width = grad.shape
    return pl.pallas_call(
        attend_back_kernel,
        grid=(rows // length,),
        in_specs=[
            pl.BlockSpec(memory_space=pltpu.SMEM),
            pl.BlockSpec((length, length), lambda b: (0, 0)),
            pl.BlockSpec((length, 3 * width), lambda b: (b, 0)),
            pl.BlockSpec((length, width), lambda b: (b, 0)),
        ],
        out_specs=pl.BlockSpec((length, 3 * width), lambda b: (b, 0)),
        out_shape=jax.ShapeDtypeStruct((rows, 3 * width), BF16),
        cost_estimate=pl.CostEstimate(
            flops=10 * rows * length * width, bytes_accessed=14 * rows * width,
            transcendentals=rows * length * width // HEAD_DIM,
        ),
        name="attend_back",
    )(slopes, distance, qkv, grad)


def norm_stats(values):
    row_mean = jnp.mean(values, axis=-1, keepdims=True)
    centred = values - row_mean
    inverse_std = lax.rsqrt(jnp.mean(centred * centred, axis=-1, keepdims=True) + EPS)
    return centred * inverse_std, inverse_std


def norm_back(grad_norm, normed, inverse_std, gain):
    scaled = grad_norm * gain
    return inverse_std * (
        scaled
        - jnp.mean(scaled, axis=-1, keepdims=True)
        - normed * jnp.mean(scaled * normed, axis=-1, keepdims=True)
    )


def dot(a, b):
    return jnp.dot(a, b, preferred_element_type=F32)


def layer(
    dp, fsdp, tokens, seq_lengths, w_qkv, bias_q, bias_v, w_out, bias_out, ln1_gain, ln1_bias,
    w_up, bias_up, w_down, bias_down, ln2_gain, ln2_bias, cotangent,
):
    length, width = tokens.shape
    shard = w_qkv.shape[0]
    ff = w_up.shape[1]
    heads = width // HEAD_DIM
    part, ff_part = width // dp, ff // dp
    local_heads = heads // dp
    spot, place = lax.axis_index("dp"), lax.axis_index("fsdp")
    rank = spot * fsdp + place
    both = (("fsdp", fsdp), ("dp", dp))

    out_w = lax.all_gather(w_out, "fsdp", axis=0, tiled=True)
    cols = w_qkv.reshape(shard, 3, dp, part).transpose(0, 2, 1, 3).reshape(shard, 3 * width)
    cols = lax.all_to_all(cols, "dp", 1, 0, tiled=True).reshape(dp, shard, 3 * part)
    qkv_w = lax.all_gather(cols, "fsdp", axis=1, tiled=True).reshape(width, 3 * part)
    w_up, cols = lax.optimization_barrier((w_up, cols))
    ups = lax.all_to_all(w_up, "dp", 1, 0, tiled=True)
    up_w = lax.all_gather(ups, "fsdp", axis=0, tiled=True)
    down_w = lax.all_gather(w_down, "fsdp", axis=0, tiled=True)
    late_tokens, _ = lax.optimization_barrier((tokens, ups))

    full_small = (bias_out, ln1_gain, ln1_bias, bias_down, ln2_gain, ln2_bias)
    row = jnp.concatenate(full_small + (bias_q, bias_v, bias_up))[None]
    table = jnp.zeros((dp * fsdp, row.shape[1]), BF16)
    table = lax.dynamic_update_slice(table, row, (rank, 0))
    wide = (4 * length, width)
    narrow = (length, width)
    kernels = dp == 4 and fsdp == 8 and length % (32 * STEPS) == 0 and ff == dp * width
    stages = len(bits_of(fsdp)) + 2
    if kernels:
        all_tokens, grad_y, table = call_exchange(
            functools.partial(gather_two_kernel, fsdp), 1, 2, 0,
            [(wide, BF16), (wide, BF16), (table.shape, BF16)], [late_tokens, cotangent, table],
            (pltpu.VMEM((stages + 1,) + table.shape, BF16), pltpu.VMEM((stages,) + table.shape, BF16)),
            (2, stages),
        )
    else:
        all_tokens, grad_y = gather_dp(late_tokens, dp), gather_dp(cotangent, dp)
        table = combine_all(table, both, jnp.add)
    table = table.astype(F32)
    small = [table[:, k * shard : (k + 1) * shard].reshape(1, width) for k in range(6)]
    out_b, gain1, shift1, down_b, gain2, shift2 = small
    mine = lax.dynamic_slice(table, (spot * fsdp, 0), (fsdp, row.shape[1]))[:, 6 * shard :]
    q_b, v_b = mine[:, :shard].reshape(1, part), mine[:, shard : 2 * shard].reshape(1, part)
    up_b = mine[:, 2 * shard :].reshape(1, ff_part)

    ranks = (spot * local_heads + 1 + jnp.arange(local_heads)).astype(F32)
    slopes = jnp.exp2(-8.0 * ranks / heads) * SCALE
    places = jnp.arange(length, dtype=jnp.int32)
    gap = places[:, None] - places[None, :]
    distance = jnp.where(gap >= 0, gap.astype(F32), MASKED)

    inputs = tokens.astype(F32)
    normed_all, _ = norm_stats(all_tokens.astype(F32))
    first_in = (normed_all * gain1 + shift1).astype(BF16)
    biases = jnp.concatenate([q_b, jnp.zeros_like(q_b), v_b], 1)
    qkv = (dot(first_in, qkv_w) + biases).astype(BF16)
    mixed, tops = attend(slopes, distance, qkv, length)
    out_part = dot(mixed, out_w).astype(BF16)
    if kernels:
        second_in, hidden = call_exchange(
            functools.partial(hidden_kernel, fsdp), 2, 2, 1, [(wide, BF16), (narrow, F32)],
            [out_part, tokens, jnp.concatenate([out_b, gain2, shift2], 0)],
        )
    else:
        hidden = inputs + scatter_dp(out_part, dp) + out_b
        normed2, inverse2 = norm_stats(hidden)
        second_in = regroup(normed2 * gain2 + shift2, dp, fsdp).astype(BF16)
        second_in = gather_dp(second_in, dp)

    upward = dot(second_in, up_w) + up_b
    cumulative = 0.5 * (1.0 + lax.erf(upward * (0.5**0.5)))
    active = (upward * cumulative).astype(BF16)
    slope = cumulative + upward * jnp.exp(-0.5 * upward * upward) * ((0.5 / jnp.pi) ** 0.5)
    active, slope = lax.optimization_barrier((active, slope.astype(BF16)))

    def reduce_rows(grad):
        return lax.psum_scatter(grad, "fsdp", scatter_dimension=0, tiled=True).astype(F32)

    def reduce_columns(grad):
        grad = grad.reshape(dp, fsdp * shard, grad.shape[1])
        return lax.psum_scatter(grad, "fsdp", scatter_dimension=1, tiled=True)

    def exchange_columns(grad):
        grad = grad.reshape(dp * shard, grad.shape[-1])
        return lax.all_to_all(grad, "dp", 0, 1, tiled=True).astype(F32)

    local_down = dot_tn(active, grad_y).astype(BF16)
    late_y, slope, _ = lax.optimization_barrier((grad_y, slope, local_down))
    grad_upward = (dot_nt(late_y, down_w) * slope).astype(BF16)
    grad_w_down = reduce_rows(local_down)
    local_up = dot_tn(second_in, grad_upward).astype(BF16)
    late_upward, _ = lax.optimization_barrier((grad_upward, local_up))
    second_part = dot_nt(late_upward, up_w).astype(BF16)
    scattered_up = lax.psum_scatter(local_up, "fsdp", scatter_dimension=0, tiled=True)
    if kernels:
        branch_all, grad_hidden, branch_sums, output_part = call_exchange(
            functools.partial(branch_kernel, fsdp), 3, 2, 1,
            [(wide, BF16), (narrow, F32), ((8, width), F32), (wide, BF16)],
            [second_part, hidden, cotangent, jnp.concatenate([out_b, gain2], 0), active, down_w],
            (pltpu.VMEM(active.shape, BF16), pltpu.VMEM(down_w.shape, BF16),
             pltpu.SemaphoreType.DMA((2,))),
            unplaced=2,
        )
    else:
        grad_second = regroup(scatter_dp(second_part, dp), fsdp, dp)
        grad_hidden = cotangent.astype(F32) + norm_back(grad_second, normed2, inverse2, gain2)
        grad_branch = grad_hidden.astype(BF16)
        branch_all = gather_dp(grad_branch, dp)
        branch_sums = jnp.stack([
            jnp.sum(piece, axis=0)
            for piece in (
                cotangent.astype(F32), grad_second * normed2, grad_second,
                grad_branch.astype(F32),
            )
        ])

    grad_mixed = dot_nt(branch_all, out_w).astype(BF16)
    grad_proj = attend_back(slopes, distance, qkv, grad_mixed, length)
    local_qkv = dot_tn(first_in, grad_proj).astype(BF16)
    late_branch, late_proj, _ = lax.optimization_barrier((branch_all, grad_proj, local_qkv))
    local_out = dot_tn(mixed, late_branch).astype(BF16)
    if not kernels:
        grad_w_qkv = exchange_columns(reduce_columns(local_qkv))
        grad_w_qkv = (
            grad_w_qkv.reshape(shard, dp, 3, part).transpose(0, 2, 1, 3).reshape(shard, 3 * width)
        )
        grad_w_out = reduce_rows(local_out)
    first_part = dot_nt(late_proj, qkv_w).astype(BF16)
    if not kernels:
        output_part = dot(active, down_w).astype(BF16)

    def spread(piece, size, fill=0.0):
        return lax.dynamic_update_slice(
            jnp.full((size,), fill, F32), piece, (spot * piece.shape[0],)
        )

    up_sum = jnp.sum(grad_upward.astype(F32), axis=0)
    q_sum = jnp.sum(grad_proj[:, :part].astype(F32), axis=0)
    v_sum = jnp.sum(grad_proj[:, 2 * part :].astype(F32), axis=0)
    if kernels:
        small = jnp.concatenate([
            branch_sums[:4].reshape(4 * width), spread(up_sum, ff), spread(q_sum, width),
            spread(v_sum, width), jnp.zeros((5 * width,), F32), spread(tops, width, -1e30),
        ]).reshape(-1, width)

        def room(grad):
            chips, piece = fsdp // 2, (grad.shape[0],) + grad.shape[2:]
            return tuple(
                pltpu.VMEM((count,) + piece, BF16) for count in (chips, chips, chips - 1, chips - 1)
            )

        def line_sems(grad):
            chips = fsdp // 2
            return pltpu.SemaphoreType.DMA((2, chips + 2 * (chips - 1) * grad.shape[0]))

        qkv_grad = local_qkv.reshape(dp, fsdp, shard, 3 * part)
        out_grad = local_out.reshape(1, fsdp, shard, width)
        grad_tokens, output, small, grad_w_qkv, grad_w_out, grad_w_up = call_exchange(
            functools.partial(last_kernel, fsdp), 4, 2, 2,
            [(narrow, BF16), (narrow, BF16), (small.shape, F32), (w_qkv.shape, BF16),
             ((1, shard, width), F32), (w_up.shape, BF16)],
            [first_part, jnp.concatenate([gain1, down_b], 0), small,
             scattered_up.reshape(dp, shard, ff_part), output_part, tokens, hidden, grad_hidden,
             qkv_grad, out_grad],
            (
                pltpu.VMEM((stages + 1,) + small.shape, F32),
                pltpu.VMEM((stages,) + small.shape, F32), pltpu.VMEM((8, width), F32),
                pltpu.VMEM(wide, BF16), pltpu.VMEM(narrow, BF16), pltpu.VMEM(narrow, F32),
                pltpu.VMEM(narrow, F32),
                *room(qkv_grad), *room(out_grad),
                pltpu.VMEM((dp, shard, 3 * part), F32), pltpu.VMEM((dp, shard, 3 * part), BF16),
                pltpu.VMEM((dp, shard, 3 * part), BF16), pltpu.VMEM((dp, shard, ff_part), BF16),
                pltpu.SemaphoreType.DMA((4,)), pltpu.SemaphoreType.DMA((fsdp // 2,)),
                pltpu.SemaphoreType.DMA((fsdp // 2,)), line_sems(qkv_grad), line_sems(out_grad),
                pltpu.SemaphoreType.DMA((2, 2, dp)),
            ),
            (2, stages), 6,
        )
        grad_w_out = grad_w_out[0]
        grad_w_qkv, grad_w_up = grad_w_qkv.astype(F32), grad_w_up.astype(F32)
    else:
        grad_first = scatter_dp(first_part, dp)
        normed1, inverse1 = norm_stats(inputs)
        grad_tokens = grad_hidden + norm_back(grad_first, normed1, inverse1, gain1)
        output = hidden + scatter_dp(output_part, dp) + down_b
        sums = (jnp.sum(grad_first * normed1, axis=0), jnp.sum(grad_first, axis=0))
        small = jnp.concatenate([
            branch_sums[:4].reshape(4 * width), spread(up_sum, ff), spread(q_sum, width),
            spread(v_sum, width), *sums, jnp.zeros((3 * width,), F32), spread(tops, width, -1e30),
        ]).reshape(-1, width)
        grad_w_up = exchange_columns(scattered_up)
        small = combine_all(small, both, sum_or_top)
    ups_at = 4 + ff // width
    owned = lax.dynamic_slice(small, (0, rank * shard), (small.shape[0], shard))
    ff_shard = ff // (dp * fsdp)
    owned_up = lax.dynamic_slice(
        small[4:ups_at].reshape(ff), (rank * ff_shard,), (ff_shard,)
    )

    head_top = small[-1, :heads]
    factor = jnp.sqrt(CLIP_TAU / jnp.maximum(head_top, CLIP_TAU))
    column = jnp.repeat(factor, HEAD_DIM)
    columns = jnp.concatenate([column, column, jnp.ones((width,), F32)])
    clipped = (w_qkv.astype(F32) * columns[None, :]).astype(BF16)
    return (
        output.astype(BF16),
        grad_tokens.astype(BF16),
        grad_w_qkv,
        owned[ups_at],
        owned[ups_at + 1],
        grad_w_out,
        owned[3],
        owned[ups_at + 2],
        owned[ups_at + 3],
        grad_w_up,
        owned_up,
        grad_w_down,
        owned[0],
        owned[1],
        owned[2],
        clipped,
    )


def solution(mesh):
    rows, flat = P(("dp", "fsdp"), None), P(("dp", "fsdp"))
    return jax.shard_map(
        functools.partial(layer, mesh.shape["dp"], mesh.shape["fsdp"]),
        mesh=mesh,
        in_specs=(
            rows, flat, rows, flat, flat, rows, flat, flat, flat, rows, flat, rows, flat, flat,
            flat, rows,
        ),
        out_specs=(
            rows, rows, rows, flat, flat, rows, flat, flat, flat, rows, flat, rows, flat, flat,
            flat, rows,
        ),
        check_vma=False,
    )
```

```python
import functools

import jax
import jax.numpy as jnp
from jax import lax
from jax.experimental import pallas as pl
from jax.experimental.pallas import tpu as pltpu
from jax.sharding import PartitionSpec as P


HEAD_DIM = 64
EPS = 1e-05
CLIP_TAU = 5.0
MASKED = 1e35
F32 = jnp.float32
BF16 = jnp.bfloat16
SCALE = HEAD_DIM ** (-0.5)


def swap(value, axis, size, bit):
    return lax.ppermute(value, axis, [(i, i ^ bit) for i in range(size)])


def bits_of(size):
    return [1 << b for b in range(size.bit_length() - 1)]


def gather_path(block, size, bits):
    blocks = {0: block}
    for bit in bits:
        held = sorted(blocks)
        moved = swap(jnp.concatenate([blocks[r] for r in held], 0), "dp", size, bit)
        for place, r in enumerate(held):
            rows = block.shape[0]
            blocks[r ^ bit] = moved[place * rows : (place + 1) * rows]
    return blocks


def gather_dp(block, size):
    half = block.shape[0] // 2
    top = gather_path(block[:half], size, bits_of(size))
    low = gather_path(block[half:], size, bits_of(size)[::-1])
    parts = []
    for r in range(size):
        parts += [top[r], low[r]]
    return jnp.concatenate(parts, 0)


def scatter_path(blocks, size, bits):
    blocks = dict(blocks)
    for bit in bits:
        away = sorted(r for r in blocks if r & bit)
        rows = blocks[0].shape[0]
        sent = jnp.concatenate([blocks[r].astype(BF16) for r in away], 0)
        moved = swap(sent, "dp", size, bit)
        blocks = {
            r ^ bit: blocks[r ^ bit].astype(F32)
            + moved[place * rows : (place + 1) * rows].astype(F32)
            for place, r in enumerate(away)
        }
    return blocks[0]


def scatter_dp(partial, size):
    rows = partial.shape[0] // size
    half = rows // 2
    top = {r: partial[r * rows : r * rows + half] for r in range(size)}
    low = {r: partial[r * rows + half : (r + 1) * rows] for r in range(size)}
    return jnp.concatenate(
        [scatter_path(top, size, bits_of(size)), scatter_path(low, size, bits_of(size)[::-1])], 0
    )


def combine_all(value, sizes, join):
    for axis, size in sizes:
        for bit in bits_of(size):
            value = join(value, swap(value, axis, size, bit))
    return value


STEPS = 4
MESH_IDS = pl.DeviceIdType.MESH
PATHS = ((1, 2), (2, 1))


def flipped(axis, mask):
    me = lax.axis_index(axis)
    there = me
    for bit in bits_of(2 ** mask.bit_length()):
        if mask & bit:
            there = there + bit - 2 * bit * ((me // bit) % 2)
    return {axis: there}


def neighbours(fsdp=1, every=False):
    near = {bit: flipped("dp", bit) for bit in (1, 2)}
    partners = [near[1], near[2]] + [flipped("fsdp", bit) for bit in bits_of(fsdp)]
    greeted = partners if fsdp > 1 else [near[1], near[2]]
    if every:
        greeted = [flipped("dp", mask) for mask in (1, 2, 3)]
        greeted += [flipped("fsdp", mask) for mask in range(1, fsdp)]
    barrier = pltpu.get_barrier_semaphore()
    for where in greeted:
        pl.semaphore_signal(barrier, inc=1, device_id=where, device_id_type=MESH_IDS)
    pl.semaphore_wait(barrier, len(greeted))
    return near, partners


def remote(source, target, sems, index, where):
    return pltpu.make_async_remote_copy(
        src_ref=source, dst_ref=target, send_sem=sems.at[0, index], recv_sem=sems.at[1, index],
        device_id=where, device_id_type=MESH_IDS,
    )


def each_step(act):
    def run(step, carry):
        act(step)
        return carry

    lax.fori_loop(0, STEPS, run, 0)


class Gather:
    def __init__(self, out, sems, near):
        self.out, self.sems, self.near = out, sems, near
        self.rows = out.shape[0] // 4
        self.step_rows = self.rows // 2 // STEPS

    def span(self, block, path, step):
        start = block * self.rows + path * (self.rows // 2) + step * self.step_rows
        return pl.ds(pl.multiple_of(start, self.step_rows), self.step_rows)

    def copy(self, source, bit, path, step, kind):
        return remote(
            self.out.at[self.span(source, path, step)],
            self.out.at[self.span(source + bit, path, step)],
            self.sems, (path * 3 + kind) * STEPS + step, self.near[bit],
        )

    def send(self, path, step):
        first, second = PATHS[path]
        self.copy(0, first, path, step, 0).start()
        self.copy(0, second, path, step, 1).start()

    def forward(self, path, step):
        first, second = PATHS[path]
        self.copy(0, first, path, step, 0).wait_recv()
        self.copy(first, second, path, step, 2).start()

    def finish(self, path, step):
        first, second = PATHS[path]
        self.copy(0, first, path, step, 0).wait_send()
        self.copy(0, second, path, step, 1).wait()
        self.copy(first, second, path, step, 2).wait()


class Scatter:
    def __init__(self, partial, landing, passing, last, sems, near):
        self.partial, self.landing, self.passing, self.last = partial, landing, passing, last
        self.sems, self.near = sems, near
        self.rows = partial.shape[0] // 4
        self.step_rows = self.rows // 2 // STEPS

    def span(self, block, path, step):
        start = block * self.rows + path * (self.rows // 2) + step * self.step_rows
        return pl.ds(pl.multiple_of(start, self.step_rows), self.step_rows)

    def own(self, path, step):
        return self.span(0, path, step)

    def opening(self, path, step, kind):
        first, _ = PATHS[path]
        return remote(
            self.partial.at[self.span((first, 3)[kind], path, step)],
            self.landing.at[kind, self.own(path, step)],
            self.sems, (path * 3 + kind) * STEPS + step, self.near[first],
        )

    def closing(self, path, step):
        rows = self.own(path, step)
        return remote(
            self.passing.at[rows], self.last.at[rows], self.sems,
            (path * 3 + 2) * STEPS + step, self.near[PATHS[path][1]],
        )

    def begin(self, path, step):
        for kind in range(2):
            self.opening(path, step, kind).start()

    def relay(self, path, step):
        _, second = PATHS[path]
        self.opening(path, step, 1).wait_recv()
        rows = self.own(path, step)
        self.passing[rows] = (
            self.partial[self.span(second, path, step)].astype(F32)
            + self.landing[1, rows].astype(F32)
        ).astype(BF16)
        self.closing(path, step).start()

    def total(self, path, step):
        self.opening(path, step, 0).wait_recv()
        self.closing(path, step).wait_recv()
        rows = self.own(path, step)
        return (
            self.partial[self.span(0, path, step)].astype(F32)
            + self.landing[0, rows].astype(F32)
            + self.last[rows].astype(F32)
        )

    def finish(self, path, step):
        for kind in range(2):
            self.opening(path, step, kind).wait_send()
        self.closing(path, step).wait_send()


def regroup(values, outer, inner):
    piece = values.shape[1] // (outer * inner)
    starts = [(o * inner + i) * piece for i in range(inner) for o in range(outer)]
    return jnp.concatenate([values[:, start : start + piece] for start in starts], 1)


def regroup_pairs(values, outer, inner):
    piece = values.shape[1] // (outer * inner)
    pair = 2 * piece
    left = lax.broadcasted_iota(jnp.int32, (values.shape[0], pair), 1) < piece
    slabs = {}
    for o in range(0, outer, 2):
        for i in range(0, inner, 2):
            one, two = (
                values[:, (k * inner + i) * piece : (k * inner + i) * piece + pair]
                for k in (o, o + 1)
            )
            slabs[i, o] = jnp.where(left, one, pltpu.roll(two, piece, 1))
            slabs[i + 1, o] = jnp.where(left, pltpu.roll(one, piece, 1), two)
    return jnp.concatenate([slabs[i, o] for i in range(inner) for o in range(0, outer, 2)], 1)


def row_norm(values):
    centred = values - jnp.mean(values, axis=-1, keepdims=True)
    inverse_std = lax.rsqrt(jnp.mean(centred * centred, axis=-1, keepdims=True) + EPS)
    return centred * inverse_std, inverse_std


def row_back(grad_norm, normed, inverse_std, gain):
    scaled = grad_norm * gain
    return inverse_std * (
        scaled
        - jnp.mean(scaled, axis=-1, keepdims=True)
        - normed * jnp.mean(scaled * normed, axis=-1, keepdims=True)
    )


class Doubling:
    def __init__(self, held, landing, sems, partners, join):
        self.held, self.landing, self.sems = held, landing, sems
        self.partners, self.join = partners, join

    def copy(self, stage):
        return remote(
            self.held.at[stage], self.landing.at[stage], self.sems, stage, self.partners[stage]
        )

    def start(self, stage):
        self.copy(stage).start()

    def end(self, stage):
        self.copy(stage).wait()
        self.held[stage + 1] = self.join(self.held[stage], self.landing[stage])

    def run(self, *stages):
        for stage in stages:
            self.start(stage)
            self.end(stage)


def gather_two_kernel(
    fsdp, one_ref, two_ref, table_ref, out_one, out_two, table_out, held, landing, sems, small_sems
):
    near, partners = neighbours(fsdp)
    jobs = []
    for k, (source, out) in enumerate(((one_ref, out_one), (two_ref, out_two))):
        out[: source.shape[0]] = source[...]
        jobs.append(Gather(out, sems.at[k], near))
    held[0] = table_ref[...]
    small = Doubling(held, landing, small_sems, partners[2:] + partners[:2], jnp.add)

    def paths(act):
        each_step(lambda step: [act(path, step) for path in range(2)])

    paths(jobs[0].send)
    small.run(*range(len(partners) - 2))
    small.start(len(partners) - 2)
    paths(jobs[0].forward)
    small.end(len(partners) - 2)
    small.start(len(partners) - 1)
    paths(jobs[1].send)
    small.end(len(partners) - 1)
    table_out[...] = held[len(partners)]
    paths(jobs[1].forward)
    for job in jobs:
        paths(job.finish)


def exchange(scatter, gather, rows_of, beside=None):
    each_step(lambda step: [scatter.begin(path, step) for path in range(2)])
    if beside is not None:
        beside()
    each_step(lambda step: [scatter.relay(path, step) for path in range(2)])

    def middle(step):
        for path in range(2):
            rows = scatter.own(path, step)
            gather.out[rows] = rows_of(rows, scatter.total(path, step))
            gather.send(path, step)

        @pl.when(step > 0)
        def _():
            for path in range(2):
                gather.forward(path, step - 1)

    each_step(middle)
    for path in range(2):
        gather.forward(path, STEPS - 1)
    each_step(lambda step: [scatter.finish(path, step) for path in range(2)])
    each_step(lambda step: [gather.finish(path, step) for path in range(2)])


def add_sums(sums_ref, values, start=0):
    for k, value in enumerate(values):
        row = start + k
        sums_ref[row : row + 1] += jnp.sum(value, axis=0, keepdims=True)


def hidden_kernel(
    fsdp, partial_ref, tokens_ref, params_ref, out_ref, hidden_ref, landing, passing, last, sems
):
    near, _ = neighbours()

    def rows_of(rows, total):
        hidden = tokens_ref[rows].astype(F32) + total + params_ref[0:1]
        hidden_ref[rows] = hidden
        normed, _ = row_norm(hidden)
        return regroup_pairs(
            normed * params_ref[1:2] + params_ref[2:3], 4, fsdp
        ).astype(BF16)

    exchange(
        Scatter(partial_ref, landing, passing, last, sems.at[0], near),
        Gather(out_ref, sems.at[1], near), rows_of,
    )


def branch_kernel(
    fsdp, partial_ref, hidden_ref, cotangent_ref, params_ref, active_ref, weight_ref, out_ref, grad_ref,
    sums_ref, output_ref, landing, passing, last, active, weight, copy_sems, sems,
):
    copies = [
        pltpu.make_async_copy(active_ref, active, copy_sems.at[0]),
        pltpu.make_async_copy(weight_ref, weight, copy_sems.at[1]),
    ]
    for copy in copies:
        copy.start()
    near, _ = neighbours()
    sums_ref[...] = jnp.zeros_like(sums_ref)

    def rows_of(rows, total):
        total = regroup_pairs(total, fsdp, 4)
        normed, inverse_std = row_norm(hidden_ref[rows])
        upper = cotangent_ref[rows].astype(F32)
        grad = upper + row_back(total, normed, inverse_std, params_ref[1:2])
        grad_ref[rows] = grad
        branch = grad.astype(BF16)
        add_sums(sums_ref, (upper, total * normed, total, branch.astype(F32)))
        return branch

    def output_tile(tile, carry):
        columns = pl.ds(pl.multiple_of(tile * 256, 256), 256)
        output_ref[:, columns] = dot(active[...], weight[:, columns]).astype(BF16)
        return carry

    def beside():
        for copy in copies:
            copy.wait()
        lax.fori_loop(0, output_ref.shape[1] // 256, output_tile, 0)

    exchange(
        Scatter(partial_ref, landing, passing, last, sems.at[0], near),
        Gather(out_ref, sems.at[1], near), rows_of, beside,
    )


def sum_or_top(a, b):
    row = lax.broadcasted_iota(jnp.int32, a.shape, 0)
    return jnp.where(row < a.shape[0] - 1, a + b, jnp.maximum(a, b))


class LineSum:
    def __init__(self, grad, own, merged, down, up, own_sems, sems, size):
        self.grad, self.merged, self.flows, self.sems = grad, merged, (down, up), sems
        self.own, self.own_sems = own, own_sems
        self.chips, self.chunks = size // 2, grad.shape[0]
        place = lax.axis_index("fsdp")
        self.chip, self.core = place // 2, place % 2
        self.next = ({"fsdp": place - 2}, {"fsdp": place + 2})

    def core_copy(self, piece):
        return remote(
            self.grad.at[:, piece * 2 + 1 - self.core], self.merged.at[piece], self.sems, piece,
            flipped("fsdp", 1),
        )

    def own_copy(self, piece):
        return pltpu.make_async_copy(
            self.grad.at[:, piece * 2 + self.core], self.own.at[piece], self.own_sems.at[piece]
        )

    def begin(self):
        for piece in range(self.chips):
            self.core_copy(piece).start()
            self.own_copy(piece).start()

    def each_chunk(self, act):
        if self.chunks == 1:
            return act(0)

        def run(chunk, carry):
            act(chunk)
            return carry

        return lax.fori_loop(0, self.chunks, run, 0)

    def merge(self):
        for piece in range(self.chips):
            self.core_copy(piece).wait_recv()
            self.own_copy(piece).wait()

            def add(chunk, piece=piece):
                self.merged[piece, chunk] = (
                    self.merged[piece, chunk].astype(F32)
                    + self.own[piece, chunk].astype(F32)
                ).astype(BF16)

            self.each_chunk(add)

    def hop(self, flow, step, chunk, source):
        index = self.chips + (flow * (self.chips - 1) + step - 1) * self.chunks + chunk
        return remote(
            source, self.flows[flow].at[step - 1, chunk], self.sems, index, self.next[flow]
        )

    def landed(self, flow, step, chunk):
        return self.hop(flow, step, chunk, self.flows[flow].at[step - 1, chunk])

    def ends(self, flow):
        return self.chip == (self.chips - 1, 0)[flow]

    def receives(self, flow, step):
        far = (self.chips - 1 - self.chip, self.chip)[flow]
        return (far >= 1) & (far <= step)

    def sends(self, flow, step):
        far = (self.chips - 1 - self.chip, self.chip)[flow]
        return far <= step - 1

    def piece(self, flow, step):
        return self.chip + (step - self.chips + 1, self.chips - 1 - step)[flow]

    def open(self, step):
        for flow in range(2):
            piece = (step - 1, self.chips - step)[flow]

            @pl.when(self.ends(flow))
            def _(flow=flow, piece=piece):
                self.each_chunk(
                    lambda chunk: self.hop(
                        flow, step, chunk, self.merged.at[piece, chunk]
                    ).start()
                )

    def relay(self, step):
        def one(chunk):
            for flow in range(2):

                @pl.when(self.receives(flow, step))
                def _(flow=flow):
                    self.landed(flow, step, chunk).wait_recv()
                    held = self.flows[flow]
                    held[step - 1, chunk] = (
                        held[step - 1, chunk].astype(F32)
                        + self.merged[self.piece(flow, step), chunk].astype(F32)
                    ).astype(BF16)
                    self.hop(flow, step + 1, chunk, held.at[step - 1, chunk]).start()

        self.each_chunk(one)

    def total(self, out, chunk):
        step = self.chips - 1
        out[chunk] = self.merged[self.chip, chunk].astype(F32)
        for flow in range(2):

            @pl.when(self.receives(flow, step))
            def _(flow=flow):
                self.landed(flow, step, chunk).wait_recv()
                out[chunk] += self.flows[flow][step - 1, chunk].astype(F32)

    def finish(self):
        for piece in range(self.chips):
            self.core_copy(piece).wait_send()
        for flow in range(2):
            for step in range(1, self.chips):

                @pl.when(self.sends(flow, step))
                def _(flow=flow, step=step):
                    self.each_chunk(lambda chunk: self.landed(flow, step, chunk).wait_send())


class Across:
    def __init__(self, source, landing, sems):
        self.source, self.landing, self.sems = source, landing, sems
        self.me = lax.axis_index("dp")

    def copy(self, chunk, slot):
        return pltpu.make_async_remote_copy(
            src_ref=self.source.at[chunk], dst_ref=self.landing.at[slot],
            send_sem=self.sems.at[0, chunk], recv_sem=self.sems.at[1, slot],
            device_id={"dp": chunk}, device_id_type=MESH_IDS,
        )

    def send(self, chunk):
        @pl.when(self.me != chunk)
        def _():
            self.copy(chunk, self.me).start()

        @pl.when(self.me == chunk)
        def _():
            self.landing[chunk] = self.source[chunk]

    def receive(self, slot):
        @pl.when(self.me != slot)
        def _():
            self.copy(slot, slot).wait_recv()

    def finish(self, chunk):
        @pl.when(self.me != chunk)
        def _():
            self.copy(chunk, self.me).wait_send()


def last_kernel(
    fsdp, first_ref, params_ref, small_ref, up_ref, output_any, tokens_any, hidden_any, grad_any,
    qkv_ref, out_ref, tokens_out, output_out, small_out, qkv_out, out_out, up_out, landing,
    passing, last, held, small_landing, sums, output_ref, tokens_ref, hidden_ref, grad_ref,
    qkv_own, qkv_merged, qkv_down, qkv_up, out_own, out_merged, out_down, out_up, qkv_total,
    qkv_low, qkv_in, up_in, copy_sems, qkv_own_sems, out_own_sems, qkv_sems, out_sems,
    across_sems, sems, small_sems,
):
    copies = [
        pltpu.make_async_copy(source, target, copy_sems.at[k])
        for k, (source, target) in enumerate((
            (output_any, output_ref), (tokens_any, tokens_ref), (hidden_any, hidden_ref),
            (grad_any, grad_ref),
        ))
    ]
    near, partners = neighbours(fsdp, True)
    dp, part = qkv_ref.shape[0], qkv_ref.shape[3] // 3
    chips = fsdp // 2
    lines = (
        LineSum(qkv_ref, qkv_own, qkv_merged, qkv_down, qkv_up, qkv_own_sems, qkv_sems, fsdp),
        LineSum(out_ref, out_own, out_merged, out_down, out_up, out_own_sems, out_sems, fsdp),
    )
    up_across = Across(up_ref, up_in, across_sems.at[0])
    qkv_across = Across(qkv_low, qkv_in, across_sems.at[1])
    small = Doubling(held, small_landing, small_sems, partners, sum_or_top)
    first, second = (
        Scatter(ref, landing.at[k], passing.at[k], last.at[k], sems.at[k], near)
        for k, ref in enumerate((first_ref, output_ref))
    )

    def first_rows(path, step):
        rows = first.own(path, step)
        total = first.total(path, step)
        normed, inverse_std = row_norm(tokens_ref[rows].astype(F32))
        grad = grad_ref[rows] + row_back(total, normed, inverse_std, params_ref[0:1])
        tokens_out[rows] = grad.astype(BF16)
        add_sums(sums, (total * normed, total), 2)

    def second_rows(path, step):
        rows = second.own(path, step)
        total = second.total(path, step)
        output_out[rows] = (hidden_ref[rows] + total + params_ref[1:2]).astype(BF16)

    def paths(act):
        each_step(lambda step: [act(path, step) for path in range(2)])

    paths(first.begin)
    for line in lines:
        line.begin()
    for copy in copies:
        copy.start()
    sums[...] = jnp.zeros_like(sums)
    for line in lines:
        line.merge()
    for step in range(1, chips):
        for line in lines:
            line.open(step)
    for copy in copies:
        copy.wait()
    paths(first.relay)
    paths(second.begin)
    for line in lines:
        line.relay(1)
    paths(first_rows)
    held[0, :8] = small_ref[:8]
    held[0, 8:] = small_ref[8:] + sums[...]
    small.start(0)
    paths(second.relay)
    small.end(0)
    small.start(1)
    for chunk in range(dp):
        up_across.send(chunk)
    for step in range(2, chips - 1):
        for line in lines:
            line.relay(step)
    small.end(1)
    small.start(2)
    paths(second_rows)
    small.end(2)
    small.start(3)
    for chunk in range(dp):
        lines[0].total(qkv_total, chunk)
        qkv_low[chunk] = qkv_total[chunk].astype(BF16)
        qkv_across.send(chunk)
    small.end(3)
    small.start(4)
    lines[1].total(out_out, 0)
    columns = up_ref.shape[2]
    for slot in range(dp):
        up_across.receive(slot)
        up_out[:, slot * columns : (slot + 1) * columns] = up_in[slot].astype(F32)
    small.end(4)
    small_out[...] = held[len(partners)]
    for slot in range(dp):
        qkv_across.receive(slot)
        for third in range(3):
            start = (third * dp + slot) * part
            qkv_out[:, start : start + part] = qkv_in[
                slot, :, third * part : (third + 1) * part
            ].astype(F32)
    paths(first.finish)
    paths(second.finish)
    for line in lines:
        line.finish()
    for chunk in range(dp):
        up_across.finish(chunk)
        qkv_across.finish(chunk)


def call_exchange(kernel, number, jobs, scatters, outs, args, extra=(), stages=0, unplaced=0):
    rows, width = args[0].shape if scatters else (4 * args[0].shape[0], args[0].shape[1])
    own = rows // 4
    room = []
    if scatters == 1:
        room = [(2, own, width), (own, width), (own, width)]
    if scatters == 2:
        room = [(2, 2, own, width), (2, own, width), (2, own, width)]
    return pl.pallas_call(
        kernel,
        in_specs=[pl.BlockSpec(memory_space=pltpu.VMEM)] * (len(args) - unplaced)
        + [pl.BlockSpec(memory_space=pl.ANY)] * unplaced,
        out_specs=[pl.BlockSpec(memory_space=pltpu.VMEM)] * len(outs),
        out_shape=[jax.ShapeDtypeStruct(shape, dtype) for shape, dtype in outs],
        scratch_shapes=[
            *(pltpu.VMEM(shape, BF16) for shape in room),
            *extra,
            pltpu.SemaphoreType.DMA((jobs, 2, 6 * STEPS)),
            *([pltpu.SemaphoreType.DMA(stages)] if stages else []),
        ],
        compiler_params=pltpu.CompilerParams(
            collective_id=number, has_side_effects=True, vmem_limit_bytes=60 << 20
        ),
        cost_estimate=pl.CostEstimate(
            flops=rows * width, bytes_accessed=200 << 20, transcendentals=0
        ),
    )(*args)


def pair_span(offset, pair):
    return pl.ds(offset + pair * 2 * HEAD_DIM, 2 * HEAD_DIM)


def head_parts(ref, offset, pair):
    both = ref[:, pair_span(offset, pair)]
    return both[:, :HEAD_DIM], both[:, HEAD_DIM:]


def dot_nt(a, b):
    return lax.dot_general(a, b, (((1,), (1,)), ((), ())), preferred_element_type=F32)


def dot_tn(a, b):
    return lax.dot_general(a, b, (((0,), (0,)), ((), ())), preferred_element_type=F32)


def attend_kernel(slope_ref, distance_ref, qkv_ref, mixed_ref, top_ref):
    width = mixed_ref.shape[1]
    lane = lax.broadcasted_iota(jnp.int32, (8, 128), 1)

    distance = distance_ref[...]
    tops = jnp.zeros((8, 128), F32)
    for pair in range(width // HEAD_DIM // 2):
        outs = []
        for t, (q, k, v) in enumerate(
            zip(*(head_parts(qkv_ref, part * width, pair) for part in range(3)))
        ):
            logits = dot_nt(q * jnp.asarray(SCALE, BF16), k)
            head_top = jnp.max(jnp.where(distance < MASKED, logits, -1e30))
            tops = jnp.where(lane == pair * 2 + t, head_top, tops)
            scores = logits - slope_ref[pair * 2 + t] * distance
            expos = jnp.exp(scores - jnp.max(scores, axis=-1, keepdims=True))
            probs = expos * (1.0 / jnp.sum(expos, axis=-1, keepdims=True))
            outs.append(jnp.dot(probs.astype(BF16), v, preferred_element_type=F32))
        mixed_ref[:, pair_span(0, pair)] = jnp.concatenate(outs, 1).astype(BF16)
    top_ref[...] = tops


def attend_back_kernel(slope_ref, distance_ref, qkv_ref, grad_ref, out_ref):
    width = grad_ref.shape[1]

    distance = distance_ref[...]
    for pair in range(width // HEAD_DIM // 2):
        outs = ([], [], [])
        parts = [head_parts(qkv_ref, part * width, pair) for part in range(3)]
        parts.append(head_parts(grad_ref, 0, pair))
        for t, (q, k, v, grad) in enumerate(zip(*parts)):
            low_q = q * jnp.asarray(SCALE, BF16)
            scores = dot_nt(low_q, k) - slope_ref[pair * 2 + t] * distance
            expos = jnp.exp(scores - jnp.max(scores, axis=-1, keepdims=True))
            probs = expos * (1.0 / jnp.sum(expos, axis=-1, keepdims=True))
            outs[2].append(dot_tn(probs.astype(BF16), grad))
            grad_probs = dot_nt(grad, v)
            inner = jnp.sum(grad_probs * probs, axis=-1, keepdims=True)
            grad_scores = (probs * (grad_probs - inner)).astype(BF16)
            outs[0].append(jnp.dot(grad_scores, k, preferred_element_type=F32) * SCALE)
            outs[1].append(dot_tn(grad_scores, low_q))
        for part in range(3):
            out_ref[:, pair_span(part * width, pair)] = jnp.concatenate(outs[part], 1).astype(BF16)


def attend(slopes, distance, qkv, length):
    rows, width = qkv.shape[0], qkv.shape[1] // 3
    blocks = rows // length
    mixed, tops = pl.pallas_call(
        attend_kernel,
        grid=(blocks,),
        in_specs=[
            pl.BlockSpec(memory_space=pltpu.SMEM),
            pl.BlockSpec((length, length), lambda b: (0, 0)),
            pl.BlockSpec((length, 3 * width), lambda b: (b, 0)),
        ],
        out_specs=[
            pl.BlockSpec((length, width), lambda b: (b, 0)),
            pl.BlockSpec((8, 128), lambda b: (b, 0)),
        ],
        out_shape=[
            jax.ShapeDtypeStruct((rows, width), BF16),
            jax.ShapeDtypeStruct((blocks * 8, 128), F32),
        ],
        cost_estimate=pl.CostEstimate(
            flops=4 * rows * length * width, bytes_accessed=8 * rows * width,
            transcendentals=rows * length * width // HEAD_DIM,
        ),
        name="attend",
    )(slopes, distance, qkv)
    return mixed, jnp.max(tops, axis=0)[: width // HEAD_DIM]


def attend_back(slopes, distance, qkv, grad, length):
    rows, width = grad.shape
    return pl.pallas_call(
        attend_back_kernel,
        grid=(rows // length,),
        in_specs=[
            pl.BlockSpec(memory_space=pltpu.SMEM),
            pl.BlockSpec((length, length), lambda b: (0, 0)),
            pl.BlockSpec((length, 3 * width), lambda b: (b, 0)),
            pl.BlockSpec((length, width), lambda b: (b, 0)),
        ],
        out_specs=pl.BlockSpec((length, 3 * width), lambda b: (b, 0)),
        out_shape=jax.ShapeDtypeStruct((rows, 3 * width), BF16),
        cost_estimate=pl.CostEstimate(
            flops=10 * rows * length * width, bytes_accessed=14 * rows * width,
            transcendentals=rows * length * width // HEAD_DIM,
        ),
        name="attend_back",
    )(slopes, distance, qkv, grad)


def norm_stats(values):
    row_mean = jnp.mean(values, axis=-1, keepdims=True)
    centred = values - row_mean
    inverse_std = lax.rsqrt(jnp.mean(centred * centred, axis=-1, keepdims=True) + EPS)
    return centred * inverse_std, inverse_std


def norm_back(grad_norm, normed, inverse_std, gain):
    scaled = grad_norm * gain
    return inverse_std * (
        scaled
        - jnp.mean(scaled, axis=-1, keepdims=True)
        - normed * jnp.mean(scaled * normed, axis=-1, keepdims=True)
    )


def dot(a, b):
    return jnp.dot(a, b, preferred_element_type=F32)


def layer(
    dp, fsdp, tokens, seq_lengths, w_qkv, bias_q, bias_v, w_out, bias_out, ln1_gain, ln1_bias,
    w_up, bias_up, w_down, bias_down, ln2_gain, ln2_bias, cotangent,
):
    length, width = tokens.shape
    shard = w_qkv.shape[0]
    ff = w_up.shape[1]
    heads = width // HEAD_DIM
    part, ff_part = width // dp, ff // dp
    local_heads = heads // dp
    spot, place = lax.axis_index("dp"), lax.axis_index("fsdp")
    rank = spot * fsdp + place
    both = (("fsdp", fsdp), ("dp", dp))

    out_w = lax.all_gather(w_out, "fsdp", axis=0, tiled=True)
    cols = w_qkv.reshape(shard, 3, dp, part).transpose(0, 2, 1, 3).reshape(shard, 3 * width)
    cols = lax.all_to_all(cols, "dp", 1, 0, tiled=True).reshape(dp, shard, 3 * part)
    qkv_w = lax.all_gather(cols, "fsdp", axis=1, tiled=True).reshape(width, 3 * part)
    w_up, cols = lax.optimization_barrier((w_up, cols))
    ups = lax.all_to_all(w_up, "dp", 1, 0, tiled=True)
    up_w = lax.all_gather(ups, "fsdp", axis=0, tiled=True)
    down_w = lax.all_gather(w_down, "fsdp", axis=0, tiled=True)
    late_tokens, _ = lax.optimization_barrier((tokens, ups))

    full_small = (bias_out, ln1_gain, ln1_bias, bias_down, ln2_gain, ln2_bias)
    row = jnp.concatenate(full_small + (bias_q, bias_v, bias_up))[None]
    table = jnp.zeros((dp * fsdp, row.shape[1]), BF16)
    table = lax.dynamic_update_slice(table, row, (rank, 0))
    wide = (4 * length, width)
    narrow = (length, width)
    kernels = dp == 4 and fsdp == 8 and length % (32 * STEPS) == 0 and ff == dp * width and shard == 64
    stages = len(bits_of(fsdp)) + 2
    if kernels:
        all_tokens, grad_y, table = call_exchange(
            functools.partial(gather_two_kernel, fsdp), 1, 2, 0,
            [(wide, BF16), (wide, BF16), (table.shape, BF16)], [late_tokens, cotangent, table],
            (pltpu.VMEM((stages + 1,) + table.shape, BF16), pltpu.VMEM((stages,) + table.shape, BF16)),
            (2, stages),
        )
    else:
        all_tokens, grad_y = gather_dp(late_tokens, dp), gather_dp(cotangent, dp)
        table = combine_all(table, both, jnp.add)
    table = table.astype(F32)
    small = [table[:, k * shard : (k + 1) * shard].reshape(1, width) for k in range(6)]
    out_b, gain1, shift1, down_b, gain2, shift2 = small
    mine = lax.dynamic_slice(table, (spot * fsdp, 0), (fsdp, row.shape[1]))[:, 6 * shard :]
    q_b, v_b = mine[:, :shard].reshape(1, part), mine[:, shard : 2 * shard].reshape(1, part)
    up_b = mine[:, 2 * shard :].reshape(1, ff_part)

    ranks = (spot * local_heads + 1 + jnp.arange(local_heads)).astype(F32)
    slopes = jnp.exp2(-8.0 * ranks / heads) * SCALE
    places = jnp.arange(length, dtype=jnp.int32)
    gap = places[:, None] - places[None, :]
    distance = jnp.where(gap >= 0, gap.astype(F32), MASKED)

    inputs = tokens.astype(F32)
    normed_all, _ = norm_stats(all_tokens.astype(F32))
    first_in = (normed_all * gain1 + shift1).astype(BF16)
    biases = jnp.concatenate([q_b, jnp.zeros_like(q_b), v_b], 1)
    qkv = (dot(first_in, qkv_w) + biases).astype(BF16)
    mixed, tops = attend(slopes, distance, qkv, length)
    out_part = dot(mixed, out_w).astype(BF16)
    if kernels:
        second_in, hidden = call_exchange(
            functools.partial(hidden_kernel, fsdp), 2, 2, 1, [(wide, BF16), (narrow, F32)],
            [out_part, tokens, jnp.concatenate([out_b, gain2, shift2], 0)],
        )
    else:
        hidden = inputs + scatter_dp(out_part, dp) + out_b
        normed2, inverse2 = norm_stats(hidden)
        second_in = regroup(normed2 * gain2 + shift2, dp, fsdp).astype(BF16)
        second_in = gather_dp(second_in, dp)

    upward = dot(second_in, up_w) + up_b
    cumulative = 0.5 * (1.0 + lax.erf(upward * (0.5**0.5)))
    active = (upward * cumulative).astype(BF16)
    slope = cumulative + upward * jnp.exp(-0.5 * upward * upward) * ((0.5 / jnp.pi) ** 0.5)
    active, slope = lax.optimization_barrier((active, slope.astype(BF16)))

    def reduce_rows(grad):
        return lax.psum_scatter(grad, "fsdp", scatter_dimension=0, tiled=True).astype(F32)

    def reduce_columns(grad):
        grad = grad.reshape(dp, fsdp * shard, grad.shape[1])
        return lax.psum_scatter(grad, "fsdp", scatter_dimension=1, tiled=True)

    def exchange_columns(grad):
        grad = grad.reshape(dp * shard, grad.shape[-1])
        return lax.all_to_all(grad, "dp", 0, 1, tiled=True).astype(F32)

    local_down = dot_tn(active, grad_y).astype(BF16)
    late_y, slope, _ = lax.optimization_barrier((grad_y, slope, local_down))
    grad_upward = (dot_nt(late_y, down_w) * slope).astype(BF16)
    grad_w_down = reduce_rows(local_down)
    local_up = dot_tn(second_in, grad_upward).astype(BF16)
    late_upward, _ = lax.optimization_barrier((grad_upward, local_up))
    second_part = dot_nt(late_upward, up_w).astype(BF16)
    scattered_up = lax.psum_scatter(local_up, "fsdp", scatter_dimension=0, tiled=True)
    if kernels:
        branch_all, grad_hidden, branch_sums, output_part = call_exchange(
            functools.partial(branch_kernel, fsdp), 3, 2, 1,
            [(wide, BF16), (narrow, F32), ((8, width), F32), (wide, BF16)],
            [second_part, hidden, cotangent, jnp.concatenate([out_b, gain2], 0), active, down_w],
            (pltpu.VMEM(active.shape, BF16), pltpu.VMEM(down_w.shape, BF16),
             pltpu.SemaphoreType.DMA((2,))),
            unplaced=2,
        )
    else:
        grad_second = regroup(scatter_dp(second_part, dp), fsdp, dp)
        grad_hidden = cotangent.astype(F32) + norm_back(grad_second, normed2, inverse2, gain2)
        grad_branch = grad_hidden.astype(BF16)
        branch_all = gather_dp(grad_branch, dp)
        branch_sums = jnp.stack([
            jnp.sum(piece, axis=0)
            for piece in (
                cotangent.astype(F32), grad_second * normed2, grad_second,
                grad_branch.astype(F32),
            )
        ])

    grad_mixed = dot_nt(branch_all, out_w).astype(BF16)
    grad_proj = attend_back(slopes, distance, qkv, grad_mixed, length)
    local_qkv = dot_tn(first_in, grad_proj).astype(BF16)
    late_branch, late_proj, _ = lax.optimization_barrier((branch_all, grad_proj, local_qkv))
    local_out = dot_tn(mixed, late_branch).astype(BF16)
    if not kernels:
        grad_w_qkv = exchange_columns(reduce_columns(local_qkv))
        grad_w_qkv = (
            grad_w_qkv.reshape(shard, dp, 3, part).transpose(0, 2, 1, 3).reshape(shard, 3 * width)
        )
        grad_w_out = reduce_rows(local_out)
    first_part = dot_nt(late_proj, qkv_w).astype(BF16)
    if not kernels:
        output_part = dot(active, down_w).astype(BF16)

    def spread(piece, size, fill=0.0):
        return lax.dynamic_update_slice(
            jnp.full((size,), fill, F32), piece, (spot * piece.shape[0],)
        )

    up_sum = jnp.sum(grad_upward.astype(F32), axis=0)
    q_sum = jnp.sum(grad_proj[:, :part].astype(F32), axis=0)
    v_sum = jnp.sum(grad_proj[:, 2 * part :].astype(F32), axis=0)
    if kernels:
        small = jnp.concatenate([
            branch_sums[:4].reshape(4 * width), spread(up_sum, ff), spread(q_sum, width),
            spread(v_sum, width), jnp.zeros((5 * width,), F32), spread(tops, width, -1e30),
        ]).reshape(-1, width)

        def room(grad):
            chips, piece = fsdp // 2, (grad.shape[0],) + grad.shape[2:]
            return tuple(
                pltpu.VMEM((count,) + piece, BF16) for count in (chips, chips, chips - 1, chips - 1)
            )

        def line_sems(grad):
            chips = fsdp // 2
            return pltpu.SemaphoreType.DMA((2, chips + 2 * (chips - 1) * grad.shape[0]))

        qkv_grad = local_qkv.reshape(dp, fsdp, shard, 3 * part)
        out_grad = local_out.reshape(1, fsdp, shard, width)
        grad_tokens, output, small, grad_w_qkv, grad_w_out, grad_w_up = call_exchange(
            functools.partial(last_kernel, fsdp), 4, 2, 2,
            [(narrow, BF16), (narrow, BF16), (small.shape, F32), (w_qkv.shape, F32),
             ((1, shard, width), F32), (w_up.shape, F32)],
            [first_part, jnp.concatenate([gain1, down_b], 0), small,
             scattered_up.reshape(dp, shard, ff_part), output_part, tokens, hidden, grad_hidden,
             qkv_grad, out_grad],
            (
                pltpu.VMEM((stages + 1,) + small.shape, F32),
                pltpu.VMEM((stages,) + small.shape, F32), pltpu.VMEM((8, width), F32),
                pltpu.VMEM(wide, BF16), pltpu.VMEM(narrow, BF16), pltpu.VMEM(narrow, F32),
                pltpu.VMEM(narrow, F32),
                *room(qkv_grad), *room(out_grad),
                pltpu.VMEM((dp, shard, 3 * part), F32), pltpu.VMEM((dp, shard, 3 * part), BF16),
                pltpu.VMEM((dp, shard, 3 * part), BF16), pltpu.VMEM((dp, shard, ff_part), BF16),
                pltpu.SemaphoreType.DMA((4,)), pltpu.SemaphoreType.DMA((fsdp // 2,)),
                pltpu.SemaphoreType.DMA((fsdp // 2,)), line_sems(qkv_grad), line_sems(out_grad),
                pltpu.SemaphoreType.DMA((2, 2, dp)),
            ),
            (2, stages), 6,
        )
        grad_w_out = grad_w_out[0]
    else:
        grad_first = scatter_dp(first_part, dp)
        normed1, inverse1 = norm_stats(inputs)
        grad_tokens = grad_hidden + norm_back(grad_first, normed1, inverse1, gain1)
        output = hidden + scatter_dp(output_part, dp) + down_b
        sums = (jnp.sum(grad_first * normed1, axis=0), jnp.sum(grad_first, axis=0))
        small = jnp.concatenate([
            branch_sums[:4].reshape(4 * width), spread(up_sum, ff), spread(q_sum, width),
            spread(v_sum, width), *sums, jnp.zeros((3 * width,), F32), spread(tops, width, -1e30),
        ]).reshape(-1, width)
        grad_w_up = exchange_columns(scattered_up)
        small = combine_all(small, both, sum_or_top)
    ups_at = 4 + ff // width
    owned = lax.dynamic_slice(small, (0, rank * shard), (small.shape[0], shard))
    ff_shard = ff // (dp * fsdp)
    owned_up = lax.dynamic_slice(
        small[4:ups_at].reshape(ff), (rank * ff_shard,), (ff_shard,)
    )

    head_top = small[-1, :heads]
    factor = jnp.sqrt(CLIP_TAU / jnp.maximum(head_top, CLIP_TAU))
    column = jnp.repeat(factor, HEAD_DIM)
    columns = jnp.concatenate([column, column, jnp.ones((width,), F32)])
    clipped = (w_qkv.astype(F32) * columns[None, :]).astype(BF16)
    return (
        output.astype(BF16),
        grad_tokens.astype(BF16),
        grad_w_qkv,
        owned[ups_at],
        owned[ups_at + 1],
        grad_w_out,
        owned[3],
        owned[ups_at + 2],
        owned[ups_at + 3],
        grad_w_up,
        owned_up,
        grad_w_down,
        owned[0],
        owned[1],
        owned[2],
        clipped,
    )


def solution(mesh):
    rows, flat = P(("dp", "fsdp"), None), P(("dp", "fsdp"))
    return jax.shard_map(
        functools.partial(layer, mesh.shape["dp"], mesh.shape["fsdp"]),
        mesh=mesh,
        in_specs=(
            rows, flat, rows, flat, flat, rows, flat, flat, flat, rows, flat, rows, flat, flat,
            flat, rows,
        ),
        out_specs=(
            rows, rows, rows, flat, flat, rows, flat, flat, flat, rows, flat, rows, flat, flat,
            flat, rows,
        ),
        check_vma=False,
    )
```
